32 devices in a mesh: dp: 4 (over x, y), fsdp: 8 (over z, core).
Axes of the slice: x: 2, y: 2, z: 4, core: 2. Of those that a mesh axis runs over, the one named last changes fastest.
Arguments:
- tokens: bfloat16 [256, 256, 2560], P(('dp', 'fsdp')), parts along dimension 0
- gain_in: bfloat16 [2560], P('fsdp')
- w_dq: bfloat16 [2560, 768], P('fsdp')
- gain_q: bfloat16 [768], P('fsdp')
- w_uq: bfloat16 [768, 3840], P('fsdp')
- w_dkv: bfloat16 [2560, 288], P('fsdp')
- gain_kv: bfloat16 [256], P('fsdp')
- w_ukv: bfloat16 [256, 5120], P('fsdp')
- w_out: bfloat16 [2560, 2560], P('fsdp')
Outputs:
- output 1: bfloat16 [256, 256, 2560], P(('dp', 'fsdp')), parts along dimension 0
- output 2: bfloat16 [256, 256, 256], P(('dp', 'fsdp')), parts along dimension 0
- output 3: bfloat16 [256, 256, 32], P(('dp', 'fsdp')), parts along dimension 0
There are 4 independent parts. The reference program is written for one: setup_inputs(seed, part) draws one part's arguments, and reference() takes and returns one part's arrays. A program takes and returns all parts, laid end to end along the dimension named above; an argument that names none is the same for every part.
All inputs are finite; a program needn't handle non-finite values.
Results may differ from the reference program's by a relative error of at most 0.00609399.
Values are sent between devices in bfloat16 or wider.
A program may use at most 1 GiB of HBM per device.

```python
import jax
import jax.numpy as jnp
from jax import lax

PROMPTS = 64
SEQ_LEN = 256
D_MODEL = 2560
N_HEADS = 40
Q_RANK = 768
KV_RANK = 256
NOPE_DIM = 64
ROPE_DIM = 32
V_DIM = 64
EPSILON = 1e-6
ROPE_THETA = 10000.0


def setup_inputs(seed: int = 0, part: int = 0) -> dict:
    key_list = jax.random.split(jax.random.key(seed), 9)

    def draw_weight(sub_key, n_rows, n_cols):
        drawn = jax.random.normal(sub_key, (n_rows, n_cols), jnp.float32) * (n_rows ** -0.5)
        return drawn.astype(jnp.bfloat16)

    def draw_gain(sub_key, n_items, centre):
        drawn = centre * (1.0 + 0.3 * jax.random.normal(sub_key, (n_items,), jnp.float32))
        return drawn.astype(jnp.bfloat16)

    tok_key = jax.random.fold_in(key_list[0], part)
    tokens = jax.random.normal(tok_key, (PROMPTS, SEQ_LEN, D_MODEL), jnp.float32).astype(jnp.bfloat16)
    return {
        'tokens': tokens,
        'gain_in': draw_gain(key_list[1], D_MODEL, 1.0),
        'w_dq': draw_weight(key_list[2], D_MODEL, Q_RANK),
        'gain_q': draw_gain(key_list[3], Q_RANK, 2.0),
        'w_uq': draw_weight(key_list[4], Q_RANK, N_HEADS * (NOPE_DIM + ROPE_DIM)),
        'w_dkv': draw_weight(key_list[5], D_MODEL, KV_RANK + ROPE_DIM),
        'gain_kv': draw_gain(key_list[6], KV_RANK, 1.0),
        'w_ukv': draw_weight(key_list[7], KV_RANK, N_HEADS * (NOPE_DIM + V_DIM)),
        'w_out': draw_weight(key_list[8], N_HEADS * V_DIM, D_MODEL),
    }


def rms_scale(values_in, gain_vec):
    values_f32 = values_in.astype(jnp.float32)
    inv_rms = lax.rsqrt(jnp.mean(values_f32 * values_f32, axis=-1, keepdims=True) + EPSILON)
    return values_f32 * inv_rms * gain_vec.astype(jnp.float32)


def rope_tables():
    half_dim = ROPE_DIM // 2
    inv_freq = ROPE_THETA ** (-2.0 * jnp.arange(half_dim, dtype=jnp.float32) / ROPE_DIM)
    angles = jnp.arange(SEQ_LEN, dtype=jnp.float32)[:, None] * inv_freq[None, :]
    return jnp.cos(angles), jnp.sin(angles)


def apply_rope(values_in, cos_t, sin_t):
    half_dim = values_in.shape[-1] // 2
    lo_half = values_in[..., :half_dim]
    hi_half = values_in[..., half_dim:]
    return jnp.concatenate([lo_half * cos_t - hi_half * sin_t, hi_half * cos_t + lo_half * sin_t], axis=-1)


def one_prompt(tok_rows, gain_in, w_dq, gain_q, w_uq, w_dkv, gain_kv, w_ukv, w_out):
    cos_t, sin_t = rope_tables()
    normed = rms_scale(tok_rows, gain_in).astype(jnp.bfloat16)
    q_down = jnp.dot(normed, w_dq, preferred_element_type=jnp.float32)
    q_lat = rms_scale(q_down, gain_q).astype(jnp.bfloat16)
    q_full = jnp.dot(q_lat, w_uq, preferred_element_type=jnp.float32).reshape(SEQ_LEN, N_HEADS, NOPE_DIM + ROPE_DIM)
    q_nope = q_full[:, :, :NOPE_DIM].astype(jnp.bfloat16)
    q_pe = apply_rope(q_full[:, :, NOPE_DIM:], cos_t[:, None, :], sin_t[:, None, :]).astype(jnp.bfloat16)
    kv_down = jnp.dot(normed, w_dkv, preferred_element_type=jnp.float32)
    latent = rms_scale(kv_down[:, :KV_RANK], gain_kv).astype(jnp.bfloat16)
    k_pe = apply_rope(kv_down[:, KV_RANK:], cos_t, sin_t).astype(jnp.bfloat16)
    kv_up = jnp.dot(latent, w_ukv, preferred_element_type=jnp.float32).astype(jnp.bfloat16)
    kv_up = kv_up.reshape(SEQ_LEN, N_HEADS, NOPE_DIM + V_DIM)
    k_nope = kv_up[:, :, :NOPE_DIM].astype(jnp.float32)
    values = kv_up[:, :, NOPE_DIM:].astype(jnp.float32)
    score_scale = (NOPE_DIM + ROPE_DIM) ** -0.5
    scores = jnp.einsum('qhd,khd->hqk', q_nope.astype(jnp.float32), k_nope)
    scores = scores + jnp.einsum('qhd,kd->hqk', q_pe.astype(jnp.float32), k_pe.astype(jnp.float32))
    causal = jnp.arange(SEQ_LEN)[:, None] >= jnp.arange(SEQ_LEN)[None, :]
    scores = jnp.where(causal[None, :, :], scores * score_scale, -1e30)
    attn_probs = jax.nn.softmax(scores, axis=-1).astype(jnp.bfloat16)
    attn_out = jnp.einsum('hqk,khd->qhd', attn_probs.astype(jnp.float32), values).astype(jnp.bfloat16)
    attn_out = attn_out.reshape(SEQ_LEN, N_HEADS * V_DIM)
    proj_out = jnp.dot(attn_out, w_out, preferred_element_type=jnp.float32)
    y_rows = (tok_rows.astype(jnp.float32) + proj_out).astype(jnp.bfloat16)
    return y_rows, latent, k_pe


def reference(tokens, gain_in, w_dq, gain_q, w_uq, w_dkv, gain_kv, w_ukv, w_out):
    def per_prompt(tok_rows):
        return one_prompt(tok_rows, gain_in, w_dq, gain_q, w_uq, w_dkv, gain_kv, w_ukv, w_out)

    y_out, kv_cache, pe_cache = lax.map(per_prompt, tokens)
    return (y_out, kv_cache, pe_cache)
```

```python
import functools

import jax
import jax.numpy as jnp
import numpy as np
from jax import lax
from jax.experimental import pallas as pl
from jax.experimental.pallas import tpu as pltpu
from jax.sharding import PartitionSpec as P

EPSILON = 1e-6
ROPE_THETA = 10000.0
LOG2E = 1.4426950408889634
VMEM_LIMIT = 64000 * 1024

NOPE, ROPE, VDIM = 64, 32, 64
HALF = ROPE // 2
GROUP = 8
PE_TILE = 4
LANES = 128


def rope_tiles(seq_len):
    inv_freq = ROPE_THETA ** (-2.0 * np.arange(HALF) / ROPE)
    angles = np.arange(seq_len)[:, None] * inv_freq[None, :]
    cos = np.tile(np.cos(angles), (1, LANES // HALF))
    sin = np.tile(np.sin(angles), (1, PE_TILE))
    return cos.astype(np.float32), np.concatenate([-sin, sin], axis=1).astype(np.float32)


def arrange_q(w):
    rows = w.shape[0]
    w = w.reshape(rows, -1, GROUP, NOPE + ROPE)
    nope = w[..., :NOPE].reshape(rows, -1, GROUP * NOPE)
    pe = w[..., NOPE:].reshape(rows, -1, GROUP // PE_TILE, PE_TILE, 2, HALF)
    pe = pe.transpose(0, 1, 2, 4, 3, 5).reshape(rows, -1, GROUP * ROPE)
    return jnp.concatenate([nope, pe], axis=-1).reshape(rows, -1)


def arrange_kv(w):
    rows = w.shape[0]
    return w.reshape(rows, -1, GROUP, 2, NOPE).transpose(0, 1, 3, 2, 4).reshape(rows, -1)


def arrange_dkv(w, kv_rank):
    lo, hi = w[:, kv_rank:kv_rank + HALF], w[:, kv_rank + HALF:]
    return jnp.concatenate([w[:, :kv_rank]] + [lo] * PE_TILE + [hi] * PE_TILE, axis=1)


def inv_rms(v):
    return lax.rsqrt(jnp.mean(v * v, axis=-1, keepdims=True) + EPSILON)


def rotate(tile, cos, sin):
    return tile * cos + pltpu.roll(tile, LANES // 2, 1) * sin


def down_kernel(x_ref, g1_ref, gq_ref, gkv_ref, wdq_ref, wdkv_ref, cos_ref, sin_ref, cq_ref, c_ref, rt_ref, r_ref):
    kv_rank = c_ref.shape[-1]
    for p in range(x_ref.shape[0]):
        x = x_ref[p].astype(jnp.float32)
        a = (x * inv_rms(x) * g1_ref[...]).astype(jnp.bfloat16)
        qd = jnp.dot(a, wdq_ref[...], preferred_element_type=jnp.float32)
        cq_ref[p] = (qd * inv_rms(qd) * gq_ref[...]).astype(jnp.bfloat16)
        kd = jnp.dot(a, wdkv_ref[...], preferred_element_type=jnp.float32)
        lat = kd[:, :kv_rank]
        c_ref[p] = (lat * inv_rms(lat) * gkv_ref[...]).astype(jnp.bfloat16)
        rt = rotate(kd[:, kv_rank:], cos_ref[...], sin_ref[...]).astype(jnp.bfloat16)
        rt_ref[p] = rt
        r_ref[p] = jnp.concatenate([rt[:, :HALF], rt[:, LANES // 2:LANES // 2 + HALF]], axis=1)


def attend_heads(q, kv, rt_slots, cos, sin, scale):
    seq_len = q.shape[0]
    half = seq_len // 2
    lane = lax.broadcasted_iota(jnp.int32, (1, LANES), 1)
    low = lane < NOPE
    diag = lax.broadcasted_iota(jnp.int32, (half, half), 0) >= lax.broadcasted_iota(jnp.int32, (half, half), 1)
    n_nope = GROUP * NOPE
    qn = q[:, :n_nope].astype(jnp.bfloat16)
    qp = [
        rotate(q[:, n_nope + t * LANES:n_nope + (t + 1) * LANES], cos, sin).astype(jnp.bfloat16)
        for t in range(GROUP // PE_TILE)
    ]
    kn = kv[:, :n_nope].astype(jnp.bfloat16)
    vv = kv[:, n_nope:].astype(jnp.bfloat16)
    zero = jnp.zeros((half, half), jnp.bfloat16)
    outs = []
    for quad in range(GROUP // 4):
        probs, vals = [], []
        for k in range(4):
            j = quad * 4 + k
            t, odd = j // 2, j % 2
            q_tile = jnp.concatenate([qn[:, t * LANES:(t + 1) * LANES], qp[j // PE_TILE]], axis=1)
            keep = low if odd == 0 else jnp.logical_not(low)
            k_tile = jnp.where(keep, kn[:, t * LANES:(t + 1) * LANES], 0)
            k_tile = jnp.concatenate([k_tile, rt_slots[j % PE_TILE]], axis=1)
            s = lax.dot_general(q_tile, k_tile, (((1,), (1,)), ((), ())), preferred_element_type=jnp.float32)
            s = s * scale
            top = jnp.where(diag, s[:half, :half], -1e30)
            left = s[half:, :half]
            right = jnp.where(diag, s[half:, half:], -1e30)
            m_top = jnp.max(top, axis=-1, keepdims=True)
            m_bot = jnp.max(jnp.maximum(left, right), axis=-1, keepdims=True)
            e_top = jnp.exp2(top - m_top)
            e_left = jnp.exp2(left - m_bot)
            e_right = jnp.exp2(right - m_bot)
            r_top = 1.0 / jnp.sum(e_top, axis=-1, keepdims=True)
            r_bot = 1.0 / jnp.sum(e_left + e_right, axis=-1, keepdims=True)
            p_top = jnp.concatenate([(e_top * r_top).astype(jnp.bfloat16), zero], axis=1)
            p_bot = jnp.concatenate([(e_left * r_bot).astype(jnp.bfloat16), (e_right * r_bot).astype(jnp.bfloat16)], axis=1)
            probs.append(jnp.concatenate([p_top, p_bot], axis=0))
            v_tile = jnp.where(keep, vv[:, t * LANES:(t + 1) * LANES], 0)
            blank = jnp.zeros_like(v_tile)
            vals.append(jnp.concatenate([v_tile, blank] if k < 2 else [blank, v_tile], axis=1))
        o = jnp.dot(
            jnp.concatenate(probs, axis=1), jnp.concatenate(vals, axis=0), preferred_element_type=jnp.float32
        )
        outs.append(o.astype(jnp.bfloat16))
    return jnp.concatenate(outs, axis=1)


def slot_masks(rt):
    lane = lax.broadcasted_iota(jnp.int32, (1, LANES), 1)
    slot = lax.rem(lane, LANES // 2) // HALF
    return [jnp.where(slot == j, rt, 0) for j in range(PE_TILE)]


def attend_kernel(cq_ref, c_ref, rt_ref, wuq_ref, wukv_ref, cos_ref, sin_ref, o_ref):
    n_groups = wuq_ref.shape[1] // (GROUP * (NOPE + ROPE))
    q_cols, kv_cols, o_cols = GROUP * (NOPE + ROPE), GROUP * (NOPE + VDIM), GROUP * VDIM
    scale = (NOPE + ROPE) ** -0.5 * LOG2E
    cq = cq_ref[0]
    lat = c_ref[0]
    slots = slot_masks(rt_ref[0])

    def body(g, carry):
        wq = wuq_ref[:, pl.ds(pl.multiple_of(g * q_cols, q_cols), q_cols)]
        wkv = wukv_ref[:, pl.ds(pl.multiple_of(g * kv_cols, kv_cols), kv_cols)]
        q = jnp.dot(cq, wq, preferred_element_type=jnp.float32)
        kv = jnp.dot(lat, wkv, preferred_element_type=jnp.float32)
        o = attend_heads(q, kv, slots, cos_ref[...], sin_ref[...], scale)
        o_ref[0, :, pl.ds(pl.multiple_of(g * o_cols, o_cols), o_cols)] = o
        return carry

    lax.fori_loop(0, n_groups, body, 0)


def out_kernel(x_ref, o_ref, w_ref, y_ref):
    step = 512
    o = o_ref[...]
    for n in range(0, y_ref.shape[1], step):
        acc = jnp.dot(o, w_ref[:, n:n + step], preferred_element_type=jnp.float32)
        y_ref[:, n:n + step] = (x_ref[:, n:n + step].astype(jnp.float32) + acc).astype(jnp.bfloat16)


def whole(shape):
    return pl.BlockSpec(shape, lambda i: (0,) * len(shape))


def solution(mesh):
    n_dp = mesh.shape['dp']
    params = pltpu.CompilerParams(vmem_limit_bytes=VMEM_LIMIT, dimension_semantics=("arbitrary",))

    def gather(w):
        rows = w.shape[0] // n_dp
        part = lax.dynamic_slice_in_dim(w, lax.axis_index('dp') * rows, rows, 0)
        return lax.all_gather(part, ('fsdp', 'dp'), tiled=True)

    def local_block(x, g1, wdq, gq, wuq, wdkv, gkv, wukv, wout):
        n_p, seq_len, d_model = x.shape
        kv_rank = gkv.shape[0] * mesh.shape['fsdp']
        cos_np, sin_np = rope_tiles(seq_len)
        cos, sin = jnp.asarray(cos_np), jnp.asarray(sin_np)
        gains = [lax.all_gather(g, 'fsdp', tiled=True).astype(jnp.float32)[None, :] for g in (g1, gq, gkv)]
        wdq_all = gather(wdq)
        wdkv_all = gather(arrange_dkv(wdkv, kv_rank))
        q_rank = wdq.shape[1]
        per = 2
        blk = lambda cols, n: pl.BlockSpec((n, seq_len, cols), lambda i: (i, 0, 0))
        out = lambda cols: jax.ShapeDtypeStruct((n_p, seq_len, cols), jnp.bfloat16)
        cq, c, rt, r = pl.pallas_call(
            down_kernel,
            grid=(n_p // per,),
            in_specs=[blk(d_model, per)] + [whole(v.shape) for v in (*gains, wdq_all, wdkv_all, cos, sin)],
            out_specs=[blk(q_rank, per), blk(kv_rank, per), blk(LANES, per), blk(ROPE, per)],
            out_shape=[out(q_rank), out(kv_rank), out(LANES), out(ROPE)],
            compiler_params=params,
            cost_estimate=pl.CostEstimate(flops=12_000_000_000, bytes_accessed=20_000_000, transcendentals=0),
            name="down",
        )(x, *gains, wdq_all, wdkv_all, cos, sin)
        wukv_all = gather(arrange_kv(wukv))
        wuq_all = gather(arrange_q(wuq))
        wout_all = gather(wout)
        o_cols = wout_all.shape[0]
        o = pl.pallas_call(
            attend_kernel,
            grid=(n_p,),
            in_specs=[blk(q_rank, 1), blk(kv_rank, 1), blk(LANES, 1)] + [whole(v.shape) for v in (wuq_all, wukv_all, cos, sin)],
            out_specs=blk(o_cols, 1),
            out_shape=out(o_cols),
            compiler_params=params,
            cost_estimate=pl.CostEstimate(flops=60_000_000_000, bytes_accessed=20_000_000, transcendentals=0),
            name="attend",
        )(cq, c, rt, wuq_all, wukv_all, cos, sin)
        rows = 512
        tile = pl.BlockSpec((rows, d_model), lambda i: (i, 0))
        y = pl.pallas_call(
            out_kernel,
            grid=(n_p * seq_len // rows,),
            in_specs=[tile, pl.BlockSpec((rows, o_cols), lambda i: (i, 0)), whole(wout_all.shape)],
            out_specs=tile,
            out_shape=jax.ShapeDtypeStruct((n_p * seq_len, d_model), jnp.bfloat16),
            compiler_params=params,
            cost_estimate=pl.CostEstimate(flops=27_000_000_000, bytes_accessed=45_000_000, transcendentals=0),
            name="project",
        )(x.reshape(n_p * seq_len, d_model), o.reshape(n_p * seq_len, o_cols), wout_all)
        return y.reshape(x.shape), c, r

    batch, row, mat = P(('dp', 'fsdp')), P('fsdp'), P('fsdp', None)
    return jax.shard_map(
        local_block,
        mesh=mesh,
        in_specs=(batch, row, mat, row, mat, mat, row, mat, mat),
        out_specs=(batch, batch, batch),
        check_vma=False,
    )
```

```python
import functools

import jax
import jax.numpy as jnp
import numpy as np
from jax import lax
from jax.experimental import pallas as pl
from jax.experimental.pallas import tpu as pltpu
from jax.sharding import PartitionSpec as P

EPSILON = 1e-6
ROPE_THETA = 10000.0
LOG2E = 1.4426950408889634
VMEM_LIMIT = 64000 * 1024

NOPE, ROPE, VDIM = 64, 32, 64
HALF = ROPE // 2
GROUP = 8
PE_TILE = 4
LANES = 128


def rope_tiles(seq_len):
    inv_freq = ROPE_THETA ** (-2.0 * np.arange(HALF) / ROPE)
    angles = np.arange(seq_len)[:, None] * inv_freq[None, :]
    cos = np.tile(np.cos(angles), (1, LANES // HALF))
    sin = np.tile(np.sin(angles), (1, PE_TILE))
    return cos.astype(np.float32), np.concatenate([-sin, sin], axis=1).astype(np.float32)


def arrange_q(w):
    rows = w.shape[0]
    w = w.reshape(rows, -1, GROUP, NOPE + ROPE)
    nope = w[..., :NOPE].reshape(rows, -1, GROUP * NOPE)
    pe = w[..., NOPE:].reshape(rows, -1, GROUP // PE_TILE, PE_TILE, 2, HALF)
    pe = pe.transpose(0, 1, 2, 4, 3, 5).reshape(rows, -1, GROUP * ROPE)
    return jnp.concatenate([nope, pe], axis=-1).reshape(rows, -1)


def arrange_kv(w):
    rows = w.shape[0]
    return w.reshape(rows, -1, GROUP, 2, NOPE).transpose(0, 1, 3, 2, 4).reshape(rows, -1)


def arrange_dkv(w, kv_rank):
    lo, hi = w[:, kv_rank:kv_rank + HALF], w[:, kv_rank + HALF:]
    return jnp.concatenate([w[:, :kv_rank]] + [lo] * PE_TILE + [hi] * PE_TILE, axis=1)


def inv_rms(v):
    return lax.rsqrt(jnp.mean(v * v, axis=-1, keepdims=True) + EPSILON)


def rotate(tile, cos, sin):
    return tile * cos + pltpu.roll(tile, LANES // 2, 1) * sin


def attend_heads(q, kv, rt_slots, cos, sin, scale):
    seq_len = q.shape[0]
    half = seq_len // 2
    lane = lax.broadcasted_iota(jnp.int32, (1, LANES), 1)
    low = lane < NOPE
    diag = lax.broadcasted_iota(jnp.int32, (half, half), 0) >= lax.broadcasted_iota(jnp.int32, (half, half), 1)
    n_nope = GROUP * NOPE
    qn = q[:, :n_nope].astype(jnp.bfloat16)
    qp = [
        rotate(q[:, n_nope + t * LANES:n_nope + (t + 1) * LANES], cos, sin).astype(jnp.bfloat16)
        for t in range(GROUP // PE_TILE)
    ]
    kn = kv[:, :n_nope].astype(jnp.bfloat16)
    vv = kv[:, n_nope:].astype(jnp.bfloat16)
    zero = jnp.zeros((half, half), jnp.bfloat16)
    outs = []
    for quad in range(GROUP // 4):
        probs, vals = [], []
        for k in range(4):
            j = quad * 4 + k
            t, odd = j // 2, j % 2
            q_tile = jnp.concatenate([qn[:, t * LANES:(t + 1) * LANES], qp[j // PE_TILE]], axis=1)
            keep = low if odd == 0 else jnp.logical_not(low)
            k_tile = jnp.where(keep, kn[:, t * LANES:(t + 1) * LANES], 0)
            k_tile = jnp.concatenate([k_tile, rt_slots[j % PE_TILE]], axis=1)
            s = lax.dot_general(q_tile, k_tile, (((1,), (1,)), ((), ())), preferred_element_type=jnp.float32)
            s = s * scale
            top = jnp.where(diag, s[:half, :half], -1e30)
            left = s[half:, :half]
            right = jnp.where(diag, s[half:, half:], -1e30)
            m_top = jnp.max(top, axis=-1, keepdims=True)
            m_bot = jnp.max(jnp.maximum(left, right), axis=-1, keepdims=True)
            e_top = jnp.exp2(top - m_top)
            e_left = jnp.exp2(left - m_bot)
            e_right = jnp.exp2(right - m_bot)
            r_top = 1.0 / jnp.sum(e_top, axis=-1, keepdims=True)
            r_bot = 1.0 / jnp.sum(e_left + e_right, axis=-1, keepdims=True)
            p_top = jnp.concatenate([(e_top * r_top).astype(jnp.bfloat16), zero], axis=1)
            p_bot = jnp.concatenate([(e_left * r_bot).astype(jnp.bfloat16), (e_right * r_bot).astype(jnp.bfloat16)], axis=1)
            probs.append(jnp.concatenate([p_top, p_bot], axis=0))
            v_tile = jnp.where(keep, vv[:, t * LANES:(t + 1) * LANES], 0)
            blank = jnp.zeros_like(v_tile)
            vals.append(jnp.concatenate([v_tile, blank] if k < 2 else [blank, v_tile], axis=1))
        o = jnp.dot(
            jnp.concatenate(probs, axis=1), jnp.concatenate(vals, axis=0), preferred_element_type=jnp.float32
        )
        outs.append(o.astype(jnp.bfloat16))
    return jnp.concatenate(outs, axis=1)


def slot_masks(rt):
    lane = lax.broadcasted_iota(jnp.int32, (1, LANES), 1)
    slot = lax.rem(lane, LANES // 2) // HALF
    return [jnp.where(slot == j, rt, 0) for j in range(PE_TILE)]


MESH = pl.DeviceIdType.MESH
GROUPS_FIRST = 2
GAIN_ROWS = 32
N_SEND, N_RECV = 19, 19


class Item:
    def __init__(self, index, shard, col, cols, full):
        self.index, self.shard, self.col, self.cols, self.full = index, shard, col, cols, full
        self.rows = shard.shape[0]
        if (self.rows // 4) % 16 == 0:
            self.q_rows, self.q_cols = self.rows // 4, cols
        elif (cols // 4) % LANES == 0 and self.rows == 32:
            self.q_rows, self.q_cols = self.rows, cols // 4
        else:
            self.q_rows, self.q_cols = self.rows // 2, cols // 2
        if self.q_rows == self.rows:
            n = self.q_rows // 2
            self.halves = [(0, n, 0, self.q_cols), (n, n, 0, self.q_cols)]
        else:
            n = -(-self.q_cols // (2 * LANES)) * LANES
            self.halves = [(0, self.q_rows, 0, n), (0, self.q_rows, n, self.q_cols - n)]

    def quarter(self, q):
        per_row = self.cols // self.q_cols
        return (q // per_row) * self.q_rows, lax.rem(q, per_row) * self.q_cols

    def source(self, q):
        r, c = self.quarter(q)
        return self.shard.at[pl.ds(pl.multiple_of(r, 16), self.q_rows), pl.ds(pl.multiple_of(self.col + c, LANES), self.q_cols)]

    def own(self):
        return self.shard.at[:, pl.ds(self.col, self.cols)]

    def place(self, f, q=None, half=None):
        r, c = (0, 0) if q is None else self.quarter(q)
        r = f * self.rows + r
        if q is None:
            n_r, n_c = self.rows, self.cols
        elif half is None:
            n_r, n_c = self.q_rows, self.q_cols
        else:
            dr, n_r, dc, n_c = self.halves[half]
            r, c = r + dr, c + dc
        if n_c == self.cols:
            return self.full.at[pl.ds(pl.multiple_of(r, 16), n_r)]
        return self.full.at[pl.ds(pl.multiple_of(r, 16), n_r), pl.ds(pl.multiple_of(c, LANES), n_c)]


def core_kernel(
    n_prompts, x_ref, gs_ref, dq_s, dkv_s, uq_s, ukv_s, out_s, cos_ref, sin_ref,
    c_ref, r_ref, oa_ref, ob_ref, wout_ref,
    wdq, wdkv, wuqa, wuqb, wukva, wukvb, gains, gvec, cq_all, c_all, rt_all, stage,
    send_sem, recv_sem, g_send, g_recv, local_sem,
):
    i = pl.program_id(0)
    d, f = lax.axis_index('dp'), lax.axis_index('fsdp')
    z, core = f // 2, lax.rem(f, 2)
    dx = lax.rem(d + 2, 4)
    dy = d + 1 - 2 * lax.rem(d, 2)
    dd = lax.rem(dy + 2, 4)
    sib = z * 2 + 1 - core
    n_a = wuqa.shape[1]
    m_a = wukva.shape[1]
    dkv = Item(0, dkv_s, 0, wdkv.shape[1], wdkv)
    dq = Item(1, dq_s, 0, wdq.shape[1], wdq)
    ukva = Item(2, ukv_s, 0, m_a, wukva)
    uqa = Item(3, uq_s, 0, n_a, wuqa)
    ukvb = Item(4, ukv_s, m_a, wukvb.shape[1], wukvb)
    uqb = Item(5, uq_s, n_a, wuqb.shape[1], wuqb)
    wo = Item(6, out_s, 0, wout_ref.shape[1], wout_ref)
    items = [dkv, dq, ukva, uqa, ukvb, uqb, wo]

    def to(k):
        return lax.rem(z + k, 4) * 2 + core

    def origin(k):
        return lax.rem(z + 4 - k, 4) * 2 + core

    def copy(it, src, dst, s, r, dev):
        return pltpu.make_async_remote_copy(
            src_ref=src, dst_ref=dst, send_sem=send_sem.at[it.index, s], recv_sem=recv_sem.at[it.index, r],
            device_id=dev, device_id_type=MESH,
        )

    def along_z(it, k):
        return copy(it, it.source(d), it.place(f, d), k - 1, k - 1, (d, to(k)))

    def to_x(it, k):
        ref = it.place(origin(k), d)
        return copy(it, ref, ref, 2 + k, 2 + k, (dx, f))

    def to_y(it, k):
        ref = it.place(origin(k), d)
        return copy(it, ref, ref, 5 + k, 5 + k, (dy, f))

    def diag_y(it, k):
        ref = it.place(origin(k), dx, 0)
        return copy(it, ref, ref, 8 + k, 8 + k, (dy, f))

    def diag_x(it, k):
        ref = it.place(origin(k), dy, 1)
        return copy(it, ref, ref, 11 + k, 11 + k, (dx, f))

    def to_core(it, k):
        ref = it.place(origin(k))
        return copy(it, ref, ref, 14 + k, 14 + k, (d, sib))

    def own_copy(it):
        return copy(it, it.own(), it.place(f), 18, 18, (d, sib))

    def arrived(it, ref, r):
        return copy(it, ref, ref, 0, r, (d, f)).wait_recv()

    def keep(it):
        return pltpu.make_async_copy(it.own(), stage if it is wo else it.place(f), local_sem.at[it.index])

    def keep_out():
        return pltpu.make_async_copy(stage, wo.place(f), local_sem.at[7])

    def gain_copy(j):
        return pltpu.make_async_remote_copy(
            src_ref=gs_ref, dst_ref=gains.at[f], send_sem=g_send.at[j - 1], recv_sem=g_recv.at[j - 1],
            device_id=(d, lax.rem(f + j, 8)), device_id_type=MESH,
        )

    def a2(it, ks=(1, 2, 3)):
        for k in ks:
            arrived(it, it.place(origin(k), d), k - 1)
            to_x(it, k).start()
            to_y(it, k).start()

    def a3(it, ks=(1, 2, 3)):
        for k in ks:
            arrived(it, it.place(origin(k), dx), 2 + k)
            diag_y(it, k).start()
            arrived(it, it.place(origin(k), dy), 5 + k)
            diag_x(it, k).start()

    def a4(it, ks=(1, 2, 3)):
        for k in ks:
            arrived(it, it.place(origin(k), dd, 0), 8 + k)
            arrived(it, it.place(origin(k), dd, 1), 11 + k)
            to_core(it, k).start()

    def a5(it):
        (keep_out() if it is wo else keep(it)).wait()
        for k in (1, 2, 3):
            arrived(it, it.place(lax.rem(z + 4 - k, 4) * 2 + 1 - core), 14 + k)
        arrived(it, it.place(sib), 18)

    def sent(it):
        for k in (1, 2, 3):
            for make in (along_z, to_x, to_y, diag_y, diag_x, to_core):
                make(it, k).wait_send()

    @pl.when(i == 0)
    def _():
        barrier = pltpu.get_barrier_semaphore()
        peers = [(dx, f), (dy, f)] + [(d, lax.rem(f + j, 8)) for j in range(1, 8)]
        for peer in peers:
            pl.semaphore_signal(barrier, inc=1, device_id=peer, device_id_type=MESH)
        pl.semaphore_wait(barrier, len(peers))
        for j in range(1, 8):
            gain_copy(j).start()
        g_own = pltpu.make_async_copy(gs_ref, gains.at[f], local_sem.at[8])
        g_own.start()
        for it in items:
            for k in (1, 2, 3):
                along_z(it, k).start()
            own_copy(it).start()
            keep(it).start()
        keep(wo).wait()
        keep_out().start()
        for j in range(1, 8):
            gain_copy(j).wait_recv()
        g_own.wait()
        total = jnp.sum(gains[...], axis=0)
        for t in range(gvec.shape[1] // LANES):
            gvec[:, t * LANES:(t + 1) * LANES] = total[t:t + 1, :]
        a2(dkv)
        a2(dq, (1,))
        a3(dkv)
        a2(dq, (2, 3))
        a4(dkv)
        a3(dq)
        a2(ukva)
        a4(dq)
        a3(ukva)
        a5(dkv)
        a5(dq)

    plan = {
        1: lambda: (a2(uqa), a4(ukva)),
        2: lambda: (a2(ukvb), a3(uqa)),
        3: lambda: (a4(uqa), a3(ukvb)),
        5: lambda: (a4(ukvb), a2(uqb)),
        7: lambda: a3(uqb),
        8: lambda: (a5(ukva), a5(uqa), a4(uqb)),
        10: lambda: a2(wo, (1,)),
        12: lambda: a3(wo, (1,)),
        13: lambda: a2(wo, (2,)),
        14: lambda: a4(wo, (1,)),
        15: lambda: a3(wo, (2,)),
        16: lambda: (a5(ukvb), a5(uqb), a2(wo, (3,))),
        17: lambda: (a4(wo, (2,)), a3(wo, (3,))),
        19: lambda: a4(wo, (3,)),
    }
    for step, act in plan.items():
        @pl.when(i == step)
        def _(act=act):
            act()

    d_model, q_rank, kv_rank = x_ref.shape[-1], cq_all.shape[-1], c_all.shape[-1]

    @pl.when(i < n_prompts)
    def _():
        x = x_ref[0].astype(jnp.float32)
        a = (x * inv_rms(x) * gvec[:, :d_model]).astype(jnp.bfloat16)
        qd = jnp.dot(a, wdq[...], preferred_element_type=jnp.float32)
        cq_all[i] = (qd * inv_rms(qd) * gvec[:, d_model:d_model + q_rank]).astype(jnp.bfloat16)
        kd = jnp.dot(a, wdkv[...], preferred_element_type=jnp.float32)
        lat = kd[:, :kv_rank]
        lat = (lat * inv_rms(lat) * gvec[:, d_model + q_rank:]).astype(jnp.bfloat16)
        c_all[i] = lat
        c_ref[0] = lat
        rt = rotate(kd[:, kv_rank:], cos_ref[...], sin_ref[...]).astype(jnp.bfloat16)
        rt_all[i] = rt
        r_ref[0] = jnp.concatenate([rt[:, :HALF], rt[:, LANES // 2:LANES // 2 + HALF]], axis=1)

    q_cols, kv_cols, o_cols = GROUP * (NOPE + ROPE), GROUP * (NOPE + VDIM), GROUP * VDIM
    scale = (NOPE + ROPE) ** -0.5 * LOG2E

    def attend(p, wuq, wukv, o_ref):
        cq = cq_all[p]
        lat = c_all[p]
        slots = slot_masks(rt_all[p])

        def body(g, carry):
            wq = wuq[:, pl.ds(pl.multiple_of(g * q_cols, q_cols), q_cols)]
            wkv = wukv[:, pl.ds(pl.multiple_of(g * kv_cols, kv_cols), kv_cols)]
            q = jnp.dot(cq, wq, preferred_element_type=jnp.float32)
            kv = jnp.dot(lat, wkv, preferred_element_type=jnp.float32)
            o = attend_heads(q, kv, slots, cos_ref[...], sin_ref[...], scale)
            o_ref[0, :, pl.ds(pl.multiple_of(g * o_cols, o_cols), o_cols)] = o
            return carry

        lax.fori_loop(0, wuq.shape[1] // q_cols, body, 0)

    @pl.when(jnp.logical_and(i >= n_prompts, i < 2 * n_prompts))
    def _():
        attend(i - n_prompts, wuqa, wukva, oa_ref)

    @pl.when(i >= 2 * n_prompts)
    def _():
        attend(i - 2 * n_prompts, wuqb, wukvb, ob_ref)

    @pl.when(i == 3 * n_prompts - 1)
    def _():
        a5(wo)
        for j in range(1, 8):
            gain_copy(j).wait_send()
        for it in items:
            sent(it)
            own_copy(it).wait_send()


def slot_masks(rt):
    lane = lax.broadcasted_iota(jnp.int32, (1, LANES), 1)
    slot = lax.rem(lane, LANES // 2) // HALF
    return [jnp.where(slot == j, rt, 0) for j in range(PE_TILE)]


def out_kernel(x_ref, oa_ref, ob_ref, w_ref, c_in, r_in, y_ref, c_out, r_out):
    step = 512
    oa, ob = oa_ref[...], ob_ref[...]
    n_a = oa.shape[1]
    c_out[...] = c_in[...]
    r_out[...] = r_in[...]
    for n in range(0, y_ref.shape[1], step):
        acc = jnp.dot(oa, w_ref[:n_a, n:n + step], preferred_element_type=jnp.float32)
        acc += jnp.dot(ob, w_ref[n_a:, n:n + step], preferred_element_type=jnp.float32)
        y_ref[:, n:n + step] = (x_ref[:, n:n + step].astype(jnp.float32) + acc).astype(jnp.bfloat16)


def whole(shape):
    return pl.BlockSpec(shape, lambda i: (0,) * len(shape))


def solution(mesh):
    n_fsdp = mesh.shape['fsdp']

    def local_block(x, g1, wdq, gq, wuq, wdkv, gkv, wukv, wout):
        n_p, seq_len, d_model = x.shape
        kv_rank, q_rank = gkv.shape[0] * n_fsdp, wdq.shape[1]
        cos_np, sin_np = rope_tiles(seq_len)
        cos, sin = jnp.asarray(cos_np), jnp.asarray(sin_np)
        me = lax.axis_index('fsdp')
        spread = [
            lax.dynamic_update_slice(jnp.zeros(g.shape[0] * n_fsdp, jnp.float32), g.astype(jnp.float32), (me * g.shape[0],))
            for g in (g1, gq, gkv)
        ]
        n_gain = d_model + q_rank + kv_rank
        gs = jnp.concatenate(spread + [jnp.zeros(GAIN_ROWS * LANES - n_gain, jnp.float32)]).reshape(GAIN_ROWS, LANES)
        shards = [wdq, arrange_dkv(wdkv, kv_rank), arrange_q(wuq), arrange_kv(wukv), wout]
        full = lambda w, cols: pltpu.VMEM((w.shape[0] * n_fsdp, cols), jnp.bfloat16)
        q_cols, kv_cols, o_cols = GROUP * (NOPE + ROPE), GROUP * (NOPE + VDIM), GROUP * VDIM
        n_groups = wuq.shape[1] // q_cols
        first, rest = GROUPS_FIRST, n_groups - GROUPS_FIRST
        last = n_p - 1
        blk = lambda cols, lag: pl.BlockSpec((1, seq_len, cols), lambda i: (jnp.clip(i - lag * n_p, 0, last), 0, 0))
        out = lambda cols: jax.ShapeDtypeStruct((n_p, seq_len, cols), jnp.bfloat16)
        hbm = pl.BlockSpec(memory_space=pl.ANY)
        c, r, oa, ob, wout_all = pl.pallas_call(
            functools.partial(core_kernel, n_p),
            grid=(3 * n_p,),
            in_specs=[blk(d_model, 0)] + [hbm] * 6 + [whole(cos.shape)] * 2,
            out_specs=[blk(kv_rank, 0), blk(ROPE, 0), blk(first * o_cols, 1), blk(rest * o_cols, 2), hbm],
            out_shape=[
                out(kv_rank), out(ROPE), out(first * o_cols), out(rest * o_cols),
                jax.ShapeDtypeStruct((wout.shape[0] * n_fsdp, wout.shape[1]), jnp.bfloat16),
            ],
            scratch_shapes=[
                full(wdq, q_rank), full(wdkv, kv_rank + LANES),
                full(wuq, first * q_cols), full(wuq, rest * q_cols),
                full(wukv, first * kv_cols), full(wukv, rest * kv_cols),
                pltpu.VMEM((n_fsdp, GAIN_ROWS, LANES), jnp.float32),
                pltpu.VMEM((1, n_gain), jnp.float32),
                pltpu.VMEM((n_p, seq_len, q_rank), jnp.bfloat16),
                pltpu.VMEM((n_p, seq_len, kv_rank), jnp.bfloat16),
                pltpu.VMEM((n_p, seq_len, LANES), jnp.bfloat16),
                pltpu.VMEM(wout.shape, jnp.bfloat16),
                pltpu.SemaphoreType.DMA((7, N_SEND)),
                pltpu.SemaphoreType.DMA((7, N_RECV)),
                pltpu.SemaphoreType.DMA((7,)),
                pltpu.SemaphoreType.DMA((7,)),
                pltpu.SemaphoreType.DMA((9,)),
            ],
            compiler_params=pltpu.CompilerParams(
                vmem_limit_bytes=VMEM_LIMIT, dimension_semantics=("arbitrary",), collective_id=0, has_side_effects=True,
            ),
            name="core",
        )(x, gs, *shards, cos, sin)
        rows = 512
        tile = lambda cols: pl.BlockSpec((rows, cols), lambda i: (i, 0))
        flat = lambda v: v.reshape(n_p * seq_len, v.shape[-1])
        flat_out = lambda cols: jax.ShapeDtypeStruct((n_p * seq_len, cols), jnp.bfloat16)
        y, c, r = pl.pallas_call(
            out_kernel,
            grid=(n_p * seq_len // rows,),
            in_specs=[tile(d_model), tile(oa.shape[-1]), tile(ob.shape[-1]), whole(wout_all.shape), tile(kv_rank), tile(ROPE)],
            out_specs=[tile(d_model), tile(kv_rank), tile(ROPE)],
            out_shape=[flat_out(d_model), flat_out(kv_rank), flat_out(ROPE)],
            compiler_params=pltpu.CompilerParams(vmem_limit_bytes=VMEM_LIMIT, dimension_semantics=("arbitrary",)),
            name="project",
        )(flat(x), flat(oa), flat(ob), wout_all, flat(c), flat(r))
        back = lambda v: v.reshape(n_p, seq_len, v.shape[-1])
        return back(y), back(c), back(r)

    batch, row, mat = P(('dp', 'fsdp')), P('fsdp'), P('fsdp', None)
    return jax.shard_map(
        local_block,
        mesh=mesh,
        in_specs=(batch, row, mat, row, mat, mat, row, mat, mat),
        out_specs=(batch, batch, batch),
        check_vma=False,
    )
```

```python
import functools

import jax
import jax.numpy as jnp
import numpy as np
from jax import lax
from jax.experimental import pallas as pl
from jax.experimental.pallas import tpu as pltpu
from jax.sharding import PartitionSpec as P

EPSILON = 1e-6
ROPE_THETA = 10000.0
LOG2E = 1.4426950408889634
VMEM_LIMIT = 64000 * 1024

NOPE, ROPE, VDIM = 64, 32, 64
HALF = ROPE // 2
GROUP = 8
PE_TILE = 4
LANES = 128


def rope_tiles(seq_len):
    inv_freq = ROPE_THETA ** (-2.0 * np.arange(HALF) / ROPE)
    angles = np.arange(seq_len)[:, None] * inv_freq[None, :]
    cos = np.tile(np.cos(angles), (1, LANES // HALF))
    sin = np.tile(np.sin(angles), (1, PE_TILE))
    return cos.astype(np.float32), np.concatenate([-sin, sin], axis=1).astype(np.float32)


def arrange_q(w):
    rows = w.shape[0]
    w = w.reshape(rows, -1, GROUP, NOPE + ROPE)
    nope = w[..., :NOPE].reshape(rows, -1, GROUP * NOPE)
    pe = w[..., NOPE:].reshape(rows, -1, GROUP // PE_TILE, PE_TILE, 2, HALF)
    pe = pe.transpose(0, 1, 2, 4, 3, 5).reshape(rows, -1, GROUP * ROPE)
    return jnp.concatenate([nope, pe], axis=-1).reshape(rows, -1)


def arrange_kv(w):
    rows = w.shape[0]
    return w.reshape(rows, -1, GROUP, 2, NOPE).transpose(0, 1, 3, 2, 4).reshape(rows, -1)


def arrange_dkv(w, kv_rank):
    lo, hi = w[:, kv_rank:kv_rank + HALF], w[:, kv_rank + HALF:]
    return jnp.concatenate([w[:, :kv_rank]] + [lo] * PE_TILE + [hi] * PE_TILE, axis=1)


def inv_rms(v):
    return lax.rsqrt(jnp.mean(v * v, axis=-1, keepdims=True) + EPSILON)


def rotate(tile, cos, sin):
    return tile * cos + pltpu.roll(tile, LANES // 2, 1) * sin


def attend_heads(q, kv, rt_slots, cos, sin, scale):
    seq_len = q.shape[0]
    half = seq_len // 2
    lane = lax.broadcasted_iota(jnp.int32, (1, LANES), 1)
    low = lane < NOPE
    diag = lax.broadcasted_iota(jnp.int32, (half, half), 0) >= lax.broadcasted_iota(jnp.int32, (half, half), 1)
    n_nope = GROUP * NOPE
    qn = q[:, :n_nope].astype(jnp.bfloat16)
    qp = [
        rotate(q[:, n_nope + t * LANES:n_nope + (t + 1) * LANES], cos, sin).astype(jnp.bfloat16)
        for t in range(GROUP // PE_TILE)
    ]
    kn = kv[:, :n_nope].astype(jnp.bfloat16)
    vv = kv[:, n_nope:].astype(jnp.bfloat16)
    zero = jnp.zeros((half, half), jnp.bfloat16)
    outs = []
    for quad in range(GROUP // 4):
        probs, vals = [], []
        for k in range(4):
            j = quad * 4 + k
            t, odd = j // 2, j % 2
            q_tile = jnp.concatenate([qn[:, t * LANES:(t + 1) * LANES], qp[j // PE_TILE]], axis=1)
            keep = low if odd == 0 else jnp.logical_not(low)
            k_tile = jnp.where(keep, kn[:, t * LANES:(t + 1) * LANES], 0)
            k_tile = jnp.concatenate([k_tile, rt_slots[j % PE_TILE]], axis=1)
            s = lax.dot_general(q_tile, k_tile, (((1,), (1,)), ((), ())), preferred_element_type=jnp.float32)
            s = s * scale
            top = jnp.where(diag, s[:half, :half], -1e30)
            left = s[half:, :half]
            right = jnp.where(diag, s[half:, half:], -1e30)
            m_top = jnp.max(top, axis=-1, keepdims=True)
            m_bot = jnp.max(jnp.maximum(left, right), axis=-1, keepdims=True)
            e_top = jnp.exp2(top - m_top)
            e_left = jnp.exp2(left - m_bot)
            e_right = jnp.exp2(right - m_bot)
            r_top = 1.0 / jnp.sum(e_top, axis=-1, keepdims=True)
            r_bot = 1.0 / jnp.sum(e_left + e_right, axis=-1, keepdims=True)
            p_top = jnp.concatenate([(e_top * r_top).astype(jnp.bfloat16), zero], axis=1)
            p_bot = jnp.concatenate([(e_left * r_bot).astype(jnp.bfloat16), (e_right * r_bot).astype(jnp.bfloat16)], axis=1)
            probs.append(jnp.concatenate([p_top, p_bot], axis=0))
            v_tile = jnp.where(keep, vv[:, t * LANES:(t + 1) * LANES], 0)
            blank = jnp.zeros_like(v_tile)
            vals.append(jnp.concatenate([v_tile, blank] if k < 2 else [blank, v_tile], axis=1))
        o = jnp.dot(
            jnp.concatenate(probs, axis=1), jnp.concatenate(vals, axis=0), preferred_element_type=jnp.float32
        )
        outs.append(o.astype(jnp.bfloat16))
    return jnp.concatenate(outs, axis=1)


def slot_masks(rt):
    lane = lax.broadcasted_iota(jnp.int32, (1, LANES), 1)
    slot = lax.rem(lane, LANES // 2) // HALF
    return [jnp.where(slot == j, rt, 0) for j in range(PE_TILE)]


MESH = pl.DeviceIdType.MESH
GROUPS_FIRST = 2
GAIN_ROWS = 32
N_SEND, N_RECV = 19, 19


class Item:
    def __init__(self, index, shard, col, cols, full):
        self.index, self.shard, self.col, self.cols, self.full = index, shard, col, cols, full
        self.rows = shard.shape[0]
        if (self.rows // 4) % 16 == 0:
            self.q_rows, self.q_cols = self.rows // 4, cols
        elif (cols // 4) % LANES == 0 and self.rows == 32:
            self.q_rows, self.q_cols = self.rows, cols // 4
        else:
            self.q_rows, self.q_cols = self.rows // 2, cols // 2
        if self.q_rows == self.rows:
            n = self.q_rows // 2
            self.halves = [(0, n, 0, self.q_cols), (n, n, 0, self.q_cols)]
        else:
            n = -(-self.q_cols // (2 * LANES)) * LANES
            self.halves = [(0, self.q_rows, 0, n), (0, self.q_rows, n, self.q_cols - n)]

    def quarter(self, q):
        per_row = self.cols // self.q_cols
        return (q // per_row) * self.q_rows, lax.rem(q, per_row) * self.q_cols

    def source(self, q):
        r, c = self.quarter(q)
        return self.shard.at[pl.ds(pl.multiple_of(r, 16), self.q_rows), pl.ds(pl.multiple_of(self.col + c, LANES), self.q_cols)]

    def own(self):
        return self.shard.at[:, pl.ds(self.col, self.cols)]

    def place(self, f, q=None, half=None):
        r, c = (0, 0) if q is None else self.quarter(q)
        r = f * self.rows + r
        if q is None:
            n_r, n_c = self.rows, self.cols
        elif half is None:
            n_r, n_c = self.q_rows, self.q_cols
        else:
            dr, n_r, dc, n_c = self.halves[half]
            r, c = r + dr, c + dc
        if n_c == self.cols:
            return self.full.at[pl.ds(pl.multiple_of(r, 16), n_r)]
        return self.full.at[pl.ds(pl.multiple_of(r, 16), n_r), pl.ds(pl.multiple_of(c, LANES), n_c)]


def core_kernel(
    n_prompts, x_ref, gs_ref, dq_s, dkv_s, uq_s, ukv_s, out_s, cos_ref, sin_ref,
    c_all, r_ref, oa_ref, ob_ref, wout_ref,
    wdq, wdkv, wuqa, wuqb, wukva, wukvb, gains, gvec, a_all, acc, cq_all, rt_all, stage,
    send_sem, recv_sem, g_send, g_recv, local_sem,
):
    i = pl.program_id(0)
    d, f = lax.axis_index('dp'), lax.axis_index('fsdp')
    z, core = f // 2, lax.rem(f, 2)
    dx = lax.rem(d + 2, 4)
    dy = d + 1 - 2 * lax.rem(d, 2)
    dd = lax.rem(dy + 2, 4)
    sib = z * 2 + 1 - core
    n_a = wuqa.shape[1]
    m_a = wukva.shape[1]
    dkv = Item(0, dkv_s, 0, wdkv.shape[1], wdkv)
    dq = Item(1, dq_s, 0, wdq.shape[1], wdq)
    ukva = Item(2, ukv_s, 0, m_a, wukva)
    uqa = Item(3, uq_s, 0, n_a, wuqa)
    ukvb = Item(4, ukv_s, m_a, wukvb.shape[1], wukvb)
    uqb = Item(5, uq_s, n_a, wuqb.shape[1], wuqb)
    wo = Item(6, out_s, 0, wout_ref.shape[1], wout_ref)
    items = [dkv, dq, ukva, uqa, ukvb, uqb, wo]
    down, first, rest, last = (dkv, dq), (ukva, uqa), (ukvb, uqb), (wo,)

    def to(k):
        return lax.rem(z + k, 4) * 2 + core

    def origin(k):
        return lax.rem(z + 4 - k, 4) * 2 + core

    def copy(it, src, dst, s, r, dev):
        return pltpu.make_async_remote_copy(
            src_ref=src, dst_ref=dst, send_sem=send_sem.at[it.index, s], recv_sem=recv_sem.at[it.index, r],
            device_id=dev, device_id_type=MESH,
        )

    def along_z(it, k):
        return copy(it, it.source(d), it.place(f, d), k - 1, k - 1, (d, to(k)))

    def to_x(it, k):
        ref = it.place(origin(k), d)
        return copy(it, ref, ref, 2 + k, 2 + k, (dx, f))

    def to_y(it, k):
        ref = it.place(origin(k), d)
        return copy(it, ref, ref, 5 + k, 5 + k, (dy, f))

    def diag_y(it, k):
        ref = it.place(origin(k), dx, 0)
        return copy(it, ref, ref, 8 + k, 8 + k, (dy, f))

    def diag_x(it, k):
        ref = it.place(origin(k), dy, 1)
        return copy(it, ref, ref, 11 + k, 11 + k, (dx, f))

    def to_core(it, k):
        ref = it.place(origin(k))
        return copy(it, ref, ref, 14 + k, 14 + k, (d, sib))

    def own_copy(it):
        return copy(it, it.own(), it.place(f), 18, 18, (d, sib))

    def arrived(it, ref, r):
        return copy(it, ref, ref, 0, r, (d, f)).wait_recv()

    def keep(it):
        return pltpu.make_async_copy(it.own(), stage if it is wo else it.place(f), local_sem.at[it.index])

    def keep_out():
        return pltpu.make_async_copy(stage, wo.place(f), local_sem.at[7])

    def gain_copy(j):
        return pltpu.make_async_remote_copy(
            src_ref=gs_ref, dst_ref=gains.at[f], send_sem=g_send.at[j - 1], recv_sem=g_recv.at[j - 1],
            device_id=(d, lax.rem(f + j, 8)), device_id_type=MESH,
        )

    def a2(its, *ks):
        for k in ks:
            for it in its:
                arrived(it, it.place(origin(k), d), k - 1)
                to_x(it, k).start()
                to_y(it, k).start()

    def a3(its, *ks):
        for k in ks:
            for it in its:
                arrived(it, it.place(origin(k), dx), 2 + k)
                diag_y(it, k).start()
                arrived(it, it.place(origin(k), dy), 5 + k)
                diag_x(it, k).start()

    def a4(its, *ks):
        for k in ks:
            for it in its:
                arrived(it, it.place(origin(k), dd, 0), 8 + k)
                arrived(it, it.place(origin(k), dd, 1), 11 + k)
                to_core(it, k).start()

    def a5(its, *ks):
        for k in ks:
            for it in its:
                arrived(it, it.place(lax.rem(z + 4 - k, 4) * 2 + 1 - core), 14 + k)

    def a5_own(its):
        for it in its:
            (keep_out() if it is wo else keep(it)).wait()
            arrived(it, it.place(sib), 18)

    def sent(it):
        for k in (1, 2, 3):
            for make in (along_z, to_x, to_y, diag_y, diag_x, to_core):
                make(it, k).wait_send()

    @pl.when(i == 0)
    def _():
        barrier = pltpu.get_barrier_semaphore()
        peers = [(dx, f), (dy, f)] + [(d, lax.rem(f + j, 8)) for j in range(1, 8)]
        for peer in peers:
            pl.semaphore_signal(barrier, inc=1, device_id=peer, device_id_type=MESH)
        pl.semaphore_wait(barrier, len(peers))
        for j in range(1, 8):
            gain_copy(j).start()
        g_own = pltpu.make_async_copy(gs_ref, gains.at[f], local_sem.at[8])
        g_own.start()
        for it in down:
            own_copy(it).start()
            keep(it).start()
        for group in (down, first, rest, last):
            for k in (1, 2, 3):
                for it in group:
                    along_z(it, k).start()
        for it in items[2:]:
            own_copy(it).start()
            keep(it).start()
        for j in range(1, 8):
            gain_copy(j).wait_recv()
        g_own.wait()
        total = jnp.sum(gains[...], axis=0)
        for t in range(gvec.shape[1] // LANES):
            gvec[:, t * LANES:(t + 1) * LANES] = total[t:t + 1, :]
        a5_own(down)

    d_model, q_rank, kv_rank = x_ref.shape[-1], cq_all.shape[-1], c_all.shape[-1]
    k_rows = d_model // 4
    s2 = n_prompts
    s3 = s2 + 4
    s4 = s3 + n_prompts
    end = s4 + n_prompts - 1

    plan = {
        3: lambda: a2(down, 1),
        5: lambda: a3(down, 1),
        7: lambda: (a2(down, 2), a4(down, 1)),
        s2: lambda: (a3(down, 2), a5(down, 1)),
        s2 + 1: lambda: (a2(down, 3), a4(down, 2), a5(down, 2)),
        s2 + 2: lambda: (a3(down, 3), a2(first, 1), a4(down, 3), a2(first, 2), a5(down, 3)),
        s2 + 3: lambda: (a2(first, 3), a3(first, 1)),
        s3: lambda: (
            a3(first, 2), a2(rest, 1), a3(first, 3), a4(first, 1), a2(rest, 2), a4(first, 2, 3), a5_own(first), a5(first, 1, 2, 3)
        ),
        s3 + 1: lambda: (a2(rest, 3), a3(rest, 1)),
        s3 + 2: lambda: (a3(rest, 2), a2(last, 1)),
        s3 + 3: lambda: (a3(rest, 3), a4(rest, 1)),
        s3 + 4: lambda: a4(rest, 2),
        s3 + 5: lambda: (a4(rest, 3), a2(last, 2), a3(last, 1)),
        s4: lambda: (a5_own(rest), a5(rest, 1, 2, 3), a2(last, 3), a3(last, 2)),
        s4 + 1: lambda: a4(last, 1),
        s4 + 2: lambda: (a3(last, 3), a4(last, 2)),
        s4 + 4: lambda: a4(last, 3),
    }
    for step, act in plan.items():
        @pl.when(i == step)
        def _(act=act):
            act()

    @pl.when(i == 1)
    def _():
        keep(wo).wait()
        keep_out().start()

    def partial_sums(p, k):
        row = lax.rem(z + 4 - k, 4) * k_rows
        rows = pl.ds(pl.multiple_of(row, LANES), k_rows)
        a = a_all[p, :, rows]
        qd = jnp.dot(a, wdq[rows], preferred_element_type=jnp.float32)
        kd = jnp.dot(a, wdkv[rows], preferred_element_type=jnp.float32)
        if k > 0:
            qd += acc[p, :, :q_rank]
            kd += acc[p, :, q_rank:]
        return qd, kd

    def add_plane(p, k):
        qd, kd = partial_sums(p, k)
        acc[p, :, :q_rank] = qd
        acc[p, :, q_rank:] = kd

    def finish(p):
        qd, kd = partial_sums(p, 3)
        cq_all[p] = (qd * inv_rms(qd) * gvec[:, d_model:d_model + q_rank]).astype(jnp.bfloat16)
        lat = kd[:, :kv_rank]
        c_all[p] = (lat * inv_rms(lat) * gvec[:, d_model + q_rank:]).astype(jnp.bfloat16)
        rt = rotate(kd[:, kv_rank:], cos_ref[...], sin_ref[...]).astype(jnp.bfloat16)
        rt_all[p] = rt
        r_ref[p] = jnp.concatenate([rt[:, :HALF], rt[:, LANES // 2:LANES // 2 + HALF]], axis=1)

    def each(first_p, n, fn):
        def body(p, carry):
            fn(p)
            return carry
        lax.fori_loop(first_p, first_p + n, body, 0)

    @pl.when(i < n_prompts)
    def _():
        x = x_ref[0].astype(jnp.float32)
        a_all[i] = (x * inv_rms(x) * gvec[:, :d_model]).astype(jnp.bfloat16)
        add_plane(i, 0)

    @pl.when(jnp.logical_and(i >= s2, i < s2 + 2))
    def _():
        @pl.when(i == s2)
        def _():
            each(0, n_prompts, lambda p: add_plane(p, 1))

        @pl.when(i == s2 + 1)
        def _():
            each(0, n_prompts, lambda p: add_plane(p, 2))

    @pl.when(jnp.logical_and(i >= s2 + 2, i < s3))
    def _():
        half = n_prompts // 2
        each((i - s2 - 2) * half, half, finish)

    q_cols, kv_cols, o_cols = GROUP * (NOPE + ROPE), GROUP * (NOPE + VDIM), GROUP * VDIM
    scale = (NOPE + ROPE) ** -0.5 * LOG2E

    def attend(p, wuq, wukv, o_ref):
        cq = cq_all[p]
        lat = c_all[p]
        slots = slot_masks(rt_all[p])

        def body(g, carry):
            wq = wuq[:, pl.ds(pl.multiple_of(g * q_cols, q_cols), q_cols)]
            wkv = wukv[:, pl.ds(pl.multiple_of(g * kv_cols, kv_cols), kv_cols)]
            q = jnp.dot(cq, wq, preferred_element_type=jnp.float32)
            kv = jnp.dot(lat, wkv, preferred_element_type=jnp.float32)
            o = attend_heads(q, kv, slots, cos_ref[...], sin_ref[...], scale)
            o_ref[0, :, pl.ds(pl.multiple_of(g * o_cols, o_cols), o_cols)] = o
            return carry

        lax.fori_loop(0, wuq.shape[1] // q_cols, body, 0)

    @pl.when(jnp.logical_and(i >= s3, i < s4))
    def _():
        attend(i - s3, wuqa, wukva, oa_ref)

    @pl.when(i >= s4)
    def _():
        attend(i - s4, wuqb, wukvb, ob_ref)

    @pl.when(i == end)
    def _():
        a5_own(last)
        a5(last, 1, 2, 3)
        for j in range(1, 8):
            gain_copy(j).wait_send()
        for it in items:
            sent(it)
            own_copy(it).wait_send()


def slot_masks(rt):
    lane = lax.broadcasted_iota(jnp.int32, (1, LANES), 1)
    slot = lax.rem(lane, LANES // 2) // HALF
    return [jnp.where(slot == j, rt, 0) for j in range(PE_TILE)]


def out_kernel(x_ref, oa_ref, ob_ref, w_ref, c_in, r_in, y_ref, c_out, r_out):
    step = 512
    oa, ob = oa_ref[...], ob_ref[...]
    n_a = oa.shape[1]
    c_out[...] = c_in[...]
    r_out[...] = r_in[...]
    for n in range(0, y_ref.shape[1], step):
        acc = jnp.dot(oa, w_ref[:n_a, n:n + step], preferred_element_type=jnp.float32)
        acc += jnp.dot(ob, w_ref[n_a:, n:n + step], preferred_element_type=jnp.float32)
        y_ref[:, n:n + step] = (x_ref[:, n:n + step].astype(jnp.float32) + acc).astype(jnp.bfloat16)


def whole(shape):
    return pl.BlockSpec(shape, lambda i: (0,) * len(shape))


def solution(mesh):
    n_fsdp = mesh.shape['fsdp']

    def local_block(x, g1, wdq, gq, wuq, wdkv, gkv, wukv, wout):
        n_p, seq_len, d_model = x.shape
        kv_rank, q_rank = gkv.shape[0] * n_fsdp, wdq.shape[1]
        cos_np, sin_np = rope_tiles(seq_len)
        cos, sin = jnp.asarray(cos_np), jnp.asarray(sin_np)
        me = lax.axis_index('fsdp')
        spread = [
            lax.dynamic_update_slice(jnp.zeros(g.shape[0] * n_fsdp, jnp.float32), g.astype(jnp.float32), (me * g.shape[0],))
            for g in (g1, gq, gkv)
        ]
        n_gain = d_model + q_rank + kv_rank
        gs = jnp.concatenate(spread + [jnp.zeros(GAIN_ROWS * LANES - n_gain, jnp.float32)]).reshape(GAIN_ROWS, LANES)
        shards = [wdq, arrange_dkv(wdkv, kv_rank), arrange_q(wuq), arrange_kv(wukv), wout]
        full = lambda w, cols: pltpu.VMEM((w.shape[0] * n_fsdp, cols), jnp.bfloat16)
        q_cols, kv_cols, o_cols = GROUP * (NOPE + ROPE), GROUP * (NOPE + VDIM), GROUP * VDIM
        n_groups = wuq.shape[1] // q_cols
        first, rest = GROUPS_FIRST, n_groups - GROUPS_FIRST
        last = n_p - 1
        blk = lambda cols, lag: pl.BlockSpec((1, seq_len, cols), lambda i: (jnp.clip(i - lag, 0, last), 0, 0))
        out = lambda cols: jax.ShapeDtypeStruct((n_p, seq_len, cols), jnp.bfloat16)
        hbm = pl.BlockSpec(memory_space=pl.ANY)
        c, r, oa, ob, wout_all = pl.pallas_call(
            functools.partial(core_kernel, n_p),
            grid=(3 * n_p + 4,),
            in_specs=[blk(d_model, 0)] + [hbm] * 6 + [whole(cos.shape)] * 2,
            out_specs=[
                whole((n_p, seq_len, kv_rank)), whole((n_p, seq_len, ROPE)),
                blk(first * o_cols, n_p + 4), blk(rest * o_cols, 2 * n_p + 4), hbm,
            ],
            out_shape=[
                out(kv_rank), out(ROPE), out(first * o_cols), out(rest * o_cols),
                jax.ShapeDtypeStruct((wout.shape[0] * n_fsdp, wout.shape[1]), jnp.bfloat16),
            ],
            scratch_shapes=[
                full(wdq, q_rank), full(wdkv, kv_rank + LANES),
                full(wuq, first * q_cols), full(wuq, rest * q_cols),
                full(wukv, first * kv_cols), full(wukv, rest * kv_cols),
                pltpu.VMEM((n_fsdp, GAIN_ROWS, LANES), jnp.float32),
                pltpu.VMEM((1, n_gain), jnp.float32),
                pltpu.VMEM((n_p, seq_len, d_model), jnp.bfloat16),
                pltpu.VMEM((n_p, seq_len, q_rank + kv_rank + LANES), jnp.float32),
                pltpu.VMEM((n_p, seq_len, q_rank), jnp.bfloat16),
                pltpu.VMEM((n_p, seq_len, LANES), jnp.bfloat16),
                pltpu.VMEM(wout.shape, jnp.bfloat16),
                pltpu.SemaphoreType.DMA((7, N_SEND)),
                pltpu.SemaphoreType.DMA((7, N_RECV)),
                pltpu.SemaphoreType.DMA((7,)),
                pltpu.SemaphoreType.DMA((7,)),
                pltpu.SemaphoreType.DMA((9,)),
            ],
            compiler_params=pltpu.CompilerParams(
                vmem_limit_bytes=VMEM_LIMIT, dimension_semantics=("arbitrary",), collective_id=0, has_side_effects=True,
            ),
            name="core",
        )(x, gs, *shards, cos, sin)
        rows = 512
        tile = lambda cols: pl.BlockSpec((rows, cols), lambda i: (i, 0))
        flat = lambda v: v.reshape(n_p * seq_len, v.shape[-1])
        flat_out = lambda cols: jax.ShapeDtypeStruct((n_p * seq_len, cols), jnp.bfloat16)
        y, c, r = pl.pallas_call(
            out_kernel,
            grid=(n_p * seq_len // rows,),
            in_specs=[tile(d_model), tile(oa.shape[-1]), tile(ob.shape[-1]), whole(wout_all.shape), tile(kv_rank), tile(ROPE)],
            out_specs=[tile(d_model), tile(kv_rank), tile(ROPE)],
            out_shape=[flat_out(d_model), flat_out(kv_rank), flat_out(ROPE)],
            compiler_params=pltpu.CompilerParams(vmem_limit_bytes=VMEM_LIMIT, dimension_semantics=("arbitrary",)),
            name="project",
        )(flat(x), flat(oa), flat(ob), wout_all, flat(c), flat(r))
        back = lambda v: v.reshape(n_p, seq_len, v.shape[-1])
        return back(y), back(c), back(r)

    batch, row, mat = P(('dp', 'fsdp')), P('fsdp'), P('fsdp', None)
    return jax.shard_map(
        local_block,
        mesh=mesh,
        in_specs=(batch, row, mat, row, mat, mat, row, mat, mat),
        out_specs=(batch, batch, batch),
        check_vma=False,
    )
```

```python
import functools

import jax
import jax.numpy as jnp
import numpy as np
from jax import lax
from jax.experimental import pallas as pl
from jax.experimental.pallas import tpu as pltpu
from jax.sharding import PartitionSpec as P

EPSILON = 1e-6
ROPE_THETA = 10000.0
LOG2E = 1.4426950408889634
VMEM_LIMIT = 64000 * 1024

NOPE, ROPE, VDIM = 64, 32, 64
HALF = ROPE // 2
GROUP = 8
PE_TILE = 4
LANES = 128


def rope_tiles(seq_len):
    inv_freq = ROPE_THETA ** (-2.0 * np.arange(HALF) / ROPE)
    angles = np.arange(seq_len)[:, None] * inv_freq[None, :]
    cos = np.tile(np.cos(angles), (1, LANES // HALF))
    sin = np.tile(np.sin(angles), (1, PE_TILE))
    return cos.astype(np.float32), np.concatenate([-sin, sin], axis=1).astype(np.float32)


def arrange_q(w):
    rows = w.shape[0]
    w = w.reshape(rows, -1, GROUP, NOPE + ROPE)
    nope = w[..., :NOPE].reshape(rows, -1, GROUP * NOPE)
    pe = w[..., NOPE:].reshape(rows, -1, GROUP // PE_TILE, PE_TILE, 2, HALF)
    pe = pe.transpose(0, 1, 2, 4, 3, 5).reshape(rows, -1, GROUP * ROPE)
    return jnp.concatenate([nope, pe], axis=-1).reshape(rows, -1)


def arrange_kv(w):
    rows = w.shape[0]
    return w.reshape(rows, -1, GROUP, 2, NOPE).transpose(0, 1, 3, 2, 4).reshape(rows, -1)


def arrange_dkv(w, kv_rank):
    lo, hi = w[:, kv_rank:kv_rank + HALF], w[:, kv_rank + HALF:]
    return jnp.concatenate([w[:, :kv_rank]] + [lo] * PE_TILE + [hi] * PE_TILE, axis=1)


def inv_rms(v):
    return lax.rsqrt(jnp.mean(v * v, axis=-1, keepdims=True) + EPSILON)


def rotate(tile, cos, sin):
    return tile * cos + pltpu.roll(tile, LANES // 2, 1) * sin


def attend_heads(q, kv, rt_slots, cos, sin, scale):
    seq_len = q.shape[0]
    half = seq_len // 2
    lane = lax.broadcasted_iota(jnp.int32, (1, LANES), 1)
    low = lane < NOPE
    diag = lax.broadcasted_iota(jnp.int32, (half, half), 0) >= lax.broadcasted_iota(jnp.int32, (half, half), 1)
    n_nope = GROUP * NOPE
    qn = q[:, :n_nope].astype(jnp.bfloat16)
    qp = [
        rotate(q[:, n_nope + t * LANES:n_nope + (t + 1) * LANES], cos, sin).astype(jnp.bfloat16)
        for t in range(GROUP // PE_TILE)
    ]
    kn = kv[:, :n_nope].astype(jnp.bfloat16)
    vv = kv[:, n_nope:].astype(jnp.bfloat16)
    zero = jnp.zeros((half, half), jnp.bfloat16)
    outs = []
    for quad in range(GROUP // 4):
        probs, vals = [], []
        for k in range(4):
            j = quad * 4 + k
            t, odd = j // 2, j % 2
            q_tile = jnp.concatenate([qn[:, t * LANES:(t + 1) * LANES], qp[j // PE_TILE]], axis=1)
            keep = low if odd == 0 else jnp.logical_not(low)
            k_tile = jnp.where(keep, kn[:, t * LANES:(t + 1) * LANES], 0)
            k_tile = jnp.concatenate([k_tile, rt_slots[j % PE_TILE]], axis=1)
            s = lax.dot_general(q_tile, k_tile, (((1,), (1,)), ((), ())), preferred_element_type=jnp.float32)
            s = s * scale
            top = jnp.where(diag, s[:half, :half], -1e30)
            left = s[half:, :half]
            right = jnp.where(diag, s[half:, half:], -1e30)
            m_top = jnp.max(top, axis=-1, keepdims=True)
            m_bot = jnp.max(jnp.maximum(left, right), axis=-1, keepdims=True)
            e_top = jnp.exp2(top - m_top)
            e_left = jnp.exp2(left - m_bot)
            e_right = jnp.exp2(right - m_bot)
            r_top = 1.0 / jnp.sum(e_top, axis=-1, keepdims=True)
            r_bot = 1.0 / jnp.sum(e_left + e_right, axis=-1, keepdims=True)
            p_top = jnp.concatenate([(e_top * r_top).astype(jnp.bfloat16), zero], axis=1)
            p_bot = jnp.concatenate([(e_left * r_bot).astype(jnp.bfloat16), (e_right * r_bot).astype(jnp.bfloat16)], axis=1)
            probs.append(jnp.concatenate([p_top, p_bot], axis=0))
            v_tile = jnp.where(keep, vv[:, t * LANES:(t + 1) * LANES], 0)
            blank = jnp.zeros_like(v_tile)
            vals.append(jnp.concatenate([v_tile, blank] if k < 2 else [blank, v_tile], axis=1))
        o = jnp.dot(
            jnp.concatenate(probs, axis=1), jnp.concatenate(vals, axis=0), preferred_element_type=jnp.float32
        )
        outs.append(o.astype(jnp.bfloat16))
    return jnp.concatenate(outs, axis=1)


def slot_masks(rt):
    lane = lax.broadcasted_iota(jnp.int32, (1, LANES), 1)
    slot = lax.rem(lane, LANES // 2) // HALF
    return [jnp.where(slot == j, rt, 0) for j in range(PE_TILE)]


MESH = pl.DeviceIdType.MESH
GROUPS_FIRST = 2
GAIN_ROWS = 32
N_SEND, N_RECV = 19, 19


class Item:
    def __init__(self, index, shard, col, cols, full):
        self.index, self.shard, self.col, self.cols, self.full = index, shard, col, cols, full
        self.rows = shard.shape[0]
        if (self.rows // 4) % 16 == 0:
            self.q_rows, self.q_cols = self.rows // 4, cols
        elif (cols // 4) % LANES == 0 and self.rows == 32:
            self.q_rows, self.q_cols = self.rows, cols // 4
        else:
            self.q_rows, self.q_cols = self.rows // 2, cols // 2
        if self.q_rows == self.rows:
            n = self.q_rows // 2
            self.halves = [(0, n, 0, self.q_cols), (n, n, 0, self.q_cols)]
        else:
            n = -(-self.q_cols // (2 * LANES)) * LANES
            self.halves = [(0, self.q_rows, 0, n), (0, self.q_rows, n, self.q_cols - n)]

    def quarter(self, q):
        per_row = self.cols // self.q_cols
        return (q // per_row) * self.q_rows, lax.rem(q, per_row) * self.q_cols

    def source(self, q):
        r, c = self.quarter(q)
        return self.shard.at[pl.ds(pl.multiple_of(r, 16), self.q_rows), pl.ds(pl.multiple_of(self.col + c, LANES), self.q_cols)]

    def own(self):
        return self.shard.at[:, pl.ds(self.col, self.cols)]

    def place(self, f, q=None, half=None):
        r, c = (0, 0) if q is None else self.quarter(q)
        r = f * self.rows + r
        if q is None:
            n_r, n_c = self.rows, self.cols
        elif half is None:
            n_r, n_c = self.q_rows, self.q_cols
        else:
            dr, n_r, dc, n_c = self.halves[half]
            r, c = r + dr, c + dc
        if n_c == self.cols:
            return self.full.at[pl.ds(pl.multiple_of(r, 16), n_r)]
        return self.full.at[pl.ds(pl.multiple_of(r, 16), n_r), pl.ds(pl.multiple_of(c, LANES), n_c)]


def core_kernel(
    n_prompts, x_ref, gs_ref, dq_s, dkv_s, uq_s, ukv_s, out_s, cos_ref, sin_ref,
    c_all, r_ref, oa_ref, ob_ref, wout_ref,
    wdq, wdkv, wuqa, wuqb, wukva, wukvb, gains, gvec, a_all, acc, cq_all, rt_all, stage,
    send_sem, recv_sem, g_send, g_recv, local_sem,
):
    i = pl.program_id(0)
    d, f = lax.axis_index('dp'), lax.axis_index('fsdp')
    z, core = f // 2, lax.rem(f, 2)
    dx = lax.rem(d + 2, 4)
    dy = d + 1 - 2 * lax.rem(d, 2)
    dd = lax.rem(dy + 2, 4)
    sib = z * 2 + 1 - core
    n_a = wuqa.shape[1]
    m_a = wukva.shape[1]
    dkv = Item(0, dkv_s, 0, wdkv.shape[1], wdkv)
    dq = Item(1, dq_s, 0, wdq.shape[1], wdq)
    ukva = Item(2, ukv_s, 0, m_a, wukva)
    uqa = Item(3, uq_s, 0, n_a, wuqa)
    ukvb = Item(4, ukv_s, m_a, wukvb.shape[1], wukvb)
    uqb = Item(5, uq_s, n_a, wuqb.shape[1], wuqb)
    wo = Item(6, out_s, 0, wout_ref.shape[1], wout_ref)
    items = [dkv, dq, ukva, uqa, ukvb, uqb, wo]
    down, first, rest, last = (dkv, dq), (ukva, uqa), (ukvb, uqb), (wo,)

    def to(k):
        return lax.rem(z + k, 4) * 2 + core

    def origin(k):
        return lax.rem(z + 4 - k, 4) * 2 + core

    def copy(it, src, dst, s, r, dev):
        return pltpu.make_async_remote_copy(
            src_ref=src, dst_ref=dst, send_sem=send_sem.at[it.index, s], recv_sem=recv_sem.at[it.index, r],
            device_id=dev, device_id_type=MESH,
        )

    def along_z(it, k):
        return copy(it, it.source(d), it.place(f, d), k - 1, k - 1, (d, to(k)))

    def to_x(it, k):
        ref = it.place(origin(k), d)
        return copy(it, ref, ref, 2 + k, 2 + k, (dx, f))

    def to_y(it, k):
        ref = it.place(origin(k), d)
        return copy(it, ref, ref, 5 + k, 5 + k, (dy, f))

    def diag_y(it, k):
        ref = it.place(origin(k), dx, 0)
        return copy(it, ref, ref, 8 + k, 8 + k, (dy, f))

    def diag_x(it, k):
        ref = it.place(origin(k), dy, 1)
        return copy(it, ref, ref, 11 + k, 11 + k, (dx, f))

    def to_core(it, k):
        ref = it.place(origin(k))
        return copy(it, ref, ref, 14 + k, 14 + k, (d, sib))

    def own_copy(it):
        return copy(it, it.own(), it.place(f), 18, 18, (d, sib))

    def arrived(it, ref, r):
        return copy(it, ref, ref, 0, r, (d, f)).wait_recv()

    def keep(it):
        return pltpu.make_async_copy(it.own(), stage if it is wo else it.place(f), local_sem.at[it.index])

    def keep_out():
        return pltpu.make_async_copy(stage, wo.place(f), local_sem.at[7])

    def gain_copy(j):
        return pltpu.make_async_remote_copy(
            src_ref=gs_ref, dst_ref=gains.at[f], send_sem=g_send.at[j - 1], recv_sem=g_recv.at[j - 1],
            device_id=(d, lax.rem(f + j, 8)), device_id_type=MESH,
        )

    def send_z(its, *ks):
        for k in ks:
            for it in its:
                along_z(it, k).start()

    def a2(its, *ks):
        for k in ks:
            for it in its:
                arrived(it, it.place(origin(k), d), k - 1)
                to_x(it, k).start()
                to_y(it, k).start()

    def a3(its, *ks):
        for k in ks:
            for it in its:
                arrived(it, it.place(origin(k), dx), 2 + k)
                diag_y(it, k).start()
                arrived(it, it.place(origin(k), dy), 5 + k)
                diag_x(it, k).start()

    def a4(its, *ks):
        for k in ks:
            for it in its:
                arrived(it, it.place(origin(k), dd, 0), 8 + k)
                arrived(it, it.place(origin(k), dd, 1), 11 + k)
                to_core(it, k).start()

    def a5(its, *ks):
        for k in ks:
            for it in its:
                arrived(it, it.place(lax.rem(z + 4 - k, 4) * 2 + 1 - core), 14 + k)

    def a5_own(its):
        for it in its:
            (keep_out() if it is wo else keep(it)).wait()
            arrived(it, it.place(sib), 18)

    def sent(it):
        for k in (1, 2, 3):
            for make in (along_z, to_x, to_y, diag_y, diag_x, to_core):
                make(it, k).wait_send()

    @pl.when(i == 0)
    def _():
        barrier = pltpu.get_barrier_semaphore()
        peers = [(dx, f), (dy, f)] + [(d, lax.rem(f + j, 8)) for j in range(1, 8)]
        for peer in peers:
            pl.semaphore_signal(barrier, inc=1, device_id=peer, device_id_type=MESH)
        pl.semaphore_wait(barrier, len(peers))
        for j in range(1, 8):
            gain_copy(j).start()
        g_own = pltpu.make_async_copy(gs_ref, gains.at[f], local_sem.at[8])
        g_own.start()
        for it in down:
            own_copy(it).start()
            keep(it).start()
        send_z(down, 1, 2, 3)
        for it in items[2:]:
            own_copy(it).start()
            keep(it).start()
        for j in range(1, 8):
            gain_copy(j).wait_recv()
        g_own.wait()
        total = jnp.sum(gains[...], axis=0)
        for t in range(gvec.shape[1] // LANES):
            gvec[:, t * LANES:(t + 1) * LANES] = total[t:t + 1, :]
        a5_own(down)

    d_model, q_rank, kv_rank = x_ref.shape[-1], cq_all.shape[-1], c_all.shape[-1]
    k_rows = d_model // 4
    s2 = n_prompts
    s3 = s2 + 4
    s4 = s3 + n_prompts
    end = s4 + n_prompts - 1

    plan = {
        3: lambda: (a2(down, 1), send_z(first, 1)),
        5: lambda: a3(down, 1),
        7: lambda: (a2(down, 2), send_z(first, 2, 3), a4(down, 1)),
        s2: lambda: (a3(down, 2), a5(down, 1)),
        s2 + 1: lambda: (a2(down, 3), send_z(rest, 1), a4(down, 2), a5(down, 2)),
        s2 + 2: lambda: (a3(down, 3), a2(first, 1), send_z(rest, 2), a4(down, 3), a2(first, 2), send_z(rest, 3), a5(down, 3)),
        s2 + 3: lambda: (a2(first, 3), send_z(last, 1), a3(first, 1)),
        s3: lambda: (
            a3(first, 2), a2(rest, 1), a3(first, 3), a4(first, 1), a2(rest, 2), a4(first, 2, 3), a5_own(first), a5(first, 1, 2, 3)
        ),
        s3 + 1: lambda: (a2(rest, 3), send_z(last, 2), a3(rest, 1)),
        s3 + 2: lambda: (a3(rest, 2), a2(last, 1), send_z(last, 3)),
        s3 + 3: lambda: (a3(rest, 3), a4(rest, 1)),
        s3 + 4: lambda: a4(rest, 2),
        s3 + 5: lambda: (a4(rest, 3), a2(last, 2), a3(last, 1)),
        s4: lambda: (a5_own(rest), a5(rest, 1, 2, 3), a2(last, 3), a3(last, 2)),
        s4 + 1: lambda: a4(last, 1),
        s4 + 2: lambda: (a3(last, 3), a4(last, 2)),
        s4 + 4: lambda: a4(last, 3),
    }
    for step, act in plan.items():
        @pl.when(i == step)
        def _(act=act):
            act()

    @pl.when(i == 1)
    def _():
        keep(wo).wait()
        keep_out().start()

    def partial_sums(p, k):
        row = lax.rem(z + 4 - k, 4) * k_rows
        rows = pl.ds(pl.multiple_of(row, LANES), k_rows)
        a = a_all[p, :, rows]
        qd = jnp.dot(a, wdq[rows], preferred_element_type=jnp.float32)
        kd = jnp.dot(a, wdkv[rows], preferred_element_type=jnp.float32)
        if k > 0:
            qd += acc[p, :, :q_rank]
            kd += acc[p, :, q_rank:]
        return qd, kd

    def add_plane(p, k):
        qd, kd = partial_sums(p, k)
        acc[p, :, :q_rank] = qd
        acc[p, :, q_rank:] = kd

    def finish(p):
        qd, kd = partial_sums(p, 3)
        cq_all[p] = (qd * inv_rms(qd) * gvec[:, d_model:d_model + q_rank]).astype(jnp.bfloat16)
        lat = kd[:, :kv_rank]
        c_all[p] = (lat * inv_rms(lat) * gvec[:, d_model + q_rank:]).astype(jnp.bfloat16)
        rt = rotate(kd[:, kv_rank:], cos_ref[...], sin_ref[...]).astype(jnp.bfloat16)
        rt_all[p] = rt
        r_ref[p] = jnp.concatenate([rt[:, :HALF], rt[:, LANES // 2:LANES // 2 + HALF]], axis=1)

    def each(first_p, n, fn):
        def body(p, carry):
            fn(p)
            return carry
        lax.fori_loop(first_p, first_p + n, body, 0)

    @pl.when(i < n_prompts)
    def _():
        x = x_ref[0].astype(jnp.float32)
        a_all[i] = (x * inv_rms(x) * gvec[:, :d_model]).astype(jnp.bfloat16)
        add_plane(i, 0)

    @pl.when(jnp.logical_and(i >= s2, i < s2 + 2))
    def _():
        @pl.when(i == s2)
        def _():
            each(0, n_prompts, lambda p: add_plane(p, 1))

        @pl.when(i == s2 + 1)
        def _():
            each(0, n_prompts, lambda p: add_plane(p, 2))

    @pl.when(jnp.logical_and(i >= s2 + 2, i < s3))
    def _():
        half = n_prompts // 2
        each((i - s2 - 2) * half, half, finish)

    q_cols, kv_cols, o_cols = GROUP * (NOPE + ROPE), GROUP * (NOPE + VDIM), GROUP * VDIM
    scale = (NOPE + ROPE) ** -0.5 * LOG2E

    def attend(p, wuq, wukv, o_ref):
        cq = cq_all[p]
        lat = c_all[p]
        slots = slot_masks(rt_all[p])

        def body(g, carry):
            wq = wuq[:, pl.ds(pl.multiple_of(g * q_cols, q_cols), q_cols)]
            wkv = wukv[:, pl.ds(pl.multiple_of(g * kv_cols, kv_cols), kv_cols)]
            q = jnp.dot(cq, wq, preferred_element_type=jnp.float32)
            kv = jnp.dot(lat, wkv, preferred_element_type=jnp.float32)
            o = attend_heads(q, kv, slots, cos_ref[...], sin_ref[...], scale)
            o_ref[0, :, pl.ds(pl.multiple_of(g * o_cols, o_cols), o_cols)] = o
            return carry

        lax.fori_loop(0, wuq.shape[1] // q_cols, body, 0)

    @pl.when(jnp.logical_and(i >= s3, i < s4))
    def _():
        attend(i - s3, wuqa, wukva, oa_ref)

    @pl.when(i >= s4)
    def _():
        attend(i - s4, wuqb, wukvb, ob_ref)

    @pl.when(i == end)
    def _():
        a5_own(last)
        a5(last, 1, 2, 3)
        for j in range(1, 8):
            gain_copy(j).wait_send()
        for it in items:
            sent(it)
            own_copy(it).wait_send()


def slot_masks(rt):
    lane = lax.broadcasted_iota(jnp.int32, (1, LANES), 1)
    slot = lax.rem(lane, LANES // 2) // HALF
    return [jnp.where(slot == j, rt, 0) for j in range(PE_TILE)]


def out_kernel(x_ref, oa_ref, ob_ref, w_ref, c_in, r_in, y_ref, c_out, r_out):
    step = 512
    oa, ob = oa_ref[...], ob_ref[...]
    n_a = oa.shape[1]
    c_out[...] = c_in[...]
    r_out[...] = r_in[...]
    for n in range(0, y_ref.shape[1], step):
        acc = jnp.dot(oa, w_ref[:n_a, n:n + step], preferred_element_type=jnp.float32)
        acc += jnp.dot(ob, w_ref[n_a:, n:n + step], preferred_element_type=jnp.float32)
        y_ref[:, n:n + step] = (x_ref[:, n:n + step].astype(jnp.float32) + acc).astype(jnp.bfloat16)


def whole(shape):
    return pl.BlockSpec(shape, lambda i: (0,) * len(shape))


def solution(mesh):
    n_fsdp = mesh.shape['fsdp']

    def local_block(x, g1, wdq, gq, wuq, wdkv, gkv, wukv, wout):
        n_p, seq_len, d_model = x.shape
        kv_rank, q_rank = gkv.shape[0] * n_fsdp, wdq.shape[1]
        cos_np, sin_np = rope_tiles(seq_len)
        cos, sin = jnp.asarray(cos_np), jnp.asarray(sin_np)
        me = lax.axis_index('fsdp')
        spread = [
            lax.dynamic_update_slice(jnp.zeros(g.shape[0] * n_fsdp, jnp.float32), g.astype(jnp.float32), (me * g.shape[0],))
            for g in (g1, gq, gkv)
        ]
        n_gain = d_model + q_rank + kv_rank
        gs = jnp.concatenate(spread + [jnp.zeros(GAIN_ROWS * LANES - n_gain, jnp.float32)]).reshape(GAIN_ROWS, LANES)
        shards = [wdq, arrange_dkv(wdkv, kv_rank), arrange_q(wuq), arrange_kv(wukv), wout]
        full = lambda w, cols: pltpu.VMEM((w.shape[0] * n_fsdp, cols), jnp.bfloat16)
        q_cols, kv_cols, o_cols = GROUP * (NOPE + ROPE), GROUP * (NOPE + VDIM), GROUP * VDIM
        n_groups = wuq.shape[1] // q_cols
        first, rest = GROUPS_FIRST, n_groups - GROUPS_FIRST
        last = n_p - 1
        blk = lambda cols, lag: pl.BlockSpec((1, seq_len, cols), lambda i: (jnp.clip(i - lag, 0, last), 0, 0))
        out = lambda cols: jax.ShapeDtypeStruct((n_p, seq_len, cols), jnp.bfloat16)
        hbm = pl.BlockSpec(memory_space=pl.ANY)
        c, r, oa, ob, wout_all = pl.pallas_call(
            functools.partial(core_kernel, n_p),
            grid=(3 * n_p + 4,),
            in_specs=[blk(d_model, 0)] + [hbm] * 6 + [whole(cos.shape)] * 2,
            out_specs=[
                whole((n_p, seq_len, kv_rank)), whole((n_p, seq_len, ROPE)),
                blk(first * o_cols, n_p + 4), blk(rest * o_cols, 2 * n_p + 4), hbm,
            ],
            out_shape=[
                out(kv_rank), out(ROPE), out(first * o_cols), out(rest * o_cols),
                jax.ShapeDtypeStruct((wout.shape[0] * n_fsdp, wout.shape[1]), jnp.bfloat16),
            ],
            scratch_shapes=[
                full(wdq, q_rank), full(wdkv, kv_rank + LANES),
                full(wuq, first * q_cols), full(wuq, rest * q_cols),
                full(wukv, first * kv_cols), full(wukv, rest * kv_cols),
                pltpu.VMEM((n_fsdp, GAIN_ROWS, LANES), jnp.float32),
                pltpu.VMEM((1, n_gain), jnp.float32),
                pltpu.VMEM((n_p, seq_len, d_model), jnp.bfloat16),
                pltpu.VMEM((n_p, seq_len, q_rank + kv_rank + LANES), jnp.float32),
                pltpu.VMEM((n_p, seq_len, q_rank), jnp.bfloat16),
                pltpu.VMEM((n_p, seq_len, LANES), jnp.bfloat16),
                pltpu.VMEM(wout.shape, jnp.bfloat16),
                pltpu.SemaphoreType.DMA((7, N_SEND)),
                pltpu.SemaphoreType.DMA((7, N_RECV)),
                pltpu.SemaphoreType.DMA((7,)),
                pltpu.SemaphoreType.DMA((7,)),
                pltpu.SemaphoreType.DMA((9,)),
            ],
            compiler_params=pltpu.CompilerParams(
                vmem_limit_bytes=VMEM_LIMIT, dimension_semantics=("arbitrary",), collective_id=0, has_side_effects=True,
            ),
            name="core",
        )(x, gs, *shards, cos, sin)
        rows = 512
        tile = lambda cols: pl.BlockSpec((rows, cols), lambda i: (i, 0))
        flat = lambda v: v.reshape(n_p * seq_len, v.shape[-1])
        flat_out = lambda cols: jax.ShapeDtypeStruct((n_p * seq_len, cols), jnp.bfloat16)
        y, c, r = pl.pallas_call(
            out_kernel,
            grid=(n_p * seq_len // rows,),
            in_specs=[tile(d_model), tile(oa.shape[-1]), tile(ob.shape[-1]), whole(wout_all.shape), tile(kv_rank), tile(ROPE)],
            out_specs=[tile(d_model), tile(kv_rank), tile(ROPE)],
            out_shape=[flat_out(d_model), flat_out(kv_rank), flat_out(ROPE)],
            compiler_params=pltpu.CompilerParams(vmem_limit_bytes=VMEM_LIMIT, dimension_semantics=("arbitrary",)),
            name="project",
        )(flat(x), flat(oa), flat(ob), wout_all, flat(c), flat(r))
        back = lambda v: v.reshape(n_p, seq_len, v.shape[-1])
        return back(y), back(c), back(r)

    batch, row, mat = P(('dp', 'fsdp')), P('fsdp'), P('fsdp', None)
    return jax.shard_map(
        local_block,
        mesh=mesh,
        in_specs=(batch, row, mat, row, mat, mat, row, mat, mat),
        out_specs=(batch, batch, batch),
        check_vma=False,
    )
```

```python
import functools

import jax
import jax.numpy as jnp
import numpy as np
from jax import lax
from jax.experimental import pallas as pl
from jax.experimental.pallas import tpu as pltpu
from jax.sharding import PartitionSpec as P

EPSILON = 1e-6
ROPE_THETA = 10000.0
LOG2E = 1.4426950408889634
VMEM_LIMIT = 64000 * 1024

NOPE, ROPE, VDIM = 64, 32, 64
HALF = ROPE // 2
GROUP = 8
PE_TILE = 4
LANES = 128


def rope_tiles(seq_len):
    inv_freq = ROPE_THETA ** (-2.0 * np.arange(HALF) / ROPE)
    angles = np.arange(seq_len)[:, None] * inv_freq[None, :]
    cos = np.tile(np.cos(angles), (1, LANES // HALF))
    sin = np.tile(np.sin(angles), (1, PE_TILE))
    return cos.astype(np.float32), np.concatenate([-sin, sin], axis=1).astype(np.float32)


def arrange_q(w):
    rows = w.shape[0]
    w = w.reshape(rows, -1, GROUP, NOPE + ROPE)
    nope = w[..., :NOPE].reshape(rows, -1, GROUP * NOPE)
    pe = w[..., NOPE:].reshape(rows, -1, GROUP // PE_TILE, PE_TILE, 2, HALF)
    pe = pe.transpose(0, 1, 2, 4, 3, 5).reshape(rows, -1, GROUP * ROPE)
    return jnp.concatenate([nope, pe], axis=-1).reshape(rows, -1)


def arrange_kv(w):
    rows = w.shape[0]
    return w.reshape(rows, -1, GROUP, 2, NOPE).transpose(0, 1, 3, 2, 4).reshape(rows, -1)


def arrange_dkv(w, kv_rank):
    lo, hi = w[:, kv_rank:kv_rank + HALF], w[:, kv_rank + HALF:]
    return jnp.concatenate([w[:, :kv_rank]] + [lo] * PE_TILE + [hi] * PE_TILE, axis=1)


def inv_rms(v):
    return lax.rsqrt(jnp.mean(v * v, axis=-1, keepdims=True) + EPSILON)


def rotate(tile, cos, sin):
    return tile * cos + pltpu.roll(tile, LANES // 2, 1) * sin


def attend_heads(q, kv, rt_slots, cos, sin, scale):
    seq_len = q.shape[0]
    half = seq_len // 2
    lane = lax.broadcasted_iota(jnp.int32, (1, LANES), 1)
    low = lane < NOPE
    diag = lax.broadcasted_iota(jnp.int32, (half, half), 0) >= lax.broadcasted_iota(jnp.int32, (half, half), 1)
    n_nope = GROUP * NOPE
    qn = q[:, :n_nope].astype(jnp.bfloat16)
    qp = [
        rotate(q[:, n_nope + t * LANES:n_nope + (t + 1) * LANES], cos, sin).astype(jnp.bfloat16)
        for t in range(GROUP // PE_TILE)
    ]
    kn = kv[:, :n_nope].astype(jnp.bfloat16)
    vv = kv[:, n_nope:].astype(jnp.bfloat16)
    zero = jnp.zeros((half, half), jnp.bfloat16)
    outs = []
    for quad in range(GROUP // 4):
        probs, vals = [], []
        for k in range(4):
            j = quad * 4 + k
            t, odd = j // 2, j % 2
            q_tile = jnp.concatenate([qn[:, t * LANES:(t + 1) * LANES], qp[j // PE_TILE]], axis=1)
            keep = low if odd == 0 else jnp.logical_not(low)
            k_tile = jnp.where(keep, kn[:, t * LANES:(t + 1) * LANES], 0)
            k_tile = jnp.concatenate([k_tile, rt_slots[j % PE_TILE]], axis=1)
            s = lax.dot_general(q_tile, k_tile, (((1,), (1,)), ((), ())), preferred_element_type=jnp.float32)
            s = s * scale
            top = jnp.where(diag, s[:half, :half], -1e30)
            left = s[half:, :half]
            right = jnp.where(diag, s[half:, half:], -1e30)
            m_top = jnp.max(top, axis=-1, keepdims=True)
            m_bot = jnp.max(jnp.maximum(left, right), axis=-1, keepdims=True)
            e_top = jnp.exp2(top - m_top)
            e_left = jnp.exp2(left - m_bot)
            e_right = jnp.exp2(right - m_bot)
            r_top = 1.0 / jnp.sum(e_top, axis=-1, keepdims=True)
            r_bot = 1.0 / jnp.sum(e_left + e_right, axis=-1, keepdims=True)
            p_top = jnp.concatenate([(e_top * r_top).astype(jnp.bfloat16), zero], axis=1)
            p_bot = jnp.concatenate([(e_left * r_bot).astype(jnp.bfloat16), (e_right * r_bot).astype(jnp.bfloat16)], axis=1)
            probs.append(jnp.concatenate([p_top, p_bot], axis=0))
            v_tile = jnp.where(keep, vv[:, t * LANES:(t + 1) * LANES], 0)
            blank = jnp.zeros_like(v_tile)
            vals.append(jnp.concatenate([v_tile, blank] if k < 2 else [blank, v_tile], axis=1))
        o = jnp.dot(
            jnp.concatenate(probs, axis=1), jnp.concatenate(vals, axis=0), preferred_element_type=jnp.float32
        )
        outs.append(o.astype(jnp.bfloat16))
    return jnp.concatenate(outs, axis=1)


def slot_masks(rt):
    lane = lax.broadcasted_iota(jnp.int32, (1, LANES), 1)
    slot = lax.rem(lane, LANES // 2) // HALF
    return [jnp.where(slot == j, rt, 0) for j in range(PE_TILE)]


MESH = pl.DeviceIdType.MESH
GAIN_ROWS = 32
N_SEND, N_RECV = 19, 19


class Item:
    def __init__(self, index, shard, col, cols, full):
        self.index, self.shard, self.col, self.cols, self.full = index, shard, col, cols, full
        self.rows = shard.shape[0]
        if (self.rows // 4) % 16 == 0:
            self.q_rows, self.q_cols = self.rows // 4, cols
        elif (cols // 4) % LANES == 0 and self.rows == 32:
            self.q_rows, self.q_cols = self.rows, cols // 4
        else:
            self.q_rows, self.q_cols = self.rows // 2, cols // 2
        if self.q_rows == self.rows:
            n = self.q_rows // 2
            self.halves = [(0, n, 0, self.q_cols), (n, n, 0, self.q_cols)]
        else:
            n = -(-self.q_cols // (2 * LANES)) * LANES
            self.halves = [(0, self.q_rows, 0, n), (0, self.q_rows, n, self.q_cols - n)]

    def quarter(self, q):
        per_row = self.cols // self.q_cols
        return (q // per_row) * self.q_rows, lax.rem(q, per_row) * self.q_cols

    def source(self, q):
        r, c = self.quarter(q)
        return self.shard.at[pl.ds(pl.multiple_of(r, 16), self.q_rows), pl.ds(pl.multiple_of(self.col + c, LANES), self.q_cols)]

    def own(self):
        return self.shard.at[:, pl.ds(self.col, self.cols)]

    def place(self, f, q=None, half=None):
        r, c = (0, 0) if q is None else self.quarter(q)
        r = f * self.rows + r
        if q is None:
            n_r, n_c = self.rows, self.cols
        elif half is None:
            n_r, n_c = self.q_rows, self.q_cols
        else:
            dr, n_r, dc, n_c = self.halves[half]
            r, c = r + dr, c + dc
        if n_c == self.cols:
            return self.full.at[pl.ds(pl.multiple_of(r, 16), n_r)]
        return self.full.at[pl.ds(pl.multiple_of(r, 16), n_r), pl.ds(pl.multiple_of(c, LANES), n_c)]


class Net:
    def __init__(self, send_sem, recv_sem):
        self.send_sem, self.recv_sem = send_sem, recv_sem
        self.d, self.f = lax.axis_index('dp'), lax.axis_index('fsdp')
        self.z, self.core = self.f // 2, lax.rem(self.f, 2)
        self.dx = lax.rem(self.d + 2, 4)
        self.dy = self.d + 1 - 2 * lax.rem(self.d, 2)
        self.dd = lax.rem(self.dy + 2, 4)
        self.sib = self.z * 2 + 1 - self.core

    def to(self, k):
        return lax.rem(self.z + k, 4) * 2 + self.core

    def plane(self, k):
        return lax.rem(self.z + 4 - k, 4)

    def origin(self, k):
        return self.plane(k) * 2 + self.core

    def copy(self, it, src, dst, s, r, dev):
        return pltpu.make_async_remote_copy(
            src_ref=src, dst_ref=dst, send_sem=self.send_sem.at[it.index, s], recv_sem=self.recv_sem.at[it.index, r],
            device_id=dev, device_id_type=MESH,
        )

    def along_z(self, it, k):
        return self.copy(it, it.source(self.d), it.place(self.f, self.d), k - 1, k - 1, (self.d, self.to(k)))

    def to_x(self, it, k):
        ref = it.place(self.origin(k), self.d)
        return self.copy(it, ref, ref, 2 + k, 2 + k, (self.dx, self.f))

    def to_y(self, it, k):
        ref = it.place(self.origin(k), self.d)
        return self.copy(it, ref, ref, 5 + k, 5 + k, (self.dy, self.f))

    def diag_y(self, it, k):
        ref = it.place(self.origin(k), self.dx, 0)
        return self.copy(it, ref, ref, 8 + k, 8 + k, (self.dy, self.f))

    def diag_x(self, it, k):
        ref = it.place(self.origin(k), self.dy, 1)
        return self.copy(it, ref, ref, 11 + k, 11 + k, (self.dx, self.f))

    def to_core(self, it, k):
        ref = it.place(self.origin(k))
        return self.copy(it, ref, ref, 14 + k, 14 + k, (self.d, self.sib))

    def own_copy(self, it):
        return self.copy(it, it.own(), it.place(self.f), 18, 18, (self.d, self.sib))

    def arrived(self, it, ref, r):
        self.copy(it, ref, ref, 0, r, (self.d, self.f)).wait_recv()

    def barrier(self, peers):
        sem = pltpu.get_barrier_semaphore()
        for peer in peers:
            pl.semaphore_signal(sem, inc=1, device_id=peer, device_id_type=MESH)
        pl.semaphore_wait(sem, len(peers))

    def send_z(self, its, *ks):
        for k in ks:
            for it in its:
                self.along_z(it, k).start()

    def a2(self, its, *ks):
        for k in ks:
            for it in its:
                self.arrived(it, it.place(self.origin(k), self.d), k - 1)
                self.to_x(it, k).start()
                self.to_y(it, k).start()

    def a3(self, its, *ks):
        for k in ks:
            for it in its:
                self.arrived(it, it.place(self.origin(k), self.dx), 2 + k)
                self.diag_y(it, k).start()
                self.arrived(it, it.place(self.origin(k), self.dy), 5 + k)
                self.diag_x(it, k).start()

    def a4(self, its, *ks):
        for k in ks:
            for it in its:
                self.arrived(it, it.place(self.origin(k), self.dd, 0), 8 + k)
                self.arrived(it, it.place(self.origin(k), self.dd, 1), 11 + k)
                self.to_core(it, k).start()

    def a5(self, its, *ks):
        for k in ks:
            for it in its:
                self.arrived(it, it.place(self.plane(k) * 2 + 1 - self.core), 14 + k)

    def from_core(self, its):
        for it in its:
            self.arrived(it, it.place(self.sib), 18)

    def sent(self, its):
        for it in its:
            for k in (1, 2, 3):
                for make in (self.along_z, self.to_x, self.to_y, self.diag_y, self.diag_x, self.to_core):
                    make(it, k).wait_send()
            self.own_copy(it).wait_send()


def run_plan(i, plan):
    for step, act in plan.items():
        @pl.when(i == step)
        def _(act=act):
            act()


def down_kernel(
    n_prompts, x_ref, gs_ref, dq_s, dkv_s, uq_s, ukv_s, cos_ref, sin_ref,
    c_all, r_ref, cq_all, rt_all, wuq_out, wukv_out,
    wdq, wdkv, wuq, wukv, gains, gvec, a_all, acc,
    send_sem, recv_sem, g_send, g_recv, local_sem,
):
    i = pl.program_id(0)
    net = Net(send_sem, recv_sem)
    d, f, z = net.d, net.f, net.z
    items = [
        Item(0, dkv_s, 0, wdkv.shape[1], wdkv), Item(1, dq_s, 0, wdq.shape[1], wdq),
        Item(2, ukv_s, 0, wukv.shape[1], wukv), Item(3, uq_s, 0, wuq.shape[1], wuq),
    ]
    down, up = items[:2], items[2:]
    others = range(1, 8)

    def keep(it):
        return pltpu.make_async_copy(it.own(), it.place(f), local_sem.at[it.index])

    def keep_gain():
        return pltpu.make_async_copy(gs_ref, gains.at[f], local_sem.at[4])

    def gain_copy(j):
        return pltpu.make_async_remote_copy(
            src_ref=gs_ref, dst_ref=gains.at[f], send_sem=g_send.at[j - 1], recv_sem=g_recv.at[j - 1],
            device_id=(d, lax.rem(f + j, 8)), device_id_type=MESH,
        )

    @pl.when(i == 0)
    def _():
        net.barrier([(net.dx, f), (net.dy, f)] + [(d, lax.rem(f + j, 8)) for j in others])
        for j in others:
            gain_copy(j).start()
        keep_gain().start()
        for it in down:
            net.own_copy(it).start()
            keep(it).start()
        net.send_z(down, 1, 2, 3)
        net.send_z(up, 1, 2, 3)
        for it in up:
            net.own_copy(it).start()
            keep(it).start()
        for j in others:
            gain_copy(j).wait_recv()
        keep_gain().wait()
        total = jnp.sum(gains[...], axis=0)
        for t in range(gvec.shape[1] // LANES):
            gvec[:, t * LANES:(t + 1) * LANES] = total[t:t + 1, :]
        for it in down:
            keep(it).wait()
        net.from_core(down)

    d_model, q_rank, kv_rank = x_ref.shape[-1], cq_all.shape[-1], c_all.shape[-1]
    k_rows = d_model // 4
    s2 = n_prompts
    end = s2 + 3

    run_plan(i, {
        3: lambda: net.a2(down, 1),
        5: lambda: net.a3(down, 1),
        7: lambda: (net.a2(down, 2), net.a4(down, 1)),
        s2: lambda: (net.a3(down, 2), net.a5(down, 1)),
        s2 + 1: lambda: (net.a2(down, 3), net.a4(down, 2), net.a5(down, 2)),
        s2 + 2: lambda: (net.a3(down, 3), net.a2(up, 1), net.a4(down, 3), net.a5(down, 3)),
        s2 + 3: lambda: (net.a2(up, 2), net.a3(up, 1)),
    })

    def partial_sums(p, k):
        rows = pl.ds(pl.multiple_of(net.plane(k) * k_rows, LANES), k_rows)
        a = a_all[p, :, rows]
        qd = jnp.dot(a, wdq[rows], preferred_element_type=jnp.float32)
        kd = jnp.dot(a, wdkv[rows], preferred_element_type=jnp.float32)
        if k > 0:
            qd += acc[p, :, :q_rank]
            kd += acc[p, :, q_rank:]
        return qd, kd

    def add_plane(p, k):
        qd, kd = partial_sums(p, k)
        acc[p, :, :q_rank] = qd
        acc[p, :, q_rank:] = kd

    def finish(p):
        qd, kd = partial_sums(p, 3)
        cq_all[p] = (qd * inv_rms(qd) * gvec[:, d_model:d_model + q_rank]).astype(jnp.bfloat16)
        lat = kd[:, :kv_rank]
        c_all[p] = (lat * inv_rms(lat) * gvec[:, d_model + q_rank:]).astype(jnp.bfloat16)
        rt = rotate(kd[:, kv_rank:], cos_ref[...], sin_ref[...]).astype(jnp.bfloat16)
        rt_all[p] = rt
        r_ref[p] = jnp.concatenate([rt[:, :HALF], rt[:, LANES // 2:LANES // 2 + HALF]], axis=1)

    def each(first_p, n, fn):
        def body(p, carry):
            fn(p)
            return carry
        lax.fori_loop(first_p, first_p + n, body, 0)

    @pl.when(i < n_prompts)
    def _():
        x = x_ref[0].astype(jnp.float32)
        a_all[i] = (x * inv_rms(x) * gvec[:, :d_model]).astype(jnp.bfloat16)
        add_plane(i, 0)

    @pl.when(i == s2)
    def _():
        each(0, n_prompts, lambda p: add_plane(p, 1))

    @pl.when(i == s2 + 1)
    def _():
        each(0, n_prompts, lambda p: add_plane(p, 2))

    @pl.when(i >= s2 + 2)
    def _():
        half = n_prompts // 2
        each((i - s2 - 2) * half, half, finish)

    @pl.when(i == end)
    def _():
        net.a3(up, 2)
        net.a2(up, 3)
        net.a4(up, 1)
        net.a3(up, 3)
        net.a4(up, 2, 3)
        for it in up:
            keep(it).wait()
        net.from_core(up)
        net.a5(up, 1, 2, 3)
        outs = [pltpu.make_async_copy(it.full, o, local_sem.at[n]) for n, (it, o) in enumerate(zip(up, (wukv_out, wuq_out)))]
        for out in outs:
            out.start()
        for out in outs:
            out.wait()
        for j in others:
            gain_copy(j).wait_send()
        net.sent(items)


def attend_kernel(
    n_prompts, cq_ref, c_ref, rt_ref, wuq, wukv, cos_ref, sin_ref, out_s,
    o_ref, wout_ref, stage, send_sem, recv_sem, local_sem,
):
    i = pl.program_id(0)
    net = Net(send_sem, recv_sem)
    d, f = net.d, net.f
    last = [Item(0, out_s, 0, wout_ref.shape[1], wout_ref)]

    def take():
        return pltpu.make_async_copy(last[0].own(), stage, local_sem.at[0])

    def put():
        return pltpu.make_async_copy(stage, last[0].place(f), local_sem.at[1])

    @pl.when(i == 0)
    def _():
        net.barrier([(net.dx, f), (net.dy, f), (d, net.sib)] + [(d, net.to(k)) for k in (1, 2, 3)])
        net.send_z(last, 1, 2, 3)
        net.own_copy(last[0]).start()
        take().start()

    run_plan(i, {
        1: lambda: (take().wait(), put().start()),
        2: lambda: net.a2(last, 1),
        3: lambda: (net.a2(last, 2), net.a3(last, 1)),
        4: lambda: (net.a2(last, 3), net.a3(last, 2), net.a4(last, 1)),
        5: lambda: (net.a3(last, 3), net.a4(last, 2)),
        6: lambda: net.a4(last, 3),
    })

    q_cols, kv_cols, o_cols = GROUP * (NOPE + ROPE), GROUP * (NOPE + VDIM), GROUP * VDIM
    scale = (NOPE + ROPE) ** -0.5 * LOG2E
    cq = cq_ref[0]
    lat = c_ref[0]
    slots = slot_masks(rt_ref[0])

    def body(g, carry):
        wq = wuq[:, pl.ds(pl.multiple_of(g * q_cols, q_cols), q_cols)]
        wkv = wukv[:, pl.ds(pl.multiple_of(g * kv_cols, kv_cols), kv_cols)]
        q = jnp.dot(cq, wq, preferred_element_type=jnp.float32)
        kv = jnp.dot(lat, wkv, preferred_element_type=jnp.float32)
        o = attend_heads(q, kv, slots, cos_ref[...], sin_ref[...], scale)
        o_ref[0, :, pl.ds(pl.multiple_of(g * o_cols, o_cols), o_cols)] = o
        return carry

    lax.fori_loop(0, wuq.shape[1] // q_cols, body, 0)

    @pl.when(i == n_prompts - 1)
    def _():
        put().wait()
        net.from_core(last)
        net.a5(last, 1, 2, 3)
        net.sent(last)


def slot_masks(rt):
    lane = lax.broadcasted_iota(jnp.int32, (1, LANES), 1)
    slot = lax.rem(lane, LANES // 2) // HALF
    return [jnp.where(slot == j, rt, 0) for j in range(PE_TILE)]


MESH = pl.DeviceIdType.MESH
GAIN_ROWS = 32
N_SEND, N_RECV = 19, 19


class Item:
    def __init__(self, index, shard, col, cols, full):
        self.index, self.shard, self.col, self.cols, self.full = index, shard, col, cols, full
        self.rows = shard.shape[0]
        if (self.rows // 4) % 16 == 0:
            self.q_rows, self.q_cols = self.rows // 4, cols
        elif (cols // 4) % LANES == 0 and self.rows == 32:
            self.q_rows, self.q_cols = self.rows, cols // 4
        else:
            self.q_rows, self.q_cols = self.rows // 2, cols // 2
        if self.q_rows == self.rows:
            n = self.q_rows // 2
            self.halves = [(0, n, 0, self.q_cols), (n, n, 0, self.q_cols)]
        else:
            n = -(-self.q_cols // (2 * LANES)) * LANES
            self.halves = [(0, self.q_rows, 0, n), (0, self.q_rows, n, self.q_cols - n)]

    def quarter(self, q):
        per_row = self.cols // self.q_cols
        return (q // per_row) * self.q_rows, lax.rem(q, per_row) * self.q_cols

    def source(self, q):
        r, c = self.quarter(q)
        return self.shard.at[pl.ds(pl.multiple_of(r, 16), self.q_rows), pl.ds(pl.multiple_of(self.col + c, LANES), self.q_cols)]

    def own(self):
        return self.shard.at[:, pl.ds(self.col, self.cols)]

    def place(self, f, q=None, half=None):
        r, c = (0, 0) if q is None else self.quarter(q)
        r = f * self.rows + r
        if q is None:
            n_r, n_c = self.rows, self.cols
        elif half is None:
            n_r, n_c = self.q_rows, self.q_cols
        else:
            dr, n_r, dc, n_c = self.halves[half]
            r, c = r + dr, c + dc
        if n_c == self.cols:
            return self.full.at[pl.ds(pl.multiple_of(r, 16), n_r)]
        return self.full.at[pl.ds(pl.multiple_of(r, 16), n_r), pl.ds(pl.multiple_of(c, LANES), n_c)]


def core_kernel(
    n_prompts, x_ref, gs_ref, dq_s, dkv_s, uq_s, ukv_s, out_s, cos_ref, sin_ref,
    c_all, r_ref, oa_ref, ob_ref, wout_ref,
    wdq, wdkv, wuqa, wuqb, wukva, wukvb, gains, gvec, a_all, acc, cq_all, rt_all, stage,
    send_sem, recv_sem, g_send, g_recv, local_sem,
):
    i = pl.program_id(0)
    d, f = lax.axis_index('dp'), lax.axis_index('fsdp')
    z, core = f // 2, lax.rem(f, 2)
    dx = lax.rem(d + 2, 4)
    dy = d + 1 - 2 * lax.rem(d, 2)
    dd = lax.rem(dy + 2, 4)
    sib = z * 2 + 1 - core
    n_a = wuqa.shape[1]
    m_a = wukva.shape[1]
    dkv = Item(0, dkv_s, 0, wdkv.shape[1], wdkv)
    dq = Item(1, dq_s, 0, wdq.shape[1], wdq)
    ukva = Item(2, ukv_s, 0, m_a, wukva)
    uqa = Item(3, uq_s, 0, n_a, wuqa)
    ukvb = Item(4, ukv_s, m_a, wukvb.shape[1], wukvb)
    uqb = Item(5, uq_s, n_a, wuqb.shape[1], wuqb)
    wo = Item(6, out_s, 0, wout_ref.shape[1], wout_ref)
    items = [dkv, dq, ukva, uqa, ukvb, uqb, wo]
    down, first, rest, last = (dkv, dq), (ukva, uqa), (ukvb, uqb), (wo,)

    def to(k):
        return lax.rem(z + k, 4) * 2 + core

    def origin(k):
        return lax.rem(z + 4 - k, 4) * 2 + core

    def copy(it, src, dst, s, r, dev):
        return pltpu.make_async_remote_copy(
            src_ref=src, dst_ref=dst, send_sem=send_sem.at[it.index, s], recv_sem=recv_sem.at[it.index, r],
            device_id=dev, device_id_type=MESH,
        )

    def along_z(it, k):
        return copy(it, it.source(d), it.place(f, d), k - 1, k - 1, (d, to(k)))

    def to_x(it, k):
        ref = it.place(origin(k), d)
        return copy(it, ref, ref, 2 + k, 2 + k, (dx, f))

    def to_y(it, k):
        ref = it.place(origin(k), d)
        return copy(it, ref, ref, 5 + k, 5 + k, (dy, f))

    def diag_y(it, k):
        ref = it.place(origin(k), dx, 0)
        return copy(it, ref, ref, 8 + k, 8 + k, (dy, f))

    def diag_x(it, k):
        ref = it.place(origin(k), dy, 1)
        return copy(it, ref, ref, 11 + k, 11 + k, (dx, f))

    def to_core(it, k):
        ref = it.place(origin(k))
        return copy(it, ref, ref, 14 + k, 14 + k, (d, sib))

    def own_copy(it):
        return copy(it, it.own(), it.place(f), 18, 18, (d, sib))

    def arrived(it, ref, r):
        return copy(it, ref, ref, 0, r, (d, f)).wait_recv()

    def keep(it):
        return pltpu.make_async_copy(it.own(), stage if it is wo else it.place(f), local_sem.at[it.index])

    def keep_out():
        return pltpu.make_async_copy(stage, wo.place(f), local_sem.at[7])

    def gain_copy(j):
        return pltpu.make_async_remote_copy(
            src_ref=gs_ref, dst_ref=gains.at[f], send_sem=g_send.at[j - 1], recv_sem=g_recv.at[j - 1],
            device_id=(d, lax.rem(f + j, 8)), device_id_type=MESH,
        )

    def a2(its, *ks):
        for k in ks:
            for it in its:
                arrived(it, it.place(origin(k), d), k - 1)
                to_x(it, k).start()
                to_y(it, k).start()

    def a3(its, *ks):
        for k in ks:
            for it in its:
                arrived(it, it.place(origin(k), dx), 2 + k)
                diag_y(it, k).start()
                arrived(it, it.place(origin(k), dy), 5 + k)
                diag_x(it, k).start()

    def a4(its, *ks):
        for k in ks:
            for it in its:
                arrived(it, it.place(origin(k), dd, 0), 8 + k)
                arrived(it, it.place(origin(k), dd, 1), 11 + k)
                to_core(it, k).start()

    def a5(its, *ks):
        for k in ks:
            for it in its:
                arrived(it, it.place(lax.rem(z + 4 - k, 4) * 2 + 1 - core), 14 + k)

    def a5_own(its):
        for it in its:
            (keep_out() if it is wo else keep(it)).wait()
            arrived(it, it.place(sib), 18)

    def sent(it):
        for k in (1, 2, 3):
            for make in (along_z, to_x, to_y, diag_y, diag_x, to_core):
                make(it, k).wait_send()

    @pl.when(i == 0)
    def _():
        barrier = pltpu.get_barrier_semaphore()
        peers = [(dx, f), (dy, f)] + [(d, lax.rem(f + j, 8)) for j in range(1, 8)]
        for peer in peers:
            pl.semaphore_signal(barrier, inc=1, device_id=peer, device_id_type=MESH)
        pl.semaphore_wait(barrier, len(peers))
        for j in range(1, 8):
            gain_copy(j).start()
        g_own = pltpu.make_async_copy(gs_ref, gains.at[f], local_sem.at[8])
        g_own.start()
        for it in down:
            own_copy(it).start()
            keep(it).start()
        for group in (down, first, rest, last):
            for k in (1, 2, 3):
                for it in group:
                    along_z(it, k).start()
        for it in items[2:]:
            own_copy(it).start()
            keep(it).start()
        for j in range(1, 8):
            gain_copy(j).wait_recv()
        g_own.wait()
        total = jnp.sum(gains[...], axis=0)
        for t in range(gvec.shape[1] // LANES):
            gvec[:, t * LANES:(t + 1) * LANES] = total[t:t + 1, :]
        a5_own(down)

    d_model, q_rank, kv_rank = x_ref.shape[-1], cq_all.shape[-1], c_all.shape[-1]
    k_rows = d_model // 4
    s2 = n_prompts
    s3 = s2 + 4
    s4 = s3 + n_prompts
    end = s4 + n_prompts - 1

    plan = {
        3: lambda: a2(down, 1),
        5: lambda: a3(down, 1),
        7: lambda: (a2(down, 2), a4(down, 1)),
        s2: lambda: (a3(down, 2), a5(down, 1)),
        s2 + 1: lambda: (a2(down, 3), a4(down, 2), a5(down, 2)),
        s2 + 2: lambda: (a3(down, 3), a2(first, 1), a4(down, 3), a2(first, 2), a5(down, 3)),
        s2 + 3: lambda: (a2(first, 3), a3(first, 1)),
        s3: lambda: (
            a3(first, 2), a2(rest, 1), a3(first, 3), a4(first, 1), a2(rest, 2), a4(first, 2, 3), a5_own(first), a5(first, 1, 2, 3)
        ),
        s3 + 1: lambda: (a2(rest, 3), a3(rest, 1)),
        s3 + 2: lambda: (a3(rest, 2), a2(last, 1)),
        s3 + 3: lambda: (a3(rest, 3), a4(rest, 1)),
        s3 + 4: lambda: a4(rest, 2),
        s3 + 5: lambda: (a4(rest, 3), a2(last, 2), a3(last, 1)),
        s4: lambda: (a5_own(rest), a5(rest, 1, 2, 3), a2(last, 3), a3(last, 2)),
        s4 + 1: lambda: a4(last, 1),
        s4 + 2: lambda: (a3(last, 3), a4(last, 2)),
        s4 + 4: lambda: a4(last, 3),
    }
    for step, act in plan.items():
        @pl.when(i == step)
        def _(act=act):
            act()

    @pl.when(i == 1)
    def _():
        keep(wo).wait()
        keep_out().start()

    def partial_sums(p, k):
        row = lax.rem(z + 4 - k, 4) * k_rows
        rows = pl.ds(pl.multiple_of(row, LANES), k_rows)
        a = a_all[p, :, rows]
        qd = jnp.dot(a, wdq[rows], preferred_element_type=jnp.float32)
        kd = jnp.dot(a, wdkv[rows], preferred_element_type=jnp.float32)
        if k > 0:
            qd += acc[p, :, :q_rank]
            kd += acc[p, :, q_rank:]
        return qd, kd

    def add_plane(p, k):
        qd, kd = partial_sums(p, k)
        acc[p, :, :q_rank] = qd
        acc[p, :, q_rank:] = kd

    def finish(p):
        qd, kd = partial_sums(p, 3)
        cq_all[p] = (qd * inv_rms(qd) * gvec[:, d_model:d_model + q_rank]).astype(jnp.bfloat16)
        lat = kd[:, :kv_rank]
        c_all[p] = (lat * inv_rms(lat) * gvec[:, d_model + q_rank:]).astype(jnp.bfloat16)
        rt = rotate(kd[:, kv_rank:], cos_ref[...], sin_ref[...]).astype(jnp.bfloat16)
        rt_all[p] = rt
        r_ref[p] = jnp.concatenate([rt[:, :HALF], rt[:, LANES // 2:LANES // 2 + HALF]], axis=1)

    def each(first_p, n, fn):
        def body(p, carry):
            fn(p)
            return carry
        lax.fori_loop(first_p, first_p + n, body, 0)

    @pl.when(i < n_prompts)
    def _():
        x = x_ref[0].astype(jnp.float32)
        a_all[i] = (x * inv_rms(x) * gvec[:, :d_model]).astype(jnp.bfloat16)
        add_plane(i, 0)

    @pl.when(jnp.logical_and(i >= s2, i < s2 + 2))
    def _():
        @pl.when(i == s2)
        def _():
            each(0, n_prompts, lambda p: add_plane(p, 1))

        @pl.when(i == s2 + 1)
        def _():
            each(0, n_prompts, lambda p: add_plane(p, 2))

    @pl.when(jnp.logical_and(i >= s2 + 2, i < s3))
    def _():
        half = n_prompts // 2
        each((i - s2 - 2) * half, half, finish)

    q_cols, kv_cols, o_cols = GROUP * (NOPE + ROPE), GROUP * (NOPE + VDIM), GROUP * VDIM
    scale = (NOPE + ROPE) ** -0.5 * LOG2E

    def attend(p, wuq, wukv, o_ref):
        cq = cq_all[p]
        lat = c_all[p]
        slots = slot_masks(rt_all[p])

        def body(g, carry):
            wq = wuq[:, pl.ds(pl.multiple_of(g * q_cols, q_cols), q_cols)]
            wkv = wukv[:, pl.ds(pl.multiple_of(g * kv_cols, kv_cols), kv_cols)]
            q = jnp.dot(cq, wq, preferred_element_type=jnp.float32)
            kv = jnp.dot(lat, wkv, preferred_element_type=jnp.float32)
            o = attend_heads(q, kv, slots, cos_ref[...], sin_ref[...], scale)
            o_ref[0, :, pl.ds(pl.multiple_of(g * o_cols, o_cols), o_cols)] = o
            return carry

        lax.fori_loop(0, wuq.shape[1] // q_cols, body, 0)

    @pl.when(jnp.logical_and(i >= s3, i < s4))
    def _():
        attend(i - s3, wuqa, wukva, oa_ref)

    @pl.when(i >= s4)
    def _():
        attend(i - s4, wuqb, wukvb, ob_ref)

    @pl.when(i == end)
    def _():
        a5_own(last)
        a5(last, 1, 2, 3)
        for j in range(1, 8):
            gain_copy(j).wait_send()
        for it in items:
            sent(it)
            own_copy(it).wait_send()


def slot_masks(rt):
    lane = lax.broadcasted_iota(jnp.int32, (1, LANES), 1)
    slot = lax.rem(lane, LANES // 2) // HALF
    return [jnp.where(slot == j, rt, 0) for j in range(PE_TILE)]


def out_kernel(x_ref, o_ref, w_ref, c_in, r_in, y_ref, c_out, r_out):
    step = 512
    o = o_ref[...]
    c_out[...] = c_in[...]
    r_out[...] = r_in[...]
    for n in range(0, y_ref.shape[1], step):
        acc = jnp.dot(o, w_ref[:, n:n + step], preferred_element_type=jnp.float32)
        y_ref[:, n:n + step] = (x_ref[:, n:n + step].astype(jnp.float32) + acc).astype(jnp.bfloat16)


def whole(shape):
    return pl.BlockSpec(shape, lambda i: (0,) * len(shape))


def solution(mesh):
    n_fsdp = mesh.shape['fsdp']

    def local_block(x, g1, wdq, gq, wuq, wdkv, gkv, wukv, wout):
        n_p, seq_len, d_model = x.shape
        kv_rank, q_rank = gkv.shape[0] * n_fsdp, wdq.shape[1]
        cos_np, sin_np = rope_tiles(seq_len)
        cos, sin = jnp.asarray(cos_np), jnp.asarray(sin_np)
        me = lax.axis_index('fsdp')
        spread = [
            lax.dynamic_update_slice(jnp.zeros(g.shape[0] * n_fsdp, jnp.float32), g.astype(jnp.float32), (me * g.shape[0],))
            for g in (g1, gq, gkv)
        ]
        n_gain = d_model + q_rank + kv_rank
        gs = jnp.concatenate(spread + [jnp.zeros(GAIN_ROWS * LANES - n_gain, jnp.float32)]).reshape(GAIN_ROWS, LANES)
        shards = [wdq, arrange_dkv(wdkv, kv_rank), arrange_q(wuq), arrange_kv(wukv)]
        full = lambda w, cols: ((w.shape[0] * n_fsdp, cols), jnp.bfloat16)
        last = n_p - 1
        blk = lambda cols: pl.BlockSpec((1, seq_len, cols), lambda i: (jnp.minimum(i, last), 0, 0))
        out = lambda cols: jax.ShapeDtypeStruct((n_p, seq_len, cols), jnp.bfloat16)
        hbm = pl.BlockSpec(memory_space=pl.ANY)
        made = [out(kv_rank), out(ROPE), out(q_rank), out(LANES)]
        made += [jax.ShapeDtypeStruct(*full(w, w.shape[1])) for w in (wuq, wukv)]
        params = lambda cid: pltpu.CompilerParams(
            vmem_limit_bytes=VMEM_LIMIT, dimension_semantics=("arbitrary",), collective_id=cid, has_side_effects=True,
        )
        vmem = pl.BlockSpec(memory_space=pltpu.VMEM)
        c, r, cq, rt, wuq_all, wukv_all = pl.pallas_call(
            functools.partial(down_kernel, n_p),
            grid=(n_p + 4,),
            in_specs=[blk(d_model)] + [hbm] * 5 + [whole(cos.shape)] * 2,
            out_specs=[vmem] * 4 + [hbm] * 2,
            out_shape=made,
            scratch_shapes=[
                pltpu.VMEM(*full(wdq, q_rank)), pltpu.VMEM(*full(wdkv, kv_rank + LANES)),
                pltpu.VMEM(*full(wuq, wuq.shape[1])), pltpu.VMEM(*full(wukv, wukv.shape[1])),
                pltpu.VMEM((n_fsdp, GAIN_ROWS, LANES), jnp.float32),
                pltpu.VMEM((1, n_gain), jnp.float32),
                pltpu.VMEM((n_p, seq_len, d_model), jnp.bfloat16),
                pltpu.VMEM((n_p, seq_len, q_rank + kv_rank + LANES), jnp.float32),
                pltpu.SemaphoreType.DMA((4, N_SEND)),
                pltpu.SemaphoreType.DMA((4, N_RECV)),
                pltpu.SemaphoreType.DMA((7,)),
                pltpu.SemaphoreType.DMA((7,)),
                pltpu.SemaphoreType.DMA((5,)),
            ],
            compiler_params=params(0),
            name="down",
        )(x, gs, *shards, cos, sin)
        o_cols = wout.shape[0] * n_fsdp
        o, wout_all = pl.pallas_call(
            functools.partial(attend_kernel, n_p),
            grid=(n_p,),
            in_specs=[blk(q_rank), blk(kv_rank), blk(LANES)] + [whole(v.shape) for v in (wuq_all, wukv_all, cos, sin)] + [hbm],
            out_specs=[blk(o_cols), hbm],
            out_shape=[out(o_cols), jax.ShapeDtypeStruct(*full(wout, wout.shape[1]))],
            scratch_shapes=[
                pltpu.VMEM(wout.shape, jnp.bfloat16),
                pltpu.SemaphoreType.DMA((1, N_SEND)),
                pltpu.SemaphoreType.DMA((1, N_RECV)),
                pltpu.SemaphoreType.DMA((2,)),
            ],
            compiler_params=params(1),
            name="attend",
        )(cq, c, rt, wuq_all, wukv_all, cos, sin, wout)
        rows = 512
        tile = lambda cols: pl.BlockSpec((rows, cols), lambda i: (i, 0))
        flat = lambda v: v.reshape(n_p * seq_len, v.shape[-1])
        flat_out = lambda cols: jax.ShapeDtypeStruct((n_p * seq_len, cols), jnp.bfloat16)
        y, c, r = pl.pallas_call(
            out_kernel,
            grid=(n_p * seq_len // rows,),
            in_specs=[tile(d_model), tile(o_cols), whole(wout_all.shape), tile(kv_rank), tile(ROPE)],
            out_specs=[tile(d_model), tile(kv_rank), tile(ROPE)],
            out_shape=[flat_out(d_model), flat_out(kv_rank), flat_out(ROPE)],
            compiler_params=pltpu.CompilerParams(vmem_limit_bytes=VMEM_LIMIT, dimension_semantics=("arbitrary",)),
            name="project",
        )(flat(x), flat(o), wout_all, flat(c), flat(r))
        back = lambda v: v.reshape(n_p, seq_len, v.shape[-1])
        return back(y), back(c), back(r)

    batch, row, mat = P(('dp', 'fsdp')), P('fsdp'), P('fsdp', None)
    return jax.shard_map(
        local_block,
        mesh=mesh,
        in_specs=(batch, row, mat, row, mat, mat, row, mat, mat),
        out_specs=(batch, batch, batch),
        check_vma=False,
    )
```

```python
import functools

import jax
import jax.numpy as jnp
import numpy as np
from jax import lax
from jax.experimental import pallas as pl
from jax.experimental.pallas import tpu as pltpu
from jax.sharding import PartitionSpec as P

EPSILON = 1e-6
ROPE_THETA = 10000.0
LOG2E = 1.4426950408889634
VMEM_LIMIT = 64000 * 1024

NOPE, ROPE, VDIM = 64, 32, 64
HALF = ROPE // 2
GROUP = 8
PE_TILE = 4
LANES = 128
Q_COLS, KV_COLS = GROUP * (NOPE + ROPE), GROUP * (NOPE + VDIM)
AHEAD, SPREAD = 2, 6
MASKED = -1e30


def rope_tiles(seq_len):
    inv_freq = ROPE_THETA ** (-2.0 * np.arange(HALF) / ROPE)
    angles = np.arange(seq_len)[:, None] * inv_freq[None, :]
    cos = np.tile(np.cos(angles), (1, LANES // HALF))
    sin = np.tile(np.sin(angles), (1, PE_TILE))
    return cos.astype(np.float32), np.concatenate([-sin, sin], axis=1).astype(np.float32)


def arrange_q(w):
    rows = w.shape[0]
    w = w.reshape(rows, -1, GROUP, NOPE + ROPE)
    nope = w[..., :NOPE].reshape(rows, -1, GROUP * NOPE)
    pe = w[..., NOPE:].reshape(rows, -1, GROUP // PE_TILE, PE_TILE, 2, HALF)
    pe = pe.transpose(0, 1, 2, 4, 3, 5).reshape(rows, -1, GROUP * ROPE)
    return jnp.concatenate([nope, pe], axis=-1).reshape(rows, -1)


def arrange_kv(w):
    rows = w.shape[0]
    return w.reshape(rows, -1, GROUP, 2, NOPE).transpose(0, 1, 3, 2, 4).reshape(rows, -1)


def arrange_dkv(w, kv_rank):
    lo, hi = w[:, kv_rank:kv_rank + HALF], w[:, kv_rank + HALF:]
    return jnp.concatenate([w[:, :kv_rank]] + [lo] * PE_TILE + [hi] * PE_TILE, axis=1)


def inv_rms(v):
    return lax.rsqrt(jnp.mean(v * v, axis=-1, keepdims=True) + EPSILON)


def rotate(tile, cos, sin):
    return tile * cos + pltpu.roll(tile, LANES // 2, 1) * sin


MESH = pl.DeviceIdType.MESH
GAIN_ROWS = 32
GROUPS_FIRST = 2
N_COPIES = 19
PLANES = (1, 2, 3)


class Item:
    def __init__(self, index, shard, col, cols, full):
        self.index, self.shard, self.col, self.cols, self.full = index, shard, col, cols, full
        self.rows = shard.shape[0]
        if (self.rows // 4) % 16 == 0:
            self.q_rows, self.q_cols = self.rows // 4, cols
        elif (cols // 4) % LANES == 0 and self.rows == 32:
            self.q_rows, self.q_cols = self.rows, cols // 4
        else:
            self.q_rows, self.q_cols = self.rows // 2, cols // 2
        if self.q_rows == self.rows:
            n = self.q_rows // 2
            self.halves = [(0, n, 0, self.q_cols), (n, n, 0, self.q_cols)]
        else:
            n = -(-self.q_cols // (2 * LANES)) * LANES
            self.halves = [(0, self.q_rows, 0, n), (0, self.q_rows, n, self.q_cols - n)]

    def quarter(self, q):
        per_row = self.cols // self.q_cols
        return (q // per_row) * self.q_rows, lax.rem(q, per_row) * self.q_cols

    def source(self, q):
        r, c = self.quarter(q)
        return self.shard.at[pl.ds(pl.multiple_of(r, 16), self.q_rows), pl.ds(pl.multiple_of(self.col + c, LANES), self.q_cols)]

    def own(self):
        return self.shard.at[:, pl.ds(self.col, self.cols)]

    def place(self, f, q=None, half=None):
        r, c = (0, 0) if q is None else self.quarter(q)
        r = f * self.rows + r
        if q is None:
            n_r, n_c = self.rows, self.cols
        elif half is None:
            n_r, n_c = self.q_rows, self.q_cols
        else:
            dr, n_r, dc, n_c = self.halves[half]
            r, c = r + dr, c + dc
        if n_c == self.cols:
            return self.full.at[pl.ds(pl.multiple_of(r, 16), n_r)]
        return self.full.at[pl.ds(pl.multiple_of(r, 16), n_r), pl.ds(pl.multiple_of(c, LANES), n_c)]


class Net:
    def __init__(self, send_sem, recv_sem):
        self.send_sem, self.recv_sem = send_sem, recv_sem
        self.d, self.f = lax.axis_index('dp'), lax.axis_index('fsdp')
        self.z, self.core = self.f // 2, lax.rem(self.f, 2)
        self.dx = lax.rem(self.d + 2, 4)
        self.dy = self.d + 1 - 2 * lax.rem(self.d, 2)
        self.dd = lax.rem(self.dy + 2, 4)
        self.sib = self.z * 2 + 1 - self.core

    def to(self, k):
        return lax.rem(self.z + k, 4) * 2 + self.core

    def plane(self, k):
        return lax.rem(self.z + 4 - k, 4)

    def origin(self, k):
        return self.plane(k) * 2 + self.core

    def copy(self, it, src, dst, s, r, dev):
        return pltpu.make_async_remote_copy(
            src_ref=src, dst_ref=dst, send_sem=self.send_sem.at[it.index, s], recv_sem=self.recv_sem.at[it.index, r],
            device_id=dev, device_id_type=MESH,
        )

    def along_z(self, it, k):
        return self.copy(it, it.source(self.d), it.place(self.f, self.d), k - 1, k - 1, (self.d, self.to(k)))

    def to_x(self, it, k):
        ref = it.place(self.origin(k), self.d)
        return self.copy(it, ref, ref, 2 + k, 2 + k, (self.dx, self.f))

    def to_y(self, it, k):
        ref = it.place(self.origin(k), self.d)
        return self.copy(it, ref, ref, 5 + k, 5 + k, (self.dy, self.f))

    def diag_y(self, it, k):
        ref = it.place(self.origin(k), self.dx, 0)
        return self.copy(it, ref, ref, 8 + k, 8 + k, (self.dy, self.f))

    def diag_x(self, it, k):
        ref = it.place(self.origin(k), self.dy, 1)
        return self.copy(it, ref, ref, 11 + k, 11 + k, (self.dx, self.f))

    def to_core(self, it, k):
        ref = it.place(self.origin(k))
        return self.copy(it, ref, ref, 14 + k, 14 + k, (self.d, self.sib))

    def own_copy(self, it):
        return self.copy(it, it.own(), it.place(self.f), 18, 18, (self.d, self.sib))

    def arrived(self, it, ref, r):
        self.copy(it, ref, ref, 0, r, (self.d, self.f)).wait_recv()

    def barrier(self, peers):
        sem = pltpu.get_barrier_semaphore()
        for peer in peers:
            pl.semaphore_signal(sem, inc=1, device_id=peer, device_id_type=MESH)
        pl.semaphore_wait(sem, len(peers))

    def send_z(self, its, ks=PLANES):
        for k in ks:
            for it in its:
                self.along_z(it, k).start()

    def a2(self, its, ks=PLANES):
        for k in ks:
            for it in its:
                self.arrived(it, it.place(self.origin(k), self.d), k - 1)
                self.to_x(it, k).start()
                self.to_y(it, k).start()

    def a3(self, its, ks=PLANES):
        for k in ks:
            for it in its:
                self.arrived(it, it.place(self.origin(k), self.dx), 2 + k)
                self.diag_y(it, k).start()
                self.arrived(it, it.place(self.origin(k), self.dy), 5 + k)
                self.diag_x(it, k).start()

    def a4(self, its, ks=PLANES):
        for k in ks:
            for it in its:
                self.arrived(it, it.place(self.origin(k), self.dd, 0), 8 + k)
                self.arrived(it, it.place(self.origin(k), self.dd, 1), 11 + k)
                self.to_core(it, k).start()

    def a5(self, its, ks=PLANES):
        for k in ks:
            for it in its:
                self.arrived(it, it.place(self.plane(k) * 2 + 1 - self.core), 14 + k)

    def from_core(self, its):
        for it in its:
            self.arrived(it, it.place(self.sib), 18)

    def sent(self, its):
        for it in its:
            for k in PLANES:
                for make in (self.along_z, self.to_x, self.to_y, self.diag_y, self.diag_x, self.to_core):
                    make(it, k).wait_send()
            self.own_copy(it).wait_send()


def scores(tiles, slots, low, j):
    qn, qp, kn, _ = tiles
    t = j // 2
    keep = low if j % 2 == 0 else jnp.logical_not(low)
    q_tile = jnp.concatenate([qn[t], qp[j // PE_TILE]], axis=1)
    k_tile = jnp.concatenate([jnp.where(keep, kn[t], 0), slots[j % PE_TILE]], axis=1)
    return lax.dot_general(k_tile, q_tile, (((1,), (1,)), ((), ())), preferred_element_type=jnp.float32)


def softmax(s, diag, zero, scale):
    half = s.shape[0] // 2
    left = jnp.where(diag, s[:half, :half], MASKED)
    up = s[:half, half:]
    right = jnp.where(diag, s[half:, half:], MASKED)
    m_l = jnp.max(left, axis=0, keepdims=True) * scale
    m_r = jnp.max(jnp.maximum(up, right), axis=0, keepdims=True) * scale
    e_l = jnp.exp2(left * scale - m_l)
    e_u = jnp.exp2(up * scale - m_r)
    e_r = jnp.exp2(right * scale - m_r)
    r_l = 1.0 / jnp.sum(e_l, axis=0, keepdims=True)
    r_r = 1.0 / jnp.sum(e_u + e_r, axis=0, keepdims=True)
    p_top = jnp.concatenate([(e_l * r_l).astype(jnp.bfloat16), (e_u * r_r).astype(jnp.bfloat16)], axis=1)
    p_bot = jnp.concatenate([zero, (e_r * r_r).astype(jnp.bfloat16)], axis=1)
    return jnp.concatenate([p_top, p_bot], axis=0)


def pieces(cq, lat, wuq, wukv, g, cos, sin):
    w = 2 * LANES

    def tiles(x, weights, cols, n, pe=False):
        r = jnp.dot(x, weights[:, g * cols + n * w:g * cols + (n + 1) * w], preferred_element_type=jnp.float32)
        both = [r[:, :LANES], r[:, LANES:]]
        return [(rotate(t, cos, sin) if pe else t).astype(jnp.bfloat16) for t in both]

    n_q, n_kv = Q_COLS // w, KV_COLS // w
    return [functools.partial(tiles, cq, wuq, Q_COLS, n, n == n_q - 1) for n in range(n_q)] + [
        functools.partial(tiles, lat, wukv, KV_COLS, n) for n in range(n_kv)
    ]


def arrange_tiles(made):
    flat = [t for pair in made for t in pair]
    n = GROUP // 2
    m = n + GROUP // PE_TILE
    return flat[:n], flat[n:m], flat[m:m + n], [t.T for t in flat[m + n:]]


def attend(cq, lat, rt, cq_next, lat_next, start, wuq, wukv, cos, sin, hold, o_ref):
    n_groups = wuq.shape[1] // Q_COLS
    scale = (NOPE + ROPE) ** -0.5 * LOG2E
    seq_len = cq.shape[0]
    half = seq_len // 2
    low = lax.broadcasted_iota(jnp.int32, (1, LANES), 1) < NOPE
    diag = lax.broadcasted_iota(jnp.int32, (half, half), 0) <= lax.broadcasted_iota(jnp.int32, (half, half), 1)
    zero = jnp.zeros((half, half), jnp.bfloat16)
    slots = slot_masks(rt)
    n_pieces = hold.shape[0] // 2

    def put(n, made):
        for m, t in enumerate(made):
            hold[2 * n + m] = t

    @pl.when(start)
    def _():
        for n, make in enumerate(pieces(cq, lat, wuq, wukv, 0, cos, sin)):
            put(n, make())

    tiles = {0: arrange_tiles([[hold[2 * n], hold[2 * n + 1]] for n in range(n_pieces)])}
    total = n_groups * GROUP
    s, p, outs = {}, {}, {}
    for u in range(-AHEAD, total + 1):
        g, j = divmod(u, GROUP)
        if u >= 0 and u < total:
            p[u] = softmax(s.pop(u), diag, zero, scale)
            if j == 0:
                made = []
                if g + 1 < n_groups:
                    todo = pieces(cq, lat, wuq, wukv, g + 1, cos, sin)
                else:
                    todo = pieces(cq_next, lat_next, wuq, wukv, 0, cos, sin)
            if j < SPREAD:
                for n in range(j * n_pieces // SPREAD, (j + 1) * n_pieces // SPREAD):
                    made.append(todo[n]())
                if len(made) == n_pieces and g + 1 < n_groups:
                    tiles[g + 1] = arrange_tiles(made)
                elif len(made) == n_pieces:
                    for n, m in enumerate(made):
                        put(n, m)
        if u + AHEAD < total:
            v = u + AHEAD
            s[v] = scores(tiles[v // GROUP], slots, low, v % GROUP)
        if u >= 1:
            h = u - 1
            hj = h % GROUP
            vt = tiles[h // GROUP][3][hj // 2][hj % 2 * VDIM:(hj % 2 + 1) * VDIM]
            outs[h] = jnp.dot(vt, p.pop(h), preferred_element_type=jnp.float32).astype(jnp.bfloat16)
            if h % 2 == 1:
                pair = jnp.concatenate([outs.pop(h - 1), outs.pop(h)], axis=0)
                o_ref[0, :, h // 2 * LANES:(h // 2 + 1) * LANES] = pair.T


def slot_masks(rt):
    lane = lax.broadcasted_iota(jnp.int32, (1, LANES), 1)
    slot = lax.rem(lane, LANES // 2) // HALF
    return [jnp.where(slot == j, rt, 0) for j in range(PE_TILE)]


def core_kernel(
    n_prompts, x_ref, gs_ref, dq_s, dkv_s, uq_s, ukv_s, out_s, cos_ref, sin_ref,
    c_all, r_ref, oa_ref, ob_ref, wout_ref,
    wdq, wdkv, wuqa, wuqb, wukva, wukvb, gains, gvec, a_all, acc, cq_all, rt_all, stage, hold,
    send_sem, recv_sem, g_send, g_recv, local_sem,
):
    i = pl.program_id(0)
    net = Net(send_sem, recv_sem)
    d, f = net.d, net.f
    n_a, m_a = wuqa.shape[1], wukva.shape[1]
    todo = [
        (dkv_s, 0, wdkv), (dq_s, 0, wdq), (ukv_s, 0, wukva), (uq_s, 0, wuqa),
        (ukv_s, m_a, wukvb), (uq_s, n_a, wuqb), (out_s, 0, wout_ref),
    ]
    items = [Item(n, shard, col, full.shape[1], full) for n, (shard, col, full) in enumerate(todo)]
    down, first, rest, last = items[:2], items[2:4], items[4:6], items[6:]
    wo = items[6]
    others = range(1, 8)

    def keep(it):
        return pltpu.make_async_copy(it.own(), stage if it is wo else it.place(f), local_sem.at[it.index])

    def keep_out():
        return pltpu.make_async_copy(stage, wo.place(f), local_sem.at[7])

    def keep_gain():
        return pltpu.make_async_copy(gs_ref, gains.at[f], local_sem.at[8])

    def gain_copy(j):
        return pltpu.make_async_remote_copy(
            src_ref=gs_ref, dst_ref=gains.at[f], send_sem=g_send.at[j - 1], recv_sem=g_recv.at[j - 1],
            device_id=(d, lax.rem(f + j, 8)), device_id_type=MESH,
        )

    @pl.when(i == 0)
    def _():
        net.barrier([(net.dx, f), (net.dy, f)] + [(d, lax.rem(f + j, 8)) for j in others])
        for j in others:
            gain_copy(j).start()
        keep_gain().start()
        for it in down:
            net.own_copy(it).start()
            keep(it).start()
        for group in (down, first, rest, last):
            net.send_z(group)
        for it in items[2:]:
            net.own_copy(it).start()
            keep(it).start()
        for j in others:
            gain_copy(j).wait_recv()
        keep_gain().wait()
        total = jnp.sum(gains[...], axis=0)
        for t in range(gvec.shape[1] // LANES):
            gvec[:, t * LANES:(t + 1) * LANES] = total[t:t + 1, :]
        for it in down:
            keep(it).wait()
        net.from_core(down)

    d_model, q_rank, kv_rank = x_ref.shape[-1], cq_all.shape[-1], c_all.shape[-1]
    seq_len = x_ref.shape[1]
    k_rows = d_model // 4
    half = n_prompts // 2
    c1 = n_prompts
    c2 = c1 + half
    fin = c2 + half
    pa = fin + half
    pb = pa + n_prompts
    end = pb + n_prompts - 1
    one, two, three = ((k,) for k in PLANES)

    @pl.when(i == 1)
    def _():
        keep(wo).wait()
        keep_out().start()

    def ready(its):
        for it in its:
            (keep_out() if it is wo else keep(it)).wait()
        net.from_core(its)
        net.a5(its)

    plan = [
        (4, [(net.a2, down, one)]),
        (7, [(net.a2, down, two), (net.a3, down, one)]),
        (c1, [(net.a4, down, one), (net.a2, down, three), (net.a3, down, two), (net.a5, down, one)]),
        (c1 + 2, [(net.a4, down, two)]),
        (c1 + 3, [(net.a3, down, three), (net.a2, first, one)]),
        (c2, [(net.a2, first, two), (net.a5, down, two)]),
        (c2 + 1, [(net.a3, first, one), (net.a2, first, three)]),
        (c2 + 2, [(net.a4, down, three)]),
        (c2 + 3, [(net.a3, first, two), (net.a2, rest, one)]),
        (fin, [(net.a5, down, three), (net.a3, first, three), (net.a4, first, one)]),
        (fin + 1, [(net.a4, first, two)]),
        (fin + 2, [(net.a2, rest, two), (net.a3, rest, one), (net.a4, first, three)]),
        (pa, [(net.a2, rest, three), (net.a3, rest, two), (net.a4, rest, one)]),
        (pa + 1, [(net.a3, rest, three), (net.a4, rest, two)]),
        (pa + 2, [(net.a4, rest, three)]),
        (pa + 4, [(net.a2, last, one)]),
        (pa + 6, [(net.a3, last, one)]),
        (pb, [(net.a4, last, one), (net.a2, last, two)]),
        (pb + 2, [(net.a3, last, two)]),
        (pb + 3, [(net.a2, last, three), (net.a4, last, two)]),
        (pb + 5, [(net.a3, last, three)]),
        (pb + 6, [(net.a4, last, three)]),
    ]
    for step, acts in plan:
        @pl.when(i == step)
        def _(acts=acts):
            for act, its, ks in acts:
                act(its, ks)

    for step, its in ((pa, first), (pb, rest)):
        @pl.when(i == step)
        def _(its=its):
            ready(its)

    def partial_sums(p, n, k):
        rows = pl.ds(pl.multiple_of(net.plane(k) * k_rows, LANES), k_rows)
        a = a_all[pl.ds(p, n), :, rows].reshape(n * seq_len, k_rows)
        qd = jnp.dot(a, wdq[rows], preferred_element_type=jnp.float32)
        kd = jnp.dot(a, wdkv[rows], preferred_element_type=jnp.float32)
        if k > 0:
            old = acc[pl.ds(p, n)].reshape(n * seq_len, q_rank + kv_rank + LANES)
            qd += old[:, :q_rank]
            kd += old[:, q_rank:]
        return qd, kd

    def add_plane(p, n, k):
        qd, kd = partial_sums(p, n, k)
        acc[pl.ds(p, n), :, :q_rank] = qd.reshape(n, seq_len, q_rank)
        acc[pl.ds(p, n), :, q_rank:] = kd.reshape(n, seq_len, kv_rank + LANES)

    @pl.when(i < c1)
    def _():
        x = x_ref[0].astype(jnp.float32)
        a_all[i] = (x * inv_rms(x) * gvec[:, :d_model]).astype(jnp.bfloat16)
        add_plane(i, 1, 0)

    @pl.when(jnp.logical_and(i >= c1, i < c2))
    def _():
        add_plane((i - c1) * 2, 2, 1)

    @pl.when(jnp.logical_and(i >= c2, i < fin))
    def _():
        add_plane((i - c2) * 2, 2, 2)

    @pl.when(jnp.logical_and(i >= fin, i < pa))
    def _():
        p = (i - fin) * 2
        qd, kd = partial_sums(p, 2, 3)
        cq = (qd * inv_rms(qd) * gvec[:, d_model:d_model + q_rank]).astype(jnp.bfloat16)
        cq_all[pl.ds(p, 2)] = cq.reshape(2, seq_len, q_rank)
        lat = kd[:, :kv_rank]
        lat = (lat * inv_rms(lat) * gvec[:, d_model + q_rank:]).astype(jnp.bfloat16)
        c_all[pl.ds(p, 2)] = lat.reshape(2, seq_len, kv_rank)
        for n in range(2):
            pe = kd[n * seq_len:(n + 1) * seq_len, kv_rank:]
            rt = rotate(pe, cos_ref[...], sin_ref[...]).astype(jnp.bfloat16)
            rt_all[p + n] = rt
            rt_t = rt.T
            r_ref[p + n] = jnp.concatenate([rt_t[:HALF], rt_t[LANES // 2:LANES // 2 + HALF]], axis=0)

    def attend_step(p, wuq, wukv, o_ref):
        after = jnp.minimum(p + 1, n_prompts - 1)
        attend(
            cq_all[p], c_all[p], rt_all[p], cq_all[after], c_all[after], p == 0,
            wuq, wukv, cos_ref[...], sin_ref[...], hold, o_ref,
        )

    @pl.when(jnp.logical_and(i >= pa, i < pb))
    def _():
        attend_step(i - pa, wuqa, wukva, oa_ref)

    @pl.when(i >= pb)
    def _():
        attend_step(i - pb, wuqb, wukvb, ob_ref)

    @pl.when(i == end)
    def _():
        ready(last)
        for j in others:
            gain_copy(j).wait_send()
        net.sent(items)


def out_kernel(x_ref, oa_ref, ob_ref, w_hbm, c_in, r_in, y_ref, c_out, r_out, w, sem):
    step = 512
    n_steps = y_ref.shape[1] // step
    first = pl.program_id(0) == 0
    cols = [slice(n * step, (n + 1) * step) for n in range(n_steps)]
    load = [pltpu.make_async_copy(w_hbm.at[:, c], w.at[:, c], sem.at[n]) for n, c in enumerate(cols)]

    @pl.when(first)
    def _():
        for part in load:
            part.start()

    oa, ob = oa_ref[...], ob_ref[...]
    n_a = oa.shape[1]
    c_out[...] = c_in[...]
    r_out[...] = r_in[...]
    for part, c in zip(load, cols):
        @pl.when(first)
        def _(part=part):
            part.wait()

        acc = jnp.dot(oa, w[:n_a, c], preferred_element_type=jnp.float32)
        acc += jnp.dot(ob, w[n_a:, c], preferred_element_type=jnp.float32)
        y_ref[:, c] = (x_ref[:, c].astype(jnp.float32) + acc).astype(jnp.bfloat16)


def whole(shape):
    return pl.BlockSpec(shape, lambda i: (0,) * len(shape))


def solution(mesh):
    n_fsdp = mesh.shape['fsdp']

    def local_block(x, g1, wdq, gq, wuq, wdkv, gkv, wukv, wout):
        n_p, seq_len, d_model = x.shape
        kv_rank, q_rank = gkv.shape[0] * n_fsdp, wdq.shape[1]
        cos_np, sin_np = rope_tiles(seq_len)
        cos, sin = jnp.asarray(cos_np), jnp.asarray(sin_np)
        me = lax.axis_index('fsdp')
        spread = [
            lax.dynamic_update_slice(jnp.zeros(g.shape[0] * n_fsdp, jnp.float32), g.astype(jnp.float32), (me * g.shape[0],))
            for g in (g1, gq, gkv)
        ]
        n_gain = d_model + q_rank + kv_rank
        gs = jnp.concatenate(spread + [jnp.zeros(GAIN_ROWS * LANES - n_gain, jnp.float32)]).reshape(GAIN_ROWS, LANES)
        shards = [wdq, arrange_dkv(wdkv, kv_rank), arrange_q(wuq), arrange_kv(wukv), wout]
        full = lambda w, cols: pltpu.VMEM((w.shape[0] * n_fsdp, cols), jnp.bfloat16)
        o_cols = GROUP * VDIM
        n_groups = wuq.shape[1] // Q_COLS
        first, rest = GROUPS_FIRST, n_groups - GROUPS_FIRST
        last = n_p - 1
        pa = 2 * n_p + n_p // 2
        blk = lambda cols, lag: pl.BlockSpec((1, seq_len, cols), lambda i: (jnp.clip(i - lag, 0, last), 0, 0))
        out = lambda cols: jax.ShapeDtypeStruct((n_p, seq_len, cols), jnp.bfloat16)
        r_shape = jax.ShapeDtypeStruct((n_p, ROPE, seq_len), jnp.bfloat16)
        hbm = pl.BlockSpec(memory_space=pl.ANY)
        c, r, oa, ob, wout_all = pl.pallas_call(
            functools.partial(core_kernel, n_p),
            grid=(4 * n_p + n_p // 2,),
            in_specs=[blk(d_model, 0)] + [hbm] * 6 + [whole(cos.shape)] * 2,
            out_specs=[
                whole((n_p, seq_len, kv_rank)), whole((n_p, ROPE, seq_len)),
                blk(first * o_cols, pa), blk(rest * o_cols, pa + n_p), hbm,
            ],
            out_shape=[
                out(kv_rank), r_shape, out(first * o_cols), out(rest * o_cols),
                jax.ShapeDtypeStruct((wout.shape[0] * n_fsdp, wout.shape[1]), jnp.bfloat16),
            ],
            scratch_shapes=[
                full(wdq, q_rank), full(wdkv, kv_rank + LANES),
                full(wuq, first * Q_COLS), full(wuq, rest * Q_COLS),
                full(wukv, first * KV_COLS), full(wukv, rest * KV_COLS),
                pltpu.VMEM((n_fsdp, GAIN_ROWS, LANES), jnp.float32),
                pltpu.VMEM((1, n_gain), jnp.float32),
                pltpu.VMEM((n_p, seq_len, d_model), jnp.bfloat16),
                pltpu.VMEM((n_p, seq_len, q_rank + kv_rank + LANES), jnp.float32),
                pltpu.VMEM((n_p, seq_len, q_rank), jnp.bfloat16),
                pltpu.VMEM((n_p, seq_len, LANES), jnp.bfloat16),
                pltpu.VMEM(wout.shape, jnp.bfloat16),
                pltpu.VMEM(((Q_COLS + KV_COLS) // LANES, seq_len, LANES), jnp.bfloat16),
                pltpu.SemaphoreType.DMA((7, N_COPIES)),
                pltpu.SemaphoreType.DMA((7, N_COPIES)),
                pltpu.SemaphoreType.DMA((7,)),
                pltpu.SemaphoreType.DMA((7,)),
                pltpu.SemaphoreType.DMA((9,)),
            ],
            compiler_params=pltpu.CompilerParams(
                vmem_limit_bytes=VMEM_LIMIT, dimension_semantics=("arbitrary",), collective_id=0, has_side_effects=True,
            ),
            name="core",
        )(x, gs, *shards, cos, sin)
        rows = 512
        tile = lambda cols: pl.BlockSpec((rows, cols), lambda i: (i, 0))
        r_tile = pl.BlockSpec((rows // seq_len, ROPE, seq_len), lambda i: (i, 0, 0))
        flat = lambda v: v.reshape(n_p * seq_len, v.shape[-1])
        flat_out = lambda cols: jax.ShapeDtypeStruct((n_p * seq_len, cols), jnp.bfloat16)
        y, c, r = pl.pallas_call(
            out_kernel,
            grid=(n_p * seq_len // rows,),
            in_specs=[tile(d_model), tile(oa.shape[-1]), tile(ob.shape[-1]), hbm, tile(kv_rank), r_tile],
            out_specs=[tile(d_model), tile(kv_rank), r_tile],
            out_shape=[flat_out(d_model), flat_out(kv_rank), r_shape],
            scratch_shapes=[pltpu.VMEM(wout_all.shape, jnp.bfloat16), pltpu.SemaphoreType.DMA((8,))],
            compiler_params=pltpu.CompilerParams(vmem_limit_bytes=VMEM_LIMIT, dimension_semantics=("arbitrary",)),
            name="project",
        )(flat(x), flat(oa), flat(ob), wout_all, flat(c), r)
        back = lambda v: v.reshape(n_p, seq_len, v.shape[-1])
        return back(y), back(c), jnp.swapaxes(r, 1, 2)

    batch, row, mat = P(('dp', 'fsdp')), P('fsdp'), P('fsdp', None)
    return jax.shard_map(
        local_block,
        mesh=mesh,
        in_specs=(batch, row, mat, row, mat, mat, row, mat, mat),
        out_specs=(batch, batch, batch),
        check_vma=False,
    )
```

```python
import functools

import jax
import jax.numpy as jnp
import numpy as np
from jax import lax
from jax.experimental import pallas as pl
from jax.experimental.pallas import tpu as pltpu
from jax.sharding import PartitionSpec as P

EPSILON = 1e-6
ROPE_THETA = 10000.0
LOG2E = 1.4426950408889634
VMEM_LIMIT = 64000 * 1024

NOPE, ROPE, VDIM = 64, 32, 64
HALF = ROPE // 2
GROUP = 8
PE_TILE = 4
LANES = 128
Q_COLS, KV_COLS = GROUP * (NOPE + ROPE), GROUP * (NOPE + VDIM)
AHEAD, SPREAD = 2, 6
MASKED = -1e30


def rope_tiles(seq_len):
    inv_freq = ROPE_THETA ** (-2.0 * np.arange(HALF) / ROPE)
    angles = np.arange(seq_len)[:, None] * inv_freq[None, :]
    cos = np.tile(np.cos(angles), (1, LANES // HALF))
    sin = np.tile(np.sin(angles), (1, PE_TILE))
    return cos.astype(np.float32), np.concatenate([-sin, sin], axis=1).astype(np.float32)


def arrange_q(w):
    rows = w.shape[0]
    w = w.reshape(rows, -1, GROUP, NOPE + ROPE)
    nope = w[..., :NOPE].reshape(rows, -1, GROUP * NOPE)
    pe = w[..., NOPE:].reshape(rows, -1, GROUP // PE_TILE, PE_TILE, 2, HALF)
    pe = pe.transpose(0, 1, 2, 4, 3, 5).reshape(rows, -1, GROUP * ROPE)
    return jnp.concatenate([nope, pe], axis=-1).reshape(rows, -1)


def arrange_kv(w):
    rows = w.shape[0]
    return w.reshape(rows, -1, GROUP, 2, NOPE).transpose(0, 1, 3, 2, 4).reshape(rows, -1)


def arrange_dkv(w, kv_rank):
    lo, hi = w[:, kv_rank:kv_rank + HALF], w[:, kv_rank + HALF:]
    return jnp.concatenate([w[:, :kv_rank]] + [lo] * PE_TILE + [hi] * PE_TILE, axis=1)


def inv_rms(v):
    return lax.rsqrt(jnp.mean(v * v, axis=-1, keepdims=True) + EPSILON)


def rotate(tile, cos, sin):
    return tile * cos + pltpu.roll(tile, LANES // 2, 1) * sin


MESH = pl.DeviceIdType.MESH
GAIN_ROWS = 32
GROUPS_FIRST = 2
N_COPIES = 19
PLANES = (1, 2, 3)


class Item:
    def __init__(self, index, shard, col, cols, full):
        self.index, self.shard, self.col, self.cols, self.full = index, shard, col, cols, full
        self.rows = shard.shape[0]
        if (self.rows // 4) % 16 == 0:
            self.q_rows, self.q_cols = self.rows // 4, cols
        elif (cols // 4) % LANES == 0 and self.rows == 32:
            self.q_rows, self.q_cols = self.rows, cols // 4
        else:
            self.q_rows, self.q_cols = self.rows // 2, cols // 2
        if self.q_rows == self.rows:
            n = self.q_rows // 2
            self.halves = [(0, n, 0, self.q_cols), (n, n, 0, self.q_cols)]
        else:
            n = -(-self.q_cols // (2 * LANES)) * LANES
            self.halves = [(0, self.q_rows, 0, n), (0, self.q_rows, n, self.q_cols - n)]

    def quarter(self, q):
        per_row = self.cols // self.q_cols
        return (q // per_row) * self.q_rows, lax.rem(q, per_row) * self.q_cols

    def source(self, q):
        r, c = self.quarter(q)
        return self.shard.at[pl.ds(pl.multiple_of(r, 16), self.q_rows), pl.ds(pl.multiple_of(self.col + c, LANES), self.q_cols)]

    def own(self):
        return self.shard.at[:, pl.ds(self.col, self.cols)]

    def place(self, f, q=None, half=None):
        r, c = (0, 0) if q is None else self.quarter(q)
        r = f * self.rows + r
        if q is None:
            n_r, n_c = self.rows, self.cols
        elif half is None:
            n_r, n_c = self.q_rows, self.q_cols
        else:
            dr, n_r, dc, n_c = self.halves[half]
            r, c = r + dr, c + dc
        if n_c == self.cols:
            return self.full.at[pl.ds(pl.multiple_of(r, 16), n_r)]
        return self.full.at[pl.ds(pl.multiple_of(r, 16), n_r), pl.ds(pl.multiple_of(c, LANES), n_c)]


class Net:
    def __init__(self, send_sem, recv_sem):
        self.send_sem, self.recv_sem = send_sem, recv_sem
        self.d, self.f = lax.axis_index('dp'), lax.axis_index('fsdp')
        self.z, self.core = self.f // 2, lax.rem(self.f, 2)
        self.dx = lax.rem(self.d + 2, 4)
        self.dy = self.d + 1 - 2 * lax.rem(self.d, 2)
        self.dd = lax.rem(self.dy + 2, 4)
        self.sib = self.z * 2 + 1 - self.core

    def to(self, k):
        return lax.rem(self.z + k, 4) * 2 + self.core

    def plane(self, k):
        return lax.rem(self.z + 4 - k, 4)

    def origin(self, k):
        return self.plane(k) * 2 + self.core

    def copy(self, it, src, dst, s, r, dev):
        return pltpu.make_async_remote_copy(
            src_ref=src, dst_ref=dst, send_sem=self.send_sem.at[it.index, s], recv_sem=self.recv_sem.at[it.index, r],
            device_id=dev, device_id_type=MESH,
        )

    def along_z(self, it, k):
        return self.copy(it, it.source(self.d), it.place(self.f, self.d), k - 1, k - 1, (self.d, self.to(k)))

    def to_x(self, it, k):
        ref = it.place(self.origin(k), self.d)
        return self.copy(it, ref, ref, 2 + k, 2 + k, (self.dx, self.f))

    def to_y(self, it, k):
        ref = it.place(self.origin(k), self.d)
        return self.copy(it, ref, ref, 5 + k, 5 + k, (self.dy, self.f))

    def diag_y(self, it, k):
        ref = it.place(self.origin(k), self.dx, 0)
        return self.copy(it, ref, ref, 8 + k, 8 + k, (self.dy, self.f))

    def diag_x(self, it, k):
        ref = it.place(self.origin(k), self.dy, 1)
        return self.copy(it, ref, ref, 11 + k, 11 + k, (self.dx, self.f))

    def to_core(self, it, k):
        ref = it.place(self.origin(k))
        return self.copy(it, ref, ref, 14 + k, 14 + k, (self.d, self.sib))

    def own_copy(self, it):
        return self.copy(it, it.own(), it.place(self.f), 18, 18, (self.d, self.sib))

    def arrived(self, it, ref, r):
        self.copy(it, ref, ref, 0, r, (self.d, self.f)).wait_recv()

    def barrier(self, peers):
        sem = pltpu.get_barrier_semaphore()
        for peer in peers:
            pl.semaphore_signal(sem, inc=1, device_id=peer, device_id_type=MESH)
        pl.semaphore_wait(sem, len(peers))

    def send_z(self, its, ks=PLANES):
        for k in ks:
            for it in its:
                self.along_z(it, k).start()

    def a2(self, its, ks=PLANES):
        for k in ks:
            for it in its:
                self.arrived(it, it.place(self.origin(k), self.d), k - 1)
                self.to_x(it, k).start()
                self.to_y(it, k).start()

    def a3(self, its, ks=PLANES):
        for k in ks:
            for it in its:
                self.arrived(it, it.place(self.origin(k), self.dx), 2 + k)
                self.diag_y(it, k).start()
                self.arrived(it, it.place(self.origin(k), self.dy), 5 + k)
                self.diag_x(it, k).start()

    def a4(self, its, ks=PLANES):
        for k in ks:
            for it in its:
                self.arrived(it, it.place(self.origin(k), self.dd, 0), 8 + k)
                self.arrived(it, it.place(self.origin(k), self.dd, 1), 11 + k)
                self.to_core(it, k).start()

    def a5(self, its, ks=PLANES):
        for k in ks:
            for it in its:
                self.arrived(it, it.place(self.plane(k) * 2 + 1 - self.core), 14 + k)

    def from_core(self, its):
        for it in its:
            self.arrived(it, it.place(self.sib), 18)

    def sent(self, its):
        for it in its:
            for k in PLANES:
                for make in (self.along_z, self.to_x, self.to_y, self.diag_y, self.diag_x, self.to_core):
                    make(it, k).wait_send()
            self.own_copy(it).wait_send()


def scores(tiles, slots, low, j):
    qn, qp, kn, _ = tiles
    t = j // 2
    keep = low if j % 2 == 0 else jnp.logical_not(low)
    q_tile = jnp.concatenate([qn[t], qp[j // PE_TILE]], axis=1)
    k_tile = jnp.concatenate([jnp.where(keep, kn[t], 0), slots[j % PE_TILE]], axis=1)
    return lax.dot_general(k_tile, q_tile, (((1,), (1,)), ((), ())), preferred_element_type=jnp.float32)


def softmax(s, diag, zero, scale):
    half = s.shape[0] // 2
    left = jnp.where(diag, s[:half, :half], MASKED)
    up = s[:half, half:]
    right = jnp.where(diag, s[half:, half:], MASKED)
    m_l = jnp.max(left, axis=0, keepdims=True) * scale
    m_r = jnp.max(jnp.maximum(up, right), axis=0, keepdims=True) * scale
    e_l = jnp.exp2(left * scale - m_l)
    e_u = jnp.exp2(up * scale - m_r)
    e_r = jnp.exp2(right * scale - m_r)
    r_l = 1.0 / jnp.sum(e_l, axis=0, keepdims=True)
    r_r = 1.0 / jnp.sum(e_u + e_r, axis=0, keepdims=True)
    p_top = jnp.concatenate([(e_l * r_l).astype(jnp.bfloat16), (e_u * r_r).astype(jnp.bfloat16)], axis=1)
    p_bot = jnp.concatenate([zero, (e_r * r_r).astype(jnp.bfloat16)], axis=1)
    return jnp.concatenate([p_top, p_bot], axis=0)


def pieces(cq, lat, wuq, wukv, g, cos, sin):
    w = 2 * LANES

    def tiles(x, weights, cols, n, pe=False):
        r = jnp.dot(x, weights[:, g * cols + n * w:g * cols + (n + 1) * w], preferred_element_type=jnp.float32)
        both = [r[:, :LANES], r[:, LANES:]]
        return [(rotate(t, cos, sin) if pe else t).astype(jnp.bfloat16) for t in both]

    n_q, n_kv = Q_COLS // w, KV_COLS // w
    return [functools.partial(tiles, cq, wuq, Q_COLS, n, n == n_q - 1) for n in range(n_q)] + [
        functools.partial(tiles, lat, wukv, KV_COLS, n) for n in range(n_kv)
    ]


def arrange_tiles(made):
    flat = [t for pair in made for t in pair]
    n = GROUP // 2
    m = n + GROUP // PE_TILE
    return flat[:n], flat[n:m], flat[m:m + n], [t.T for t in flat[m + n:]]


def attend(cq, lat, rt, cq_next, lat_next, start, wuq, wukv, cos, sin, hold, o_ref):
    n_groups = wuq.shape[1] // Q_COLS
    scale = (NOPE + ROPE) ** -0.5 * LOG2E
    seq_len = cq.shape[0]
    half = seq_len // 2
    low = lax.broadcasted_iota(jnp.int32, (1, LANES), 1) < NOPE
    diag = lax.broadcasted_iota(jnp.int32, (half, half), 0) <= lax.broadcasted_iota(jnp.int32, (half, half), 1)
    zero = jnp.zeros((half, half), jnp.bfloat16)
    slots = slot_masks(rt)
    n_pieces = hold.shape[0] // 2

    def put(n, made):
        for m, t in enumerate(made):
            hold[2 * n + m] = t

    @pl.when(start)
    def _():
        for n, make in enumerate(pieces(cq, lat, wuq, wukv, 0, cos, sin)):
            put(n, make())

    tiles = {0: arrange_tiles([[hold[2 * n], hold[2 * n + 1]] for n in range(n_pieces)])}
    total = n_groups * GROUP
    s, p, outs = {}, {}, {}
    for u in range(-AHEAD, total + 1):
        g, j = divmod(u, GROUP)
        if u >= 0 and u < total:
            p[u] = softmax(s.pop(u), diag, zero, scale)
            if j == 0:
                made = []
                if g + 1 < n_groups:
                    todo = pieces(cq, lat, wuq, wukv, g + 1, cos, sin)
                else:
                    todo = pieces(cq_next, lat_next, wuq, wukv, 0, cos, sin)
            if j < SPREAD:
                for n in range(j * n_pieces // SPREAD, (j + 1) * n_pieces // SPREAD):
                    made.append(todo[n]())
                if len(made) == n_pieces and g + 1 < n_groups:
                    tiles[g + 1] = arrange_tiles(made)
                elif len(made) == n_pieces:
                    for n, m in enumerate(made):
                        put(n, m)
        if u + AHEAD < total:
            v = u + AHEAD
            s[v] = scores(tiles[v // GROUP], slots, low, v % GROUP)
        if u >= 1:
            h = u - 1
            hj = h % GROUP
            vt = tiles[h // GROUP][3][hj // 2][hj % 2 * VDIM:(hj % 2 + 1) * VDIM]
            outs[h] = jnp.dot(vt, p.pop(h), preferred_element_type=jnp.float32).astype(jnp.bfloat16)
            if h % 2 == 1:
                pair = jnp.concatenate([outs.pop(h - 1), outs.pop(h)], axis=0)
                o_ref[0, :, h // 2 * LANES:(h // 2 + 1) * LANES] = pair.T


def slot_masks(rt):
    lane = lax.broadcasted_iota(jnp.int32, (1, LANES), 1)
    slot = lax.rem(lane, LANES // 2) // HALF
    return [jnp.where(slot == j, rt, 0) for j in range(PE_TILE)]


def core_kernel(
    n_prompts, x_ref, gs_ref, dq_s, dkv_s, uq_s, ukv_s, out_s, cos_ref, sin_ref,
    c_all, r_ref, oa_ref, ob_ref, wout_ref,
    wdq, wdkv, wuqa, wuqb, wukva, wukvb, gains, gvec, a_all, acc, cq_all, rt_all, stage, hold,
    send_sem, recv_sem, g_send, g_recv, local_sem,
):
    i = pl.program_id(0)
    net = Net(send_sem, recv_sem)
    d, f = net.d, net.f
    n_a, m_a = wuqa.shape[1], wukva.shape[1]
    todo = [
        (dkv_s, 0, wdkv), (dq_s, 0, wdq), (ukv_s, 0, wukva), (uq_s, 0, wuqa),
        (ukv_s, m_a, wukvb), (uq_s, n_a, wuqb), (out_s, 0, wout_ref),
    ]
    items = [Item(n, shard, col, full.shape[1], full) for n, (shard, col, full) in enumerate(todo)]
    down, first, rest, last = items[:2], items[2:4], items[4:6], items[6:]
    wo = items[6]
    others = range(1, 8)

    def keep(it):
        return pltpu.make_async_copy(it.own(), stage if it is wo else it.place(f), local_sem.at[it.index])

    def keep_out():
        return pltpu.make_async_copy(stage, wo.place(f), local_sem.at[7])

    def keep_gain():
        return pltpu.make_async_copy(gs_ref, gains.at[f], local_sem.at[8])

    def gain_copy(j):
        return pltpu.make_async_remote_copy(
            src_ref=gs_ref, dst_ref=gains.at[f], send_sem=g_send.at[j - 1], recv_sem=g_recv.at[j - 1],
            device_id=(d, lax.rem(f + j, 8)), device_id_type=MESH,
        )

    @pl.when(i == 0)
    def _():
        net.barrier([(net.dx, f), (net.dy, f)] + [(d, lax.rem(f + j, 8)) for j in others])
        for j in others:
            gain_copy(j).start()
        keep_gain().start()
        for it in down:
            net.own_copy(it).start()
            keep(it).start()
        net.send_z(down)
        for it in items[2:]:
            net.own_copy(it).start()
            keep(it).start()
        for j in others:
            gain_copy(j).wait_recv()
        keep_gain().wait()
        total = jnp.sum(gains[...], axis=0)
        for t in range(gvec.shape[1] // LANES):
            gvec[:, t * LANES:(t + 1) * LANES] = total[t:t + 1, :]
        for it in down:
            keep(it).wait()
        net.from_core(down)

    d_model, q_rank, kv_rank = x_ref.shape[-1], cq_all.shape[-1], c_all.shape[-1]
    seq_len = x_ref.shape[1]
    k_rows = d_model // 4
    half = n_prompts // 2
    c1 = n_prompts
    c2 = c1 + half
    fin = c2 + half
    pa = fin + half
    pb = pa + n_prompts
    end = pb + n_prompts - 1
    one, two, three = ((k,) for k in PLANES)

    @pl.when(i == 1)
    def _():
        keep(wo).wait()
        keep_out().start()

    def ready(its):
        for it in its:
            (keep_out() if it is wo else keep(it)).wait()
        net.from_core(its)
        net.a5(its)

    plan = [
        (1, [(net.send_z, first, one)]),
        (2, [(net.send_z, rest, one)]),
        (3, [(net.send_z, first, three)]),
        (5, [(net.a2, down, one), (net.send_z, first, two)]),
        (6, [(net.a3, down, one)]),
        (7, [(net.a2, down, two)]),
        (8, [(net.a4, down, one), (net.a2, down, three), (net.a5, down, one), (net.a3, down, two)]),
        (9, [(net.a2, first, one)]),
        (10, [(net.send_z, rest, three), (net.send_z, last, one)]),
        (11, [(net.a4, down, two), (net.a3, down, three)]),
        (12, [(net.a2, first, three), (net.a3, first, one), (net.a5, down, two), (net.send_z, rest, two)]),
        (13, [(net.a2, first, two), (net.a2, rest, one), (net.a4, down, three)]),
        (15, [(net.a3, first, two), (net.a5, down, three)]),
        (16, [(net.a4, first, one), (net.a3, first, three), (net.a2, rest, three)]),
        (17, [(net.a4, first, two)]),
        (19, [(net.a4, first, three), (net.a3, rest, three)]),
        (20, [(net.send_z, last, two), (net.a2, rest, two)]),
        (21, [(net.a3, rest, one)]),
        (22, [(net.a2, last, one)]),
        (24, [(net.a4, rest, one), (net.send_z, last, three)]),
        (25, [(net.a3, rest, two), (net.a4, rest, three)]),
        (27, [(net.a4, rest, two), (net.a2, last, two)]),
        (28, [(net.a3, last, one)]),
        (29, [(net.a2, last, three)]),
        (31, [(net.a3, last, two)]),
        (32, [(net.a4, last, one)]),
        (33, [(net.a3, last, three)]),
        (34, [(net.a4, last, two)]),
        (35, [(net.a4, last, three)]),
    ]
    for step, acts in plan:
        @pl.when(i == step)
        def _(acts=acts):
            for act, its, ks in acts:
                act(its, ks)

    for step, its in ((pa, first), (pb, rest)):
        @pl.when(i == step)
        def _(its=its):
            ready(its)

    def partial_sums(p, n, k):
        rows = pl.ds(pl.multiple_of(net.plane(k) * k_rows, LANES), k_rows)
        a = a_all[pl.ds(p, n), :, rows].reshape(n * seq_len, k_rows)
        qd = jnp.dot(a, wdq[rows], preferred_element_type=jnp.float32)
        kd = jnp.dot(a, wdkv[rows], preferred_element_type=jnp.float32)
        if k > 0:
            old = acc[pl.ds(p, n)].reshape(n * seq_len, q_rank + kv_rank + LANES)
            qd += old[:, :q_rank]
            kd += old[:, q_rank:]
        return qd, kd

    def add_plane(p, n, k):
        qd, kd = partial_sums(p, n, k)
        acc[pl.ds(p, n), :, :q_rank] = qd.reshape(n, seq_len, q_rank)
        acc[pl.ds(p, n), :, q_rank:] = kd.reshape(n, seq_len, kv_rank + LANES)

    @pl.when(i < c1)
    def _():
        x = x_ref[0].astype(jnp.float32)
        a_all[i] = (x * inv_rms(x) * gvec[:, :d_model]).astype(jnp.bfloat16)
        add_plane(i, 1, 0)

    @pl.when(jnp.logical_and(i >= c1, i < c2))
    def _():
        add_plane((i - c1) * 2, 2, 1)

    @pl.when(jnp.logical_and(i >= c2, i < fin))
    def _():
        add_plane((i - c2) * 2, 2, 2)

    @pl.when(jnp.logical_and(i >= fin, i < pa))
    def _():
        p = (i - fin) * 2
        qd, kd = partial_sums(p, 2, 3)
        cq = (qd * inv_rms(qd) * gvec[:, d_model:d_model + q_rank]).astype(jnp.bfloat16)
        cq_all[pl.ds(p, 2)] = cq.reshape(2, seq_len, q_rank)
        lat = kd[:, :kv_rank]
        lat = (lat * inv_rms(lat) * gvec[:, d_model + q_rank:]).astype(jnp.bfloat16)
        c_all[pl.ds(p, 2)] = lat.reshape(2, seq_len, kv_rank)
        for n in range(2):
            pe = kd[n * seq_len:(n + 1) * seq_len, kv_rank:]
            rt = rotate(pe, cos_ref[...], sin_ref[...]).astype(jnp.bfloat16)
            rt_all[p + n] = rt
            rt_t = rt.T
            r_ref[p + n] = jnp.concatenate([rt_t[:HALF], rt_t[LANES // 2:LANES // 2 + HALF]], axis=0)

    def attend_step(p, wuq, wukv, o_ref):
        after = jnp.minimum(p + 1, n_prompts - 1)
        attend(
            cq_all[p], c_all[p], rt_all[p], cq_all[after], c_all[after], p == 0,
            wuq, wukv, cos_ref[...], sin_ref[...], hold, o_ref,
        )

    @pl.when(jnp.logical_and(i >= pa, i < pb))
    def _():
        attend_step(i - pa, wuqa, wukva, oa_ref)

    @pl.when(i >= pb)
    def _():
        attend_step(i - pb, wuqb, wukvb, ob_ref)

    @pl.when(i == end)
    def _():
        ready(last)
        for j in others:
            gain_copy(j).wait_send()
        net.sent(items)


def out_kernel(x_ref, oa_ref, ob_ref, w_hbm, c_in, r_in, y_ref, c_out, r_out, w, sem):
    step = 512
    n_steps = y_ref.shape[1] // step
    first = pl.program_id(0) == 0
    cols = [slice(n * step, (n + 1) * step) for n in range(n_steps)]
    load = [pltpu.make_async_copy(w_hbm.at[:, c], w.at[:, c], sem.at[n]) for n, c in enumerate(cols)]

    @pl.when(first)
    def _():
        for part in load:
            part.start()

    oa, ob = oa_ref[...], ob_ref[...]
    n_a = oa.shape[1]
    c_out[...] = c_in[...]
    r_out[...] = r_in[...]
    for part, c in zip(load, cols):
        @pl.when(first)
        def _(part=part):
            part.wait()

        acc = jnp.dot(oa, w[:n_a, c], preferred_element_type=jnp.float32)
        acc += jnp.dot(ob, w[n_a:, c], preferred_element_type=jnp.float32)
        y_ref[:, c] = (x_ref[:, c].astype(jnp.float32) + acc).astype(jnp.bfloat16)


def whole(shape):
    return pl.BlockSpec(shape, lambda i: (0,) * len(shape))


def solution(mesh):
    n_fsdp = mesh.shape['fsdp']

    def local_block(x, g1, wdq, gq, wuq, wdkv, gkv, wukv, wout):
        n_p, seq_len, d_model = x.shape
        kv_rank, q_rank = gkv.shape[0] * n_fsdp, wdq.shape[1]
        cos_np, sin_np = rope_tiles(seq_len)
        cos, sin = jnp.asarray(cos_np), jnp.asarray(sin_np)
        me = lax.axis_index('fsdp')
        spread = [
            lax.dynamic_update_slice(jnp.zeros(g.shape[0] * n_fsdp, jnp.float32), g.astype(jnp.float32), (me * g.shape[0],))
            for g in (g1, gq, gkv)
        ]
        n_gain = d_model + q_rank + kv_rank
        gs = jnp.concatenate(spread + [jnp.zeros(GAIN_ROWS * LANES - n_gain, jnp.float32)]).reshape(GAIN_ROWS, LANES)
        shards = [wdq, arrange_dkv(wdkv, kv_rank), arrange_q(wuq), arrange_kv(wukv), wout]
        full = lambda w, cols: pltpu.VMEM((w.shape[0] * n_fsdp, cols), jnp.bfloat16)
        o_cols = GROUP * VDIM
        n_groups = wuq.shape[1] // Q_COLS
        first, rest = GROUPS_FIRST, n_groups - GROUPS_FIRST
        last = n_p - 1
        pa = 2 * n_p + n_p // 2
        blk = lambda cols, lag: pl.BlockSpec((1, seq_len, cols), lambda i: (jnp.clip(i - lag, 0, last), 0, 0))
        out = lambda cols: jax.ShapeDtypeStruct((n_p, seq_len, cols), jnp.bfloat16)
        r_shape = jax.ShapeDtypeStruct((n_p, ROPE, seq_len), jnp.bfloat16)
        hbm = pl.BlockSpec(memory_space=pl.ANY)
        c, r, oa, ob, wout_all = pl.pallas_call(
            functools.partial(core_kernel, n_p),
            grid=(4 * n_p + n_p // 2,),
            in_specs=[blk(d_model, 0)] + [hbm] * 6 + [whole(cos.shape)] * 2,
            out_specs=[
                whole((n_p, seq_len, kv_rank)), whole((n_p, ROPE, seq_len)),
                blk(first * o_cols, pa), blk(rest * o_cols, pa + n_p), hbm,
            ],
            out_shape=[
                out(kv_rank), r_shape, out(first * o_cols), out(rest * o_cols),
                jax.ShapeDtypeStruct((wout.shape[0] * n_fsdp, wout.shape[1]), jnp.bfloat16),
            ],
            scratch_shapes=[
                full(wdq, q_rank), full(wdkv, kv_rank + LANES),
                full(wuq, first * Q_COLS), full(wuq, rest * Q_COLS),
                full(wukv, first * KV_COLS), full(wukv, rest * KV_COLS),
                pltpu.VMEM((n_fsdp, GAIN_ROWS, LANES), jnp.float32),
                pltpu.VMEM((1, n_gain), jnp.float32),
                pltpu.VMEM((n_p, seq_len, d_model), jnp.bfloat16),
                pltpu.VMEM((n_p, seq_len, q_rank + kv_rank + LANES), jnp.float32),
                pltpu.VMEM((n_p, seq_len, q_rank), jnp.bfloat16),
                pltpu.VMEM((n_p, seq_len, LANES), jnp.bfloat16),
                pltpu.VMEM(wout.shape, jnp.bfloat16),
                pltpu.VMEM(((Q_COLS + KV_COLS) // LANES, seq_len, LANES), jnp.bfloat16),
                pltpu.SemaphoreType.DMA((7, N_COPIES)),
                pltpu.SemaphoreType.DMA((7, N_COPIES)),
                pltpu.SemaphoreType.DMA((7,)),
                pltpu.SemaphoreType.DMA((7,)),
                pltpu.SemaphoreType.DMA((9,)),
            ],
            compiler_params=pltpu.CompilerParams(
                vmem_limit_bytes=VMEM_LIMIT, dimension_semantics=("arbitrary",), collective_id=0, has_side_effects=True,
            ),
            name="core",
        )(x, gs, *shards, cos, sin)
        rows = 512
        tile = lambda cols: pl.BlockSpec((rows, cols), lambda i: (i, 0))
        r_tile = pl.BlockSpec((rows // seq_len, ROPE, seq_len), lambda i: (i, 0, 0))
        flat = lambda v: v.reshape(n_p * seq_len, v.shape[-1])
        flat_out = lambda cols: jax.ShapeDtypeStruct((n_p * seq_len, cols), jnp.bfloat16)
        y, c, r = pl.pallas_call(
            out_kernel,
            grid=(n_p * seq_len // rows,),
            in_specs=[tile(d_model), tile(oa.shape[-1]), tile(ob.shape[-1]), hbm, tile(kv_rank), r_tile],
            out_specs=[tile(d_model), tile(kv_rank), r_tile],
            out_shape=[flat_out(d_model), flat_out(kv_rank), r_shape],
            scratch_shapes=[pltpu.VMEM(wout_all.shape, jnp.bfloat16), pltpu.SemaphoreType.DMA((8,))],
            compiler_params=pltpu.CompilerParams(vmem_limit_bytes=VMEM_LIMIT, dimension_semantics=("arbitrary",)),
            name="project",
        )(flat(x), flat(oa), flat(ob), wout_all, flat(c), r)
        back = lambda v: v.reshape(n_p, seq_len, v.shape[-1])
        return back(y), back(c), jnp.swapaxes(r, 1, 2)

    batch, row, mat = P(('dp', 'fsdp')), P('fsdp'), P('fsdp', None)
    return jax.shard_map(
        local_block,
        mesh=mesh,
        in_specs=(batch, row, mat, row, mat, mat, row, mat, mat),
        out_specs=(batch, batch, batch),
        check_vma=False,
    )
```

```python
import functools

import jax
import jax.numpy as jnp
import numpy as np
from jax import lax
from jax.experimental import pallas as pl
from jax.experimental.pallas import tpu as pltpu
from jax.sharding import PartitionSpec as P

EPSILON = 1e-6
ROPE_THETA = 10000.0
LOG2E = 1.4426950408889634
VMEM_LIMIT = 64000 * 1024

NOPE, ROPE, VDIM = 64, 32, 64
HALF = ROPE // 2
GROUP = 8
PE_TILE = 4
LANES = 128
Q_COLS, KV_COLS = GROUP * (NOPE + ROPE), GROUP * (NOPE + VDIM)
AHEAD, SPREAD = 2, 6
MASKED = -1e30


def rope_tiles(seq_len):
    inv_freq = ROPE_THETA ** (-2.0 * np.arange(HALF) / ROPE)
    angles = np.arange(seq_len)[:, None] * inv_freq[None, :]
    cos = np.tile(np.cos(angles), (1, LANES // HALF))
    sin = np.tile(np.sin(angles), (1, PE_TILE))
    return cos.astype(np.float32), np.concatenate([-sin, sin], axis=1).astype(np.float32)


def inv_rms(v):
    return lax.rsqrt(jnp.mean(v * v, axis=-1, keepdims=True) + EPSILON)


def rotate(tile, cos, sin):
    return tile * cos + pltpu.roll(tile, LANES // 2, 1) * sin


MESH = pl.DeviceIdType.MESH
GAIN_ROWS = 32
GROUPS_FIRST = 2
N_COPIES = 19
PLANES = (1, 2, 3)


class Item:
    def __init__(self, index, shard, col, cols, full):
        self.index, self.shard, self.col, self.cols, self.full = index, shard, col, cols, full
        self.rows = shard.shape[0]
        if (self.rows // 4) % 16 == 0:
            self.q_rows, self.q_cols = self.rows // 4, cols
        elif (cols // 4) % LANES == 0 and self.rows == 32:
            self.q_rows, self.q_cols = self.rows, cols // 4
        else:
            self.q_rows, self.q_cols = self.rows // 2, cols // 2
        if self.q_rows == self.rows:
            n = self.q_rows // 2
            self.halves = [(0, n, 0, self.q_cols), (n, n, 0, self.q_cols)]
        else:
            n = -(-self.q_cols // (2 * LANES)) * LANES
            self.halves = [(0, self.q_rows, 0, n), (0, self.q_rows, n, self.q_cols - n)]

    def quarter(self, q):
        per_row = self.cols // self.q_cols
        return (q // per_row) * self.q_rows, lax.rem(q, per_row) * self.q_cols

    def source(self, q):
        r, c = self.quarter(q)
        return self.shard.at[pl.ds(pl.multiple_of(r, 16), self.q_rows), pl.ds(pl.multiple_of(self.col + c, LANES), self.q_cols)]

    def own(self):
        return self.shard.at[:, pl.ds(self.col, self.cols)]

    def place(self, f, q=None, half=None):
        r, c = (0, 0) if q is None else self.quarter(q)
        r = f * self.rows + r
        if q is None:
            n_r, n_c = self.rows, self.cols
        elif half is None:
            n_r, n_c = self.q_rows, self.q_cols
        else:
            dr, n_r, dc, n_c = self.halves[half]
            r, c = r + dr, c + dc
        if n_c == self.cols:
            return self.full.at[pl.ds(pl.multiple_of(r, 16), n_r)]
        return self.full.at[pl.ds(pl.multiple_of(r, 16), n_r), pl.ds(pl.multiple_of(c, LANES), n_c)]


class Net:
    def __init__(self, send_sem, recv_sem):
        self.send_sem, self.recv_sem = send_sem, recv_sem
        self.d, self.f = lax.axis_index('dp'), lax.axis_index('fsdp')
        self.z, self.core = self.f // 2, lax.rem(self.f, 2)
        self.dx = lax.rem(self.d + 2, 4)
        self.dy = self.d + 1 - 2 * lax.rem(self.d, 2)
        self.dd = lax.rem(self.dy + 2, 4)
        self.sib = self.z * 2 + 1 - self.core

    def to(self, k):
        return lax.rem(self.z + k, 4) * 2 + self.core

    def plane(self, k):
        return lax.rem(self.z + 4 - k, 4)

    def origin(self, k):
        return self.plane(k) * 2 + self.core

    def copy(self, it, src, dst, s, r, dev):
        return pltpu.make_async_remote_copy(
            src_ref=src, dst_ref=dst, send_sem=self.send_sem.at[it.index, s], recv_sem=self.recv_sem.at[it.index, r],
            device_id=dev, device_id_type=MESH,
        )

    def along_z(self, it, k):
        return self.copy(it, it.source(self.d), it.place(self.f, self.d), k - 1, k - 1, (self.d, self.to(k)))

    def to_x(self, it, k):
        ref = it.place(self.origin(k), self.d)
        return self.copy(it, ref, ref, 2 + k, 2 + k, (self.dx, self.f))

    def to_y(self, it, k):
        ref = it.place(self.origin(k), self.d)
        return self.copy(it, ref, ref, 5 + k, 5 + k, (self.dy, self.f))

    def diag_y(self, it, k):
        ref = it.place(self.origin(k), self.dx, 0)
        return self.copy(it, ref, ref, 8 + k, 8 + k, (self.dy, self.f))

    def diag_x(self, it, k):
        ref = it.place(self.origin(k), self.dy, 1)
        return self.copy(it, ref, ref, 11 + k, 11 + k, (self.dx, self.f))

    def to_core(self, it, k):
        ref = it.place(self.origin(k))
        return self.copy(it, ref, ref, 14 + k, 14 + k, (self.d, self.sib))

    def own_copy(self, it):
        return self.copy(it, it.own(), it.place(self.f), 18, 18, (self.d, self.sib))

    def arrived(self, it, ref, r):
        self.copy(it, ref, ref, 0, r, (self.d, self.f)).wait_recv()

    def barrier(self, peers):
        sem = pltpu.get_barrier_semaphore()
        for peer in peers:
            pl.semaphore_signal(sem, inc=1, device_id=peer, device_id_type=MESH)
        pl.semaphore_wait(sem, len(peers))

    def send_z(self, its, ks=PLANES):
        for k in ks:
            for it in its:
                self.along_z(it, k).start()

    def a2(self, its, ks=PLANES):
        for k in ks:
            for it in its:
                self.arrived(it, it.place(self.origin(k), self.d), k - 1)
                self.to_x(it, k).start()
                self.to_y(it, k).start()

    def a3(self, its, ks=PLANES):
        for k in ks:
            for it in its:
                self.arrived(it, it.place(self.origin(k), self.dx), 2 + k)
                self.diag_y(it, k).start()
                self.arrived(it, it.place(self.origin(k), self.dy), 5 + k)
                self.diag_x(it, k).start()

    def a4(self, its, ks=PLANES):
        for k in ks:
            for it in its:
                self.arrived(it, it.place(self.origin(k), self.dd, 0), 8 + k)
                self.arrived(it, it.place(self.origin(k), self.dd, 1), 11 + k)
                self.to_core(it, k).start()

    def a5(self, its, ks=PLANES):
        for k in ks:
            for it in its:
                self.arrived(it, it.place(self.plane(k) * 2 + 1 - self.core), 14 + k)

    def from_core(self, its):
        for it in its:
            self.arrived(it, it.place(self.sib), 18)

    def sent(self, its):
        for it in its:
            for k in PLANES:
                for make in (self.along_z, self.to_x, self.to_y, self.diag_y, self.diag_x, self.to_core):
                    make(it, k).wait_send()
            self.own_copy(it).wait_send()


def scores(tiles, slots, low, j):
    qn, qp, kn, _ = tiles
    t = j // 2
    keep = low if j % 2 == 0 else jnp.logical_not(low)
    q_tile = jnp.concatenate([qn[t], qp[j // PE_TILE]], axis=0)
    k_tile = jnp.concatenate([jnp.where(keep, kn[t], 0), slots[j % PE_TILE]], axis=1)
    return jnp.dot(k_tile, q_tile, preferred_element_type=jnp.float32)


def softmax(s, diag, zero, scale):
    half = s.shape[0] // 2
    left = jnp.where(diag, s[:half, :half], MASKED)
    up = s[:half, half:]
    right = jnp.where(diag, s[half:, half:], MASKED)
    m_l = jnp.max(left, axis=0, keepdims=True) * scale
    m_r = jnp.max(jnp.maximum(up, right), axis=0, keepdims=True) * scale
    e_l = jnp.exp2(left * scale - m_l)
    e_u = jnp.exp2(up * scale - m_r)
    e_r = jnp.exp2(right * scale - m_r)
    r_l = 1.0 / jnp.sum(e_l, axis=0, keepdims=True)
    r_r = 1.0 / jnp.sum(e_u + e_r, axis=0, keepdims=True)
    p_top = jnp.concatenate([(e_l * r_l).astype(jnp.bfloat16), (e_u * r_r).astype(jnp.bfloat16)], axis=1)
    p_bot = jnp.concatenate([zero, (e_r * r_r).astype(jnp.bfloat16)], axis=1)
    return jnp.concatenate([p_top, p_bot], axis=0)


def pieces(cq, lat, wuq, wukv, g, cos, sin):
    w = 2 * LANES

    def tiles(x, weights, cols, n, pe=False):
        r = jnp.dot(x, weights[:, g * cols + n * w:g * cols + (n + 1) * w], preferred_element_type=jnp.float32)
        both = [r[:, :LANES], r[:, LANES:]]
        return [(rotate(t, cos, sin) if pe else t).astype(jnp.bfloat16) for t in both]

    n_q, n_kv = Q_COLS // w, KV_COLS // w
    return [functools.partial(tiles, cq, wuq, Q_COLS, n, n == n_q - 1) for n in range(n_q)] + [
        functools.partial(tiles, lat, wukv, KV_COLS, n) for n in range(n_kv)
    ]


def arrange_tiles(made):
    flat = [t for pair in made for t in pair]
    n = GROUP // 2
    m = n + GROUP // PE_TILE
    turned = [t.T for t in flat[:m]]
    return turned[:n], turned[n:], flat[m:m + n], [t.T for t in flat[m + n:]]


def attend(cq, lat, rt, cq_next, lat_next, start, wuq, wukv, cos, sin, hold, o_ref):
    n_groups = wuq.shape[1] // Q_COLS
    scale = (NOPE + ROPE) ** -0.5 * LOG2E
    seq_len = cq.shape[0]
    half = seq_len // 2
    low = lax.broadcasted_iota(jnp.int32, (1, LANES), 1) < NOPE
    diag = lax.broadcasted_iota(jnp.int32, (half, half), 0) <= lax.broadcasted_iota(jnp.int32, (half, half), 1)
    zero = jnp.zeros((half, half), jnp.bfloat16)
    slots = slot_masks(rt)
    n_pieces = hold.shape[0] // 2

    def put(n, made):
        for m, t in enumerate(made):
            hold[2 * n + m] = t

    @pl.when(start)
    def _():
        for n, make in enumerate(pieces(cq, lat, wuq, wukv, 0, cos, sin)):
            put(n, make())

    tiles = {0: arrange_tiles([[hold[2 * n], hold[2 * n + 1]] for n in range(n_pieces)])}
    total = n_groups * GROUP
    s, p, outs = {}, {}, {}
    for u in range(-AHEAD, total + 1):
        g, j = divmod(u, GROUP)
        if u >= 0 and u < total:
            p[u] = softmax(s.pop(u), diag, zero, scale)
            if j == 0:
                made = []
                if g + 1 < n_groups:
                    todo = pieces(cq, lat, wuq, wukv, g + 1, cos, sin)
                else:
                    todo = pieces(cq_next, lat_next, wuq, wukv, 0, cos, sin)
            if j < SPREAD:
                for n in range(j * n_pieces // SPREAD, (j + 1) * n_pieces // SPREAD):
                    made.append(todo[n]())
                if len(made) == n_pieces and g + 1 < n_groups:
                    tiles[g + 1] = arrange_tiles(made)
                elif len(made) == n_pieces:
                    for n, m in enumerate(made):
                        put(n, m)
        if u + AHEAD < total:
            v = u + AHEAD
            s[v] = scores(tiles[v // GROUP], slots, low, v % GROUP)
        if u >= 1:
            h = u - 1
            hj = h % GROUP
            vt = tiles[h // GROUP][3][hj // 2][hj % 2 * VDIM:(hj % 2 + 1) * VDIM]
            outs[h] = jnp.dot(vt, p.pop(h), preferred_element_type=jnp.float32).astype(jnp.bfloat16)
            if h % 2 == 1:
                pair = jnp.concatenate([outs.pop(h - 1), outs.pop(h)], axis=0)
                o_ref[0, :, h // 2 * LANES:(h // 2 + 1) * LANES] = pair.T


def slot_masks(rt):
    lane = lax.broadcasted_iota(jnp.int32, (1, LANES), 1)
    slot = lax.rem(lane, LANES // 2) // HALF
    return [jnp.where(slot == j, rt, 0) for j in range(PE_TILE)]


def core_kernel(
    n_prompts, x_ref, gs_ref, dq_s, dkv_s, uq_s, ukv_s, out_s, cos_ref, sin_ref,
    c_all, r_ref, oa_ref, ob_ref, wout_ref,
    wdq, wdkv, wuqa, wuqb, wukva, wukvb, gains, gvec, a_all, acc, cq_all, rt_all, stage, hold,
    send_sem, recv_sem, g_send, g_recv, local_sem,
):
    i = pl.program_id(0)
    net = Net(send_sem, recv_sem)
    d, f = net.d, net.f
    n_a, m_a = wuqa.shape[1], wukva.shape[1]
    todo = [
        (dkv_s, 0, wdkv), (dq_s, 0, wdq), (ukv_s, 0, wukva), (uq_s, 0, wuqa),
        (ukv_s, m_a, wukvb), (uq_s, n_a, wuqb), (out_s, 0, wout_ref),
    ]
    items = [Item(n, shard, col, full.shape[1], full) for n, (shard, col, full) in enumerate(todo)]
    down, first, rest, last = items[:2], items[2:4], items[4:6], items[6:]
    wo = items[6]
    others = range(1, 8)

    def keep(it):
        return pltpu.make_async_copy(it.own(), stage if it is wo else it.place(f), local_sem.at[it.index])

    def keep_out():
        return pltpu.make_async_copy(stage, wo.place(f), local_sem.at[7])

    def keep_gain():
        return pltpu.make_async_copy(gs_ref, gains.at[f], local_sem.at[8])

    def gain_copy(j):
        return pltpu.make_async_remote_copy(
            src_ref=gs_ref, dst_ref=gains.at[f], send_sem=g_send.at[j - 1], recv_sem=g_recv.at[j - 1],
            device_id=(d, lax.rem(f + j, 8)), device_id_type=MESH,
        )

    @pl.when(i == 0)
    def _():
        net.barrier([(net.dx, f), (net.dy, f)] + [(d, lax.rem(f + j, 8)) for j in others])
        for j in others:
            gain_copy(j).start()
        keep_gain().start()
        for it in down:
            net.own_copy(it).start()
            keep(it).start()
        net.send_z(down)
        for it in items[2:]:
            net.own_copy(it).start()
            keep(it).start()
        for j in others:
            gain_copy(j).wait_recv()
        keep_gain().wait()
        total = jnp.sum(gains[...], axis=0)
        for t in range(gvec.shape[1] // LANES):
            gvec[:, t * LANES:(t + 1) * LANES] = total[t:t + 1, :]
        for it in down:
            keep(it).wait()
        net.from_core(down)

    d_model, q_rank, kv_rank = x_ref.shape[-1], cq_all.shape[-1], c_all.shape[-1]
    seq_len = x_ref.shape[1]
    k_rows = d_model // 4
    half = n_prompts // 2
    c1 = n_prompts
    c2 = c1 + half
    fin = c2 + half
    pa = fin + half
    pb = pa + n_prompts
    end = pb + n_prompts - 1
    one, two, three = ((k,) for k in PLANES)

    @pl.when(i == 1)
    def _():
        keep(wo).wait()
        keep_out().start()

    def ready(its):
        for it in its:
            (keep_out() if it is wo else keep(it)).wait()
        net.from_core(its)
        net.a5(its)

    plan = [
        (1, [(net.send_z, first, one)]),
        (2, [(net.send_z, rest, one)]),
        (3, [(net.send_z, first, three)]),
        (5, [(net.a2, down, one), (net.send_z, first, two)]),
        (6, [(net.a3, down, one)]),
        (7, [(net.a2, down, two)]),
        (8, [(net.a4, down, one), (net.a2, down, three), (net.a5, down, one), (net.a3, down, two)]),
        (9, [(net.a2, first, one)]),
        (10, [(net.send_z, rest, three), (net.send_z, last, one)]),
        (11, [(net.a4, down, two), (net.a3, down, three)]),
        (12, [(net.a2, first, three), (net.a3, first, one), (net.a5, down, two), (net.send_z, rest, two)]),
        (13, [(net.a2, first, two), (net.a2, rest, one), (net.a4, down, three)]),
        (15, [(net.a3, first, two), (net.a5, down, three)]),
        (16, [(net.a4, first, one), (net.a3, first, three), (net.a2, rest, three)]),
        (17, [(net.a4, first, two)]),
        (19, [(net.a4, first, three), (net.a3, rest, three)]),
        (20, [(net.send_z, last, two), (net.a2, rest, two)]),
        (21, [(net.a3, rest, one)]),
        (22, [(net.a2, last, one)]),
        (24, [(net.a4, rest, one), (net.send_z, last, three)]),
        (25, [(net.a3, rest, two), (net.a4, rest, three)]),
        (27, [(net.a4, rest, two), (net.a2, last, two)]),
        (28, [(net.a3, last, one)]),
        (29, [(net.a2, last, three)]),
        (31, [(net.a3, last, two)]),
        (32, [(net.a4, last, one)]),
        (33, [(net.a3, last, three)]),
        (34, [(net.a4, last, two)]),
        (35, [(net.a4, last, three)]),
    ]
    for step, acts in plan:
        @pl.when(i == step)
        def _(acts=acts):
            for act, its, ks in acts:
                act(its, ks)

    for step, its in ((pa, first), (pb, rest)):
        @pl.when(i == step)
        def _(its=its):
            ready(its)

    def partial_sums(p, n, k):
        rows = pl.ds(pl.multiple_of(net.plane(k) * k_rows, LANES), k_rows)
        a = a_all[pl.ds(p, n), :, rows].reshape(n * seq_len, k_rows)
        qd = jnp.dot(a, wdq[rows], preferred_element_type=jnp.float32)
        kd = jnp.dot(a, wdkv[rows], preferred_element_type=jnp.float32)
        if k > 0:
            old = acc[pl.ds(p, n)].reshape(n * seq_len, q_rank + kv_rank + LANES)
            qd += old[:, :q_rank]
            kd += old[:, q_rank:]
        return qd, kd

    def add_plane(p, n, k):
        qd, kd = partial_sums(p, n, k)
        acc[pl.ds(p, n), :, :q_rank] = qd.reshape(n, seq_len, q_rank)
        acc[pl.ds(p, n), :, q_rank:] = kd.reshape(n, seq_len, kv_rank + LANES)

    @pl.when(i < c1)
    def _():
        x = x_ref[0].astype(jnp.float32)
        a_all[i] = (x * inv_rms(x) * gvec[:, :d_model]).astype(jnp.bfloat16)
        add_plane(i, 1, 0)

    @pl.when(jnp.logical_and(i >= c1, i < c2))
    def _():
        add_plane((i - c1) * 2, 2, 1)

    @pl.when(jnp.logical_and(i >= c2, i < fin))
    def _():
        add_plane((i - c2) * 2, 2, 2)

    @pl.when(jnp.logical_and(i >= fin, i < pa))
    def _():
        p = (i - fin) * 2
        qd, kd = partial_sums(p, 2, 3)
        cq = (qd * inv_rms(qd) * gvec[:, d_model:d_model + q_rank]).astype(jnp.bfloat16)
        cq_all[pl.ds(p, 2)] = cq.reshape(2, seq_len, q_rank)
        lat = kd[:, :kv_rank]
        lat = (lat * inv_rms(lat) * gvec[:, d_model + q_rank:]).astype(jnp.bfloat16)
        c_all[pl.ds(p, 2)] = lat.reshape(2, seq_len, kv_rank)
        for n in range(2):
            pe = kd[n * seq_len:(n + 1) * seq_len, kv_rank:]
            rt = rotate(pe, cos_ref[...], sin_ref[...]).astype(jnp.bfloat16)
            rt_all[p + n] = rt
            rt_t = rt.T
            r_ref[p + n] = jnp.concatenate([rt_t[:HALF], rt_t[LANES // 2:LANES // 2 + HALF]], axis=0)

    def attend_step(p, wuq, wukv, o_ref):
        after = jnp.minimum(p + 1, n_prompts - 1)
        attend(
            cq_all[p], c_all[p], rt_all[p], cq_all[after], c_all[after], p == 0,
            wuq, wukv, cos_ref[...], sin_ref[...], hold, o_ref,
        )

    @pl.when(jnp.logical_and(i >= pa, i < pb))
    def _():
        attend_step(i - pa, wuqa, wukva, oa_ref)

    @pl.when(i >= pb)
    def _():
        attend_step(i - pb, wuqb, wukvb, ob_ref)

    @pl.when(i == end)
    def _():
        ready(last)
        for j in others:
            gain_copy(j).wait_send()
        net.sent(items)


def one_hot(source, n_rows):
    rows = lax.broadcasted_iota(jnp.int32, (n_rows, source.shape[1]), 0)
    return (rows == source).astype(jnp.float32).astype(jnp.bfloat16)


def pick(w, matrix):
    return jnp.dot(w, matrix, preferred_element_type=jnp.float32).astype(jnp.bfloat16)


def prepare_kernel(g1_ref, gq_ref, gkv_ref, wuq_ref, wukv_ref, wdkv_ref, gs_ref, uq_ref, ukv_ref, dkv_ref):
    f = lax.axis_index('fsdp')
    row = 0
    gs_ref[...] = jnp.zeros_like(gs_ref)
    for g in (g1_ref, gq_ref, gkv_ref):
        n = g.shape[1]
        for t in range(n * 8 // LANES):
            index = lax.broadcasted_iota(jnp.int32, (1, LANES), 1) + (t * LANES - f * n)
            gs_ref[row:row + 1, :] = jnp.dot(g[...], one_hot(index, n), preferred_element_type=jnp.float32)
            row += 1

    def column(n):
        return lax.broadcasted_iota(jnp.int32, (1, n), 1)

    c = column(Q_COLS)
    n_nope = GROUP * NOPE
    pe = c - n_nope
    head = pe // LANES * PE_TILE + lax.rem(pe, LANES // 2) // HALF
    pe = head * (NOPE + ROPE) + NOPE + lax.rem(pe, LANES) // (LANES // 2) * HALF + lax.rem(pe, HALF)
    order = one_hot(jnp.where(c < n_nope, c // NOPE * (NOPE + ROPE) + lax.rem(c, NOPE), pe), Q_COLS)
    for g in range(wuq_ref.shape[1] // Q_COLS):
        cols = slice(g * Q_COLS, (g + 1) * Q_COLS)
        uq_ref[:, cols] = pick(wuq_ref[:, cols], order)

    c = column(KV_COLS)
    part = lax.rem(c, n_nope)
    order = one_hot(part // NOPE * (NOPE + VDIM) + c // n_nope * NOPE + lax.rem(part, NOPE), KV_COLS)
    for g in range(wukv_ref.shape[1] // KV_COLS):
        cols = slice(g * KV_COLS, (g + 1) * KV_COLS)
        ukv_ref[:, cols] = pick(wukv_ref[:, cols], order)

    kv_rank = dkv_ref.shape[1] - LANES
    c = column(LANES)
    dkv_ref[:, :kv_rank] = wdkv_ref[:, :kv_rank]
    order = one_hot(c // (LANES // 2) * HALF + lax.rem(c, HALF), ROPE)
    dkv_ref[:, kv_rank:] = pick(wdkv_ref[:, kv_rank:], order)


def out_kernel(x_ref, oa_ref, ob_ref, w_hbm, c_in, r_in, y_ref, c_out, r_out, w, sem):
    step = 512
    n_steps = y_ref.shape[1] // step
    first = pl.program_id(0) == 0
    cols = [slice(n * step, (n + 1) * step) for n in range(n_steps)]
    load = [pltpu.make_async_copy(w_hbm.at[:, c], w.at[:, c], sem.at[n]) for n, c in enumerate(cols)]

    @pl.when(first)
    def _():
        for part in load:
            part.start()

    o = jnp.concatenate([oa_ref[...], ob_ref[...]], axis=1)
    c_out[...] = c_in[...]
    r_out[...] = r_in[...]
    for part, c in zip(load, cols):
        @pl.when(first)
        def _(part=part):
            part.wait()

        acc = jnp.dot(o, w[:, c], preferred_element_type=jnp.float32)
        y_ref[:, c] = (x_ref[:, c].astype(jnp.float32) + acc).astype(jnp.bfloat16)


def whole(shape):
    return pl.BlockSpec(shape, lambda i: (0,) * len(shape))


def solution(mesh):
    n_fsdp = mesh.shape['fsdp']

    def local_block(x, g1, wdq, gq, wuq, wdkv, gkv, wukv, wout):
        n_p, seq_len, d_model = x.shape
        kv_rank, q_rank = gkv.shape[0] * n_fsdp, wdq.shape[1]
        cos_np, sin_np = rope_tiles(seq_len)
        cos, sin = jnp.asarray(cos_np), jnp.asarray(sin_np)
        n_gain = d_model + q_rank + kv_rank
        like = lambda w, cols: jax.ShapeDtypeStruct((w.shape[0], cols), jnp.bfloat16)
        gs, uq, ukv, dkv = pl.pallas_call(
            prepare_kernel,
            out_shape=[
                jax.ShapeDtypeStruct((GAIN_ROWS, LANES), jnp.float32),
                like(wuq, wuq.shape[1]), like(wukv, wukv.shape[1]), like(wdkv, kv_rank + LANES),
            ],
            name="prepare",
        )(g1[None], gq[None], gkv[None], wuq, wukv, wdkv)
        shards = [wdq, dkv, uq, ukv]
        full = lambda w, cols: pltpu.VMEM((w.shape[0] * n_fsdp, cols), jnp.bfloat16)
        o_cols = GROUP * VDIM
        n_groups = wuq.shape[1] // Q_COLS
        first, rest = GROUPS_FIRST, n_groups - GROUPS_FIRST
        last = n_p - 1
        pa = 2 * n_p + n_p // 2
        blk = lambda cols, lag: pl.BlockSpec((1, seq_len, cols), lambda i: (jnp.clip(i - lag, 0, last), 0, 0))
        out = lambda cols: jax.ShapeDtypeStruct((n_p, seq_len, cols), jnp.bfloat16)
        r_shape = jax.ShapeDtypeStruct((n_p, ROPE, seq_len), jnp.bfloat16)
        hbm = pl.BlockSpec(memory_space=pl.ANY)
        c, r, oa, ob, wout_all = pl.pallas_call(
            functools.partial(core_kernel, n_p),
            grid=(4 * n_p + n_p // 2,),
            in_specs=[blk(d_model, 0)] + [hbm] * 6 + [whole(cos.shape)] * 2,
            out_specs=[
                whole((n_p, seq_len, kv_rank)), whole((n_p, ROPE, seq_len)),
                blk(first * o_cols, pa), blk(rest * o_cols, pa + n_p), hbm,
            ],
            out_shape=[
                out(kv_rank), r_shape, out(first * o_cols), out(rest * o_cols),
                jax.ShapeDtypeStruct((wout.shape[0] * n_fsdp, wout.shape[1]), jnp.bfloat16),
            ],
            scratch_shapes=[
                full(wdq, q_rank), full(wdkv, kv_rank + LANES),
                full(wuq, first * Q_COLS), full(wuq, rest * Q_COLS),
                full(wukv, first * KV_COLS), full(wukv, rest * KV_COLS),
                pltpu.VMEM((n_fsdp, GAIN_ROWS, LANES), jnp.float32),
                pltpu.VMEM((1, n_gain), jnp.float32),
                pltpu.VMEM((n_p, seq_len, d_model), jnp.bfloat16),
                pltpu.VMEM((n_p, seq_len, q_rank + kv_rank + LANES), jnp.float32),
                pltpu.VMEM((n_p, seq_len, q_rank), jnp.bfloat16),
                pltpu.VMEM((n_p, seq_len, LANES), jnp.bfloat16),
                pltpu.VMEM(wout.shape, jnp.bfloat16),
                pltpu.VMEM(((Q_COLS + KV_COLS) // LANES, seq_len, LANES), jnp.bfloat16),
                pltpu.SemaphoreType.DMA((7, N_COPIES)),
                pltpu.SemaphoreType.DMA((7, N_COPIES)),
                pltpu.SemaphoreType.DMA((7,)),
                pltpu.SemaphoreType.DMA((7,)),
                pltpu.SemaphoreType.DMA((9,)),
            ],
            compiler_params=pltpu.CompilerParams(
                vmem_limit_bytes=VMEM_LIMIT, dimension_semantics=("arbitrary",), collective_id=0, has_side_effects=True,
            ),
            name="core",
        )(x, gs, *shards, wout, cos, sin)
        rows = 512
        tile = lambda cols: pl.BlockSpec((rows, cols), lambda i: (i, 0))
        r_tile = pl.BlockSpec((rows // seq_len, ROPE, seq_len), lambda i: (i, 0, 0))
        flat = lambda v: v.reshape(n_p * seq_len, v.shape[-1])
        flat_out = lambda cols: jax.ShapeDtypeStruct((n_p * seq_len, cols), jnp.bfloat16)
        y, c, r = pl.pallas_call(
            out_kernel,
            grid=(n_p * seq_len // rows,),
            in_specs=[tile(d_model), tile(oa.shape[-1]), tile(ob.shape[-1]), hbm, tile(kv_rank), r_tile],
            out_specs=[tile(d_model), tile(kv_rank), r_tile],
            out_shape=[flat_out(d_model), flat_out(kv_rank), r_shape],
            scratch_shapes=[pltpu.VMEM(wout_all.shape, jnp.bfloat16), pltpu.SemaphoreType.DMA((8,))],
            compiler_params=pltpu.CompilerParams(vmem_limit_bytes=VMEM_LIMIT, dimension_semantics=("arbitrary",)),
            name="project",
        )(flat(x), flat(oa), flat(ob), wout_all, flat(c), r)
        back = lambda v: v.reshape(n_p, seq_len, v.shape[-1])
        return back(y), back(c), jnp.swapaxes(r, 1, 2)

    batch, row, mat = P(('dp', 'fsdp')), P('fsdp'), P('fsdp', None)
    return jax.shard_map(
        local_block,
        mesh=mesh,
        in_specs=(batch, row, mat, row, mat, mat, row, mat, mat),
        out_specs=(batch, batch, batch),
        check_vma=False,
    )
```

```python
import functools

import jax
import jax.numpy as jnp
import numpy as np
from jax import lax
from jax.experimental import pallas as pl
from jax.experimental.pallas import tpu as pltpu
from jax.sharding import PartitionSpec as P

EPSILON = 1e-6
ROPE_THETA = 10000.0
LOG2E = 1.4426950408889634
VMEM_LIMIT = 64000 * 1024

NOPE, ROPE, VDIM = 64, 32, 64
HALF = ROPE // 2
GROUP = 8
PE_TILE = 4
LANES = 128
Q_COLS, KV_COLS = GROUP * (NOPE + ROPE), GROUP * (NOPE + VDIM)
AHEAD, SPREAD = 2, 6
MASKED = -1e30


def rope_tiles(seq_len):
    inv_freq = ROPE_THETA ** (-2.0 * np.arange(HALF) / ROPE)
    angles = np.arange(seq_len)[:, None] * inv_freq[None, :]
    cos = np.tile(np.cos(angles), (1, LANES // HALF))
    sin = np.tile(np.sin(angles), (1, PE_TILE))
    blank = np.zeros_like(angles)
    twice = lambda *parts: np.tile(np.concatenate(parts + (blank, blank), axis=1), (1, 2))
    one_cos, one_sin = np.cos(angles), np.sin(angles)
    key = [twice(one_cos, one_cos), twice(-one_sin, blank), twice(blank, one_sin)]
    return [v.astype(np.float32) for v in [cos, np.concatenate([-sin, sin], axis=1)] + key]


def inv_rms(v):
    return lax.rsqrt(jnp.mean(v * v, axis=-1, keepdims=True) + EPSILON)


def rotate_key(tile, cos, ahead, behind):
    return tile * cos + pltpu.roll(tile, LANES - HALF, 1) * ahead + pltpu.roll(tile, HALF, 1) * behind


def rotate(tile, cos, sin):
    return tile * cos + pltpu.roll(tile, LANES // 2, 1) * sin


MESH = pl.DeviceIdType.MESH
GAIN_ROWS = 32
GROUPS_FIRST = 2
N_COPIES = 19
PLANES = (1, 2, 3)


class Item:
    def __init__(self, index, shard, col, cols, full):
        self.index, self.shard, self.col, self.cols, self.full = index, shard, col, cols, full
        self.rows = shard.shape[0]
        if (self.rows // 4) % 16 == 0:
            self.q_rows, self.q_cols = self.rows // 4, cols
        elif (cols // 4) % LANES == 0 and self.rows == 32:
            self.q_rows, self.q_cols = self.rows, cols // 4
        else:
            self.q_rows, self.q_cols = self.rows // 2, cols // 2
        if self.q_rows == self.rows:
            n = self.q_rows // 2
            self.halves = [(0, n, 0, self.q_cols), (n, n, 0, self.q_cols)]
        else:
            n = -(-self.q_cols // (2 * LANES)) * LANES
            self.halves = [(0, self.q_rows, 0, n), (0, self.q_rows, n, self.q_cols - n)]

    def quarter(self, q):
        per_row = self.cols // self.q_cols
        return (q // per_row) * self.q_rows, lax.rem(q, per_row) * self.q_cols

    def source(self, q):
        r, c = self.quarter(q)
        return self.shard.at[pl.ds(pl.multiple_of(r, 16), self.q_rows), pl.ds(pl.multiple_of(self.col + c, LANES), self.q_cols)]

    def own(self):
        return self.shard.at[:, pl.ds(self.col, self.cols)]

    def place(self, f, q=None, half=None):
        r, c = (0, 0) if q is None else self.quarter(q)
        r = f * self.rows + r
        if q is None:
            n_r, n_c = self.rows, self.cols
        elif half is None:
            n_r, n_c = self.q_rows, self.q_cols
        else:
            dr, n_r, dc, n_c = self.halves[half]
            r, c = r + dr, c + dc
        if n_c == self.cols:
            return self.full.at[pl.ds(pl.multiple_of(r, 16), n_r)]
        return self.full.at[pl.ds(pl.multiple_of(r, 16), n_r), pl.ds(pl.multiple_of(c, LANES), n_c)]


class Net:
    def __init__(self, send_sem, recv_sem):
        self.send_sem, self.recv_sem = send_sem, recv_sem
        self.d, self.f = lax.axis_index('dp'), lax.axis_index('fsdp')
        self.z, self.core = self.f // 2, lax.rem(self.f, 2)
        self.dx = lax.rem(self.d + 2, 4)
        self.dy = self.d + 1 - 2 * lax.rem(self.d, 2)
        self.dd = lax.rem(self.dy + 2, 4)
        self.sib = self.z * 2 + 1 - self.core

    def to(self, k):
        return lax.rem(self.z + k, 4) * 2 + self.core

    def plane(self, k):
        return lax.rem(self.z + 4 - k, 4)

    def origin(self, k):
        return self.plane(k) * 2 + self.core

    def copy(self, it, src, dst, s, r, dev):
        return pltpu.make_async_remote_copy(
            src_ref=src, dst_ref=dst, send_sem=self.send_sem.at[it.index, s], recv_sem=self.recv_sem.at[it.index, r],
            device_id=dev, device_id_type=MESH,
        )

    def along_z(self, it, k):
        return self.copy(it, it.source(self.d), it.place(self.f, self.d), k - 1, k - 1, (self.d, self.to(k)))

    def to_x(self, it, k):
        ref = it.place(self.origin(k), self.d)
        return self.copy(it, ref, ref, 2 + k, 2 + k, (self.dx, self.f))

    def to_y(self, it, k):
        ref = it.place(self.origin(k), self.d)
        return self.copy(it, ref, ref, 5 + k, 5 + k, (self.dy, self.f))

    def diag_y(self, it, k):
        ref = it.place(self.origin(k), self.dx, 0)
        return self.copy(it, ref, ref, 8 + k, 8 + k, (self.dy, self.f))

    def diag_x(self, it, k):
        ref = it.place(self.origin(k), self.dy, 1)
        return self.copy(it, ref, ref, 11 + k, 11 + k, (self.dx, self.f))

    def to_core(self, it, k):
        ref = it.place(self.origin(k))
        return self.copy(it, ref, ref, 14 + k, 14 + k, (self.d, self.sib))

    def own_copy(self, it):
        return self.copy(it, it.own(), it.place(self.f), 18, 18, (self.d, self.sib))

    def arrived(self, it, ref, r):
        self.copy(it, ref, ref, 0, r, (self.d, self.f)).wait_recv()

    def barrier(self, peers):
        sem = pltpu.get_barrier_semaphore()
        for peer in peers:
            pl.semaphore_signal(sem, inc=1, device_id=peer, device_id_type=MESH)
        pl.semaphore_wait(sem, len(peers))

    def send_z(self, its, ks=PLANES):
        for k in ks:
            for it in its:
                self.along_z(it, k).start()

    def a2(self, its, ks=PLANES):
        for k in ks:
            for it in its:
                self.arrived(it, it.place(self.origin(k), self.d), k - 1)
                self.to_x(it, k).start()
                self.to_y(it, k).start()

    def a3(self, its, ks=PLANES):
        for k in ks:
            for it in its:
                self.arrived(it, it.place(self.origin(k), self.dx), 2 + k)
                self.diag_y(it, k).start()
                self.arrived(it, it.place(self.origin(k), self.dy), 5 + k)
                self.diag_x(it, k).start()

    def a4(self, its, ks=PLANES):
        for k in ks:
            for it in its:
                self.arrived(it, it.place(self.origin(k), self.dd, 0), 8 + k)
                self.arrived(it, it.place(self.origin(k), self.dd, 1), 11 + k)
                self.to_core(it, k).start()

    def a5(self, its, ks=PLANES):
        for k in ks:
            for it in its:
                self.arrived(it, it.place(self.plane(k) * 2 + 1 - self.core), 14 + k)

    def from_core(self, its):
        for it in its:
            self.arrived(it, it.place(self.sib), 18)

    def sent(self, its):
        for it in its:
            for k in PLANES:
                for make in (self.along_z, self.to_x, self.to_y, self.diag_y, self.diag_x, self.to_core):
                    make(it, k).wait_send()
            self.own_copy(it).wait_send()


def scores(tiles, rt, low, j):
    qn, qp, kn, _ = tiles
    t = j // 2
    odd, slot, pe = j % 2, j % PE_TILE * HALF, qp[j // PE_TILE]
    nope = qn[t][odd * NOPE:(odd + 1) * NOPE]
    rotary = [pe[slot:slot + HALF], pe[LANES // 2 + slot:LANES // 2 + slot + HALF]]
    rotary.append(jnp.zeros((LANES - NOPE - ROPE, pe.shape[1]), jnp.bfloat16))
    q_tile = jnp.concatenate(rotary + [nope] if odd else [nope] + rotary, axis=0)
    k_tile = jnp.where(low, rt, kn[t]) if odd else jnp.where(low, kn[t], rt)
    return jnp.dot(k_tile, q_tile, preferred_element_type=jnp.float32)


def softmax(s, diag, zero, scale):
    half = s.shape[0] // 2
    left = jnp.where(diag, s[:half, :half], MASKED)
    up = s[:half, half:]
    right = jnp.where(diag, s[half:, half:], MASKED)
    m_l = jnp.max(left, axis=0, keepdims=True) * scale
    m_r = jnp.max(jnp.maximum(up, right), axis=0, keepdims=True) * scale
    e_l = jnp.exp2(left * scale - m_l)
    e_u = jnp.exp2(up * scale - m_r)
    e_r = jnp.exp2(right * scale - m_r)
    r_l = 1.0 / jnp.sum(e_l, axis=0, keepdims=True)
    r_r = 1.0 / jnp.sum(e_u + e_r, axis=0, keepdims=True)
    p_top = jnp.concatenate([(e_l * r_l).astype(jnp.bfloat16), (e_u * r_r).astype(jnp.bfloat16)], axis=1)
    p_bot = jnp.concatenate([zero, (e_r * r_r).astype(jnp.bfloat16)], axis=1)
    return jnp.concatenate([p_top, p_bot], axis=0)


def pieces(cq, lat, wuq, wukv, g, cos, sin):
    w = 2 * LANES

    def tiles(x, weights, cols, n, pe=False):
        r = jnp.dot(x, weights[:, g * cols + n * w:g * cols + (n + 1) * w], preferred_element_type=jnp.float32)
        both = [r[:, :LANES], r[:, LANES:]]
        return [(rotate(t, cos, sin) if pe else t).astype(jnp.bfloat16) for t in both]

    n_q, n_kv = Q_COLS // w, KV_COLS // w
    return [functools.partial(tiles, cq, wuq, Q_COLS, n, n == n_q - 1) for n in range(n_q)] + [
        functools.partial(tiles, lat, wukv, KV_COLS, n) for n in range(n_kv)
    ]


def arrange_tiles(made):
    flat = [t for pair in made for t in pair]
    n = GROUP // 2
    m = n + GROUP // PE_TILE
    turned = [t.T for t in flat[:m]]
    return turned[:n], turned[n:], flat[m:m + n], [t.T for t in flat[m + n:]]


def attend(cq, lat, rt, cq_next, lat_next, start, wuq, wukv, cos, sin, hold, o_ref):
    n_groups = wuq.shape[1] // Q_COLS
    scale = (NOPE + ROPE) ** -0.5 * LOG2E
    seq_len = cq.shape[0]
    half = seq_len // 2
    low = lax.broadcasted_iota(jnp.int32, (1, LANES), 1) < NOPE
    diag = lax.broadcasted_iota(jnp.int32, (half, half), 0) <= lax.broadcasted_iota(jnp.int32, (half, half), 1)
    zero = jnp.zeros((half, half), jnp.bfloat16)
    n_pieces = hold.shape[0] // 2

    def put(n, made):
        for m, t in enumerate(made):
            hold[2 * n + m] = t

    @pl.when(start)
    def _():
        for n, make in enumerate(pieces(cq, lat, wuq, wukv, 0, cos, sin)):
            put(n, make())

    tiles = {0: arrange_tiles([[hold[2 * n], hold[2 * n + 1]] for n in range(n_pieces)])}
    total = n_groups * GROUP
    s, p, outs = {}, {}, {}
    for u in range(-AHEAD, total + 1):
        g, j = divmod(u, GROUP)
        if u >= 0 and u < total:
            p[u] = softmax(s.pop(u), diag, zero, scale)
            if j == 0:
                made = []
                if g + 1 < n_groups:
                    todo = pieces(cq, lat, wuq, wukv, g + 1, cos, sin)
                else:
                    todo = pieces(cq_next, lat_next, wuq, wukv, 0, cos, sin)
            if j < SPREAD:
                for n in range(j * n_pieces // SPREAD, (j + 1) * n_pieces // SPREAD):
                    made.append(todo[n]())
                if len(made) == n_pieces and g + 1 < n_groups:
                    tiles[g + 1] = arrange_tiles(made)
                elif len(made) == n_pieces:
                    for n, m in enumerate(made):
                        put(n, m)
        if u + AHEAD < total:
            v = u + AHEAD
            s[v] = scores(tiles[v // GROUP], rt, low, v % GROUP)
        if u >= 1:
            h = u - 1
            hj = h % GROUP
            vt = tiles[h // GROUP][3][hj // 2][hj % 2 * VDIM:(hj % 2 + 1) * VDIM]
            outs[h] = jnp.dot(vt, p.pop(h), preferred_element_type=jnp.float32).astype(jnp.bfloat16)
            if h % 2 == 1:
                pair = jnp.concatenate([outs.pop(h - 1), outs.pop(h)], axis=0)
                o_ref[0, :, h // 2 * LANES:(h // 2 + 1) * LANES] = pair.T


def core_kernel(
    n_prompts, x_ref, gs_ref, dq_s, dkv_s, uq_s, ukv_s, out_s, cos_ref, sin_ref, kcos, kahead, kbehind,
    c_all, r_ref, oa_ref, ob_ref, wout_ref,
    wdq, wdkv, wuqa, wuqb, wukva, wukvb, gains, gvec, a_all, acc, cq_all, rt_all, stage, hold,
    send_sem, recv_sem, g_send, g_recv, local_sem,
):
    i = pl.program_id(0)
    key_tables = (kcos, kahead, kbehind)
    net = Net(send_sem, recv_sem)
    d, f = net.d, net.f
    n_a, m_a = wuqa.shape[1], wukva.shape[1]
    todo = [
        (dkv_s, 0, wdkv), (dq_s, 0, wdq), (ukv_s, 0, wukva), (uq_s, 0, wuqa),
        (ukv_s, m_a, wukvb), (uq_s, n_a, wuqb), (out_s, 0, wout_ref),
    ]
    items = [Item(n, shard, col, full.shape[1], full) for n, (shard, col, full) in enumerate(todo)]
    down, first, rest, last = items[:2], items[2:4], items[4:6], items[6:]
    wo = items[6]
    others = range(1, 8)

    def keep(it):
        return pltpu.make_async_copy(it.own(), stage if it is wo else it.place(f), local_sem.at[it.index])

    def keep_out():
        return pltpu.make_async_copy(stage, wo.place(f), local_sem.at[7])

    def keep_gain():
        return pltpu.make_async_copy(gs_ref, gains.at[f], local_sem.at[8])

    def gain_copy(j):
        return pltpu.make_async_remote_copy(
            src_ref=gs_ref, dst_ref=gains.at[f], send_sem=g_send.at[j - 1], recv_sem=g_recv.at[j - 1],
            device_id=(d, lax.rem(f + j, 8)), device_id_type=MESH,
        )

    @pl.when(i == 0)
    def _():
        net.barrier([(net.dx, f), (net.dy, f)] + [(d, lax.rem(f + j, 8)) for j in others])
        for j in others:
            gain_copy(j).start()
        keep_gain().start()
        for it in down:
            net.own_copy(it).start()
            keep(it).start()
        net.send_z(down)
        for it in items[2:]:
            net.own_copy(it).start()
            keep(it).start()
        for j in others:
            gain_copy(j).wait_recv()
        keep_gain().wait()
        total = jnp.sum(gains[...], axis=0)
        for t in range(gvec.shape[1] // LANES):
            gvec[:, t * LANES:(t + 1) * LANES] = total[t:t + 1, :]
        for it in down:
            keep(it).wait()
        net.from_core(down)

    d_model, q_rank, kv_rank = x_ref.shape[-1], cq_all.shape[-1], c_all.shape[-1]
    seq_len = x_ref.shape[1]
    k_rows = d_model // 4
    half = n_prompts // 2
    c1 = n_prompts
    c2 = c1 + half
    fin = c2 + half
    pa = fin + half
    pb = pa + n_prompts
    end = pb + n_prompts - 1
    one, two, three = ((k,) for k in PLANES)

    @pl.when(i == 1)
    def _():
        keep(wo).wait()
        keep_out().start()

    def ready(its):
        for it in its:
            (keep_out() if it is wo else keep(it)).wait()
        net.from_core(its)
        net.a5(its)

    plan = [
        (0, [(net.send_z, rest, one), (net.send_z, first, two)]),
        (3, [(net.a2, down, one)]),
        (5, [(net.a3, down, one), (net.send_z, first, three)]),
        (6, [(net.a2, down, two)]),
        (7, [(net.a4, down, one), (net.a2, down, three)]),
        (8, [(net.send_z, first, one), (net.a5, down, one)]),
        (9, [(net.a3, down, two)]),
        (10, [(net.a3, down, three)]),
        (11, [(net.a4, down, two), (net.a2, first, two)]),
        (12, [(net.a2, first, three), (net.a4, down, three), (net.a5, down, two), (net.send_z, rest, two)]),
        (13, [(net.a2, first, one)]),
        (14, [(net.a5, down, three)]),
        (15, [(net.a3, first, two), (net.send_z, rest, three), (net.a3, first, three)]),
        (16, [(net.a3, first, one)]),
        (17, [(net.a4, first, two)]),
        (18, [(net.a2, rest, two), (net.send_z, last, one), (net.a4, first, three), (net.a4, first, one)]),
        (19, [(net.a2, rest, one)]),
        (20, [(net.send_z, last, two)]),
        (21, [(net.a2, rest, three), (net.a3, rest, two)]),
        (22, [(net.a3, rest, one), (net.send_z, last, three)]),
        (23, [(net.a3, rest, three), (net.a2, last, one)]),
        (24, [(net.a4, rest, two)]),
        (25, [(net.a4, rest, one)]),
        (26, [(net.a4, rest, three)]),
        (28, [(net.a2, last, two)]),
        (29, [(net.a3, last, one)]),
        (30, [(net.a2, last, three)]),
        (31, [(net.a3, last, two), (net.a4, last, one)]),
        (33, [(net.a3, last, three)]),
        (34, [(net.a4, last, two)]),
        (35, [(net.a4, last, three)]),
    ]
    for step, acts in plan:
        @pl.when(i == step)
        def _(acts=acts):
            for act, its, ks in acts:
                act(its, ks)

    for step, its in ((pa, first), (pb, rest)):
        @pl.when(i == step)
        def _(its=its):
            ready(its)

    def partial_sums(p, n, k):
        rows = pl.ds(pl.multiple_of(net.plane(k) * k_rows, LANES), k_rows)
        a = a_all[pl.ds(p, n), :, rows].reshape(n * seq_len, k_rows)
        qd = jnp.dot(a, wdq[rows], preferred_element_type=jnp.float32)
        kd = jnp.dot(a, wdkv[rows], preferred_element_type=jnp.float32)
        if k > 0:
            old = acc[pl.ds(p, n)].reshape(n * seq_len, q_rank + kv_rank + LANES)
            qd += old[:, :q_rank]
            kd += old[:, q_rank:]
        return qd, kd

    def add_plane(p, n, k):
        qd, kd = partial_sums(p, n, k)
        acc[pl.ds(p, n), :, :q_rank] = qd.reshape(n, seq_len, q_rank)
        acc[pl.ds(p, n), :, q_rank:] = kd.reshape(n, seq_len, kv_rank + LANES)

    @pl.when(i < c1)
    def _():
        x = x_ref[0].astype(jnp.float32)
        a_all[i] = (x * inv_rms(x) * gvec[:, :d_model]).astype(jnp.bfloat16)
        add_plane(i, 1, 0)

    @pl.when(jnp.logical_and(i >= c1, i < c2))
    def _():
        add_plane((i - c1) * 2, 2, 1)

    @pl.when(jnp.logical_and(i >= c2, i < fin))
    def _():
        add_plane((i - c2) * 2, 2, 2)

    @pl.when(jnp.logical_and(i >= fin, i < pa))
    def _():
        p = (i - fin) * 2
        qd, kd = partial_sums(p, 2, 3)
        cq = (qd * inv_rms(qd) * gvec[:, d_model:d_model + q_rank]).astype(jnp.bfloat16)
        cq_all[pl.ds(p, 2)] = cq.reshape(2, seq_len, q_rank)
        lat = kd[:, :kv_rank]
        lat = (lat * inv_rms(lat) * gvec[:, d_model + q_rank:]).astype(jnp.bfloat16)
        c_all[pl.ds(p, 2)] = lat.reshape(2, seq_len, kv_rank)
        for n in range(2):
            pe = kd[n * seq_len:(n + 1) * seq_len, kv_rank:]
            rt = rotate_key(pe, *[t[...] for t in key_tables]).astype(jnp.bfloat16)
            rt_all[p + n] = rt
            r_ref[p + n] = rt.T[:ROPE]

    def attend_step(p, wuq, wukv, o_ref):
        after = jnp.minimum(p + 1, n_prompts - 1)
        attend(
            cq_all[p], c_all[p], rt_all[p], cq_all[after], c_all[after], p == 0,
            wuq, wukv, cos_ref[...], sin_ref[...], hold, o_ref,
        )

    @pl.when(jnp.logical_and(i >= pa, i < pb))
    def _():
        attend_step(i - pa, wuqa, wukva, oa_ref)

    @pl.when(i >= pb)
    def _():
        attend_step(i - pb, wuqb, wukvb, ob_ref)

    @pl.when(i == end)
    def _():
        ready(last)
        for j in others:
            gain_copy(j).wait_send()
        net.sent(items)


def one_hot(source, n_rows):
    rows = lax.broadcasted_iota(jnp.int32, (n_rows, source.shape[1]), 0)
    return (rows == source).astype(jnp.float32).astype(jnp.bfloat16)


def pick(w, matrix):
    return jnp.dot(w, matrix, preferred_element_type=jnp.float32).astype(jnp.bfloat16)


def prepare_kernel(g1_ref, gq_ref, gkv_ref, wuq_ref, wukv_ref, wdkv_ref, gs_ref, uq_ref, ukv_ref, dkv_ref):
    f = lax.axis_index('fsdp')
    row = 0
    gs_ref[...] = jnp.zeros_like(gs_ref)
    for g in (g1_ref, gq_ref, gkv_ref):
        n = g.shape[1]
        for t in range(n * 8 // LANES):
            index = lax.broadcasted_iota(jnp.int32, (1, LANES), 1) + (t * LANES - f * n)
            gs_ref[row:row + 1, :] = jnp.dot(g[...], one_hot(index, n), preferred_element_type=jnp.float32)
            row += 1

    def column(n):
        return lax.broadcasted_iota(jnp.int32, (1, n), 1)

    c = column(Q_COLS)
    n_nope = GROUP * NOPE
    pe = c - n_nope
    head = pe // LANES * PE_TILE + lax.rem(pe, LANES // 2) // HALF
    pe = head * (NOPE + ROPE) + NOPE + lax.rem(pe, LANES) // (LANES // 2) * HALF + lax.rem(pe, HALF)
    order = one_hot(jnp.where(c < n_nope, c // NOPE * (NOPE + ROPE) + lax.rem(c, NOPE), pe), Q_COLS)
    for g in range(wuq_ref.shape[1] // Q_COLS):
        cols = slice(g * Q_COLS, (g + 1) * Q_COLS)
        uq_ref[:, cols] = pick(wuq_ref[:, cols], order)

    c = column(KV_COLS)
    part = lax.rem(c, n_nope)
    order = one_hot(part // NOPE * (NOPE + VDIM) + c // n_nope * NOPE + lax.rem(part, NOPE), KV_COLS)
    for g in range(wukv_ref.shape[1] // KV_COLS):
        cols = slice(g * KV_COLS, (g + 1) * KV_COLS)
        ukv_ref[:, cols] = pick(wukv_ref[:, cols], order)

    kv_rank = dkv_ref.shape[1] - LANES
    c = column(LANES)
    wdkv = wdkv_ref[...].T
    dkv_ref[:, :kv_rank] = wdkv[:, :kv_rank]
    c = lax.rem(c, LANES // 2)
    order = one_hot(jnp.where(c < ROPE, c, -1), ROPE)
    dkv_ref[:, kv_rank:] = pick(wdkv[:, kv_rank:], order)


def out_kernel(x_ref, oa_ref, ob_ref, w_hbm, c_in, r_in, y_ref, c_out, r_out, w, sem):
    step = 512
    n_steps = y_ref.shape[1] // step
    first = pl.program_id(0) == 0
    cols = [slice(n * step, (n + 1) * step) for n in range(n_steps)]
    load = [pltpu.make_async_copy(w_hbm.at[:, c], w.at[:, c], sem.at[n]) for n, c in enumerate(cols)]

    o = jnp.concatenate([oa_ref[...], ob_ref[...]], axis=1)
    c_out[...] = c_in[...]
    r_out[...] = r_in[...]

    def product(c):
        acc = jnp.dot(o, w[:, c], preferred_element_type=jnp.float32)
        y_ref[:, c] = (x_ref[:, c].astype(jnp.float32) + acc).astype(jnp.bfloat16)

    @pl.when(first)
    def _():
        for part in load:
            part.start()
        for part, c in zip(load, cols):
            part.wait()
            product(c)

    @pl.when(jnp.logical_not(first))
    def _():
        for c in cols:
            product(c)


def whole(shape):
    return pl.BlockSpec(shape, lambda i: (0,) * len(shape))


def solution(mesh):
    n_fsdp = mesh.shape['fsdp']

    def local_block(x, g1, wdq, gq, wuq, wdkv, gkv, wukv, wout):
        n_p, seq_len, d_model = x.shape
        kv_rank, q_rank = gkv.shape[0] * n_fsdp, wdq.shape[1]
        tables = [jnp.asarray(t) for t in rope_tiles(seq_len)]
        n_gain = d_model + q_rank + kv_rank
        like = lambda w, cols: jax.ShapeDtypeStruct((w.shape[0], cols), jnp.bfloat16)
        gs, uq, ukv, dkv = pl.pallas_call(
            prepare_kernel,
            out_shape=[
                jax.ShapeDtypeStruct((GAIN_ROWS, LANES), jnp.float32),
                like(wuq, wuq.shape[1]), like(wukv, wukv.shape[1]), like(wdkv, kv_rank + LANES),
            ],
            name="prepare",
        )(g1[None], gq[None], gkv[None], wuq, wukv, wdkv.T)
        shards = [wdq, dkv, uq, ukv]
        full = lambda w, cols: pltpu.VMEM((w.shape[0] * n_fsdp, cols), jnp.bfloat16)
        o_cols = GROUP * VDIM
        n_groups = wuq.shape[1] // Q_COLS
        first, rest = GROUPS_FIRST, n_groups - GROUPS_FIRST
        last = n_p - 1
        pa = 2 * n_p + n_p // 2
        blk = lambda cols, lag: pl.BlockSpec((1, seq_len, cols), lambda i: (jnp.clip(i - lag, 0, last), 0, 0))
        out = lambda cols: jax.ShapeDtypeStruct((n_p, seq_len, cols), jnp.bfloat16)
        r_shape = jax.ShapeDtypeStruct((n_p, ROPE, seq_len), jnp.bfloat16)
        hbm = pl.BlockSpec(memory_space=pl.ANY)
        c, r, oa, ob, wout_all = pl.pallas_call(
            functools.partial(core_kernel, n_p),
            grid=(4 * n_p + n_p // 2,),
            in_specs=[blk(d_model, 0)] + [hbm] * 6 + [whole(tables[0].shape)] * len(tables),
            out_specs=[
                whole((n_p, seq_len, kv_rank)), whole((n_p, ROPE, seq_len)),
                blk(first * o_cols, pa), blk(rest * o_cols, pa + n_p), hbm,
            ],
            out_shape=[
                out(kv_rank), r_shape, out(first * o_cols), out(rest * o_cols),
                jax.ShapeDtypeStruct((wout.shape[0] * n_fsdp, wout.shape[1]), jnp.bfloat16),
            ],
            scratch_shapes=[
                full(wdq, q_rank), full(wdkv, kv_rank + LANES),
                full(wuq, first * Q_COLS), full(wuq, rest * Q_COLS),
                full(wukv, first * KV_COLS), full(wukv, rest * KV_COLS),
                pltpu.VMEM((n_fsdp, GAIN_ROWS, LANES), jnp.float32),
                pltpu.VMEM((1, n_gain), jnp.float32),
                pltpu.VMEM((n_p, seq_len, d_model), jnp.bfloat16),
                pltpu.VMEM((n_p, seq_len, q_rank + kv_rank + LANES), jnp.float32),
                pltpu.VMEM((n_p, seq_len, q_rank), jnp.bfloat16),
                pltpu.VMEM((n_p, seq_len, LANES), jnp.bfloat16),
                pltpu.VMEM(wout.shape, jnp.bfloat16),
                pltpu.VMEM(((Q_COLS + KV_COLS) // LANES, seq_len, LANES), jnp.bfloat16),
                pltpu.SemaphoreType.DMA((7, N_COPIES)),
                pltpu.SemaphoreType.DMA((7, N_COPIES)),
                pltpu.SemaphoreType.DMA((7,)),
                pltpu.SemaphoreType.DMA((7,)),
                pltpu.SemaphoreType.DMA((9,)),
            ],
            compiler_params=pltpu.CompilerParams(
                vmem_limit_bytes=VMEM_LIMIT, dimension_semantics=("arbitrary",), collective_id=0, has_side_effects=True,
            ),
            name="core",
        )(x, gs, *shards, wout, *tables)
        rows = 512
        tile = lambda cols: pl.BlockSpec((rows, cols), lambda i: (i, 0))
        r_tile = pl.BlockSpec((rows // seq_len, ROPE, seq_len), lambda i: (i, 0, 0))
        flat = lambda v: v.reshape(n_p * seq_len, v.shape[-1])
        flat_out = lambda cols: jax.ShapeDtypeStruct((n_p * seq_len, cols), jnp.bfloat16)
        y, c, r = pl.pallas_call(
            out_kernel,
            grid=(n_p * seq_len // rows,),
            in_specs=[tile(d_model), tile(oa.shape[-1]), tile(ob.shape[-1]), hbm, tile(kv_rank), r_tile],
            out_specs=[tile(d_model), tile(kv_rank), r_tile],
            out_shape=[flat_out(d_model), flat_out(kv_rank), r_shape],
            scratch_shapes=[pltpu.VMEM(wout_all.shape, jnp.bfloat16), pltpu.SemaphoreType.DMA((8,))],
            compiler_params=pltpu.CompilerParams(vmem_limit_bytes=VMEM_LIMIT, dimension_semantics=("arbitrary",)),
            name="project",
        )(flat(x), flat(oa), flat(ob), wout_all, flat(c), r)
        back = lambda v: v.reshape(n_p, seq_len, v.shape[-1])
        return back(y), back(c), jnp.swapaxes(r, 1, 2)

    batch, row, mat = P(('dp', 'fsdp')), P('fsdp'), P('fsdp', None)
    return jax.shard_map(
        local_block,
        mesh=mesh,
        in_specs=(batch, row, mat, row, mat, mat, row, mat, mat),
        out_specs=(batch, batch, batch),
        check_vma=False,
    )
```

```python
import functools

import jax
import jax.numpy as jnp
import numpy as np
from jax import lax
from jax.experimental import pallas as pl
from jax.experimental.pallas import tpu as pltpu
from jax.sharding import PartitionSpec as P

EPSILON = 1e-6
ROPE_THETA = 10000.0
LOG2E = 1.4426950408889634
VMEM_LIMIT = 64000 * 1024

NOPE, ROPE, VDIM = 64, 32, 64
HALF = ROPE // 2
GROUP = 8
PE_TILE = 4
LANES = 128
Q_COLS, KV_COLS = GROUP * (NOPE + ROPE), GROUP * (NOPE + VDIM)
AHEAD, SPREAD = 2, 6
MASKED = -1e30


def rope_tiles(seq_len):
    inv_freq = ROPE_THETA ** (-2.0 * np.arange(HALF) / ROPE)
    angles = np.arange(seq_len)[:, None] * inv_freq[None, :]
    cos = np.tile(np.cos(angles), (1, LANES // HALF))
    sin = np.tile(np.sin(angles), (1, PE_TILE))
    blank = np.zeros_like(angles)
    twice = lambda *parts: np.tile(np.concatenate(parts + (blank, blank), axis=1), (1, 2))
    one_cos, one_sin = np.cos(angles), np.sin(angles)
    key = [twice(one_cos, one_cos), twice(-one_sin, blank), twice(blank, one_sin)]
    return [v.astype(np.float32) for v in [cos, np.concatenate([-sin, sin], axis=1)] + key]


def inv_rms(v):
    return lax.rsqrt(jnp.mean(v * v, axis=-1, keepdims=True) + EPSILON)


def rotate_key(tile, cos, ahead, behind):
    return tile * cos + pltpu.roll(tile, LANES - HALF, 1) * ahead + pltpu.roll(tile, HALF, 1) * behind


def rotate(tile, cos, sin):
    return tile * cos + pltpu.roll(tile, LANES // 2, 1) * sin


MESH = pl.DeviceIdType.MESH
GAIN_ROWS = 32
GROUPS_FIRST = 2
N_COPIES = 19
PLANES = (1, 2, 3)


class Item:
    def __init__(self, index, shard, col, cols, full):
        self.index, self.shard, self.col, self.cols, self.full = index, shard, col, cols, full
        self.rows = shard.shape[0]
        if (self.rows // 4) % 16 == 0:
            self.q_rows, self.q_cols = self.rows // 4, cols
        elif (cols // 4) % LANES == 0 and self.rows == 32:
            self.q_rows, self.q_cols = self.rows, cols // 4
        else:
            self.q_rows, self.q_cols = self.rows // 2, cols // 2
        if self.q_rows == self.rows:
            n = self.q_rows // 2
            self.halves = [(0, n, 0, self.q_cols), (n, n, 0, self.q_cols)]
        else:
            n = -(-self.q_cols // (2 * LANES)) * LANES
            self.halves = [(0, self.q_rows, 0, n), (0, self.q_rows, n, self.q_cols - n)]

    def quarter(self, q):
        per_row = self.cols // self.q_cols
        return (q // per_row) * self.q_rows, lax.rem(q, per_row) * self.q_cols

    def source(self, q):
        r, c = self.quarter(q)
        return self.shard.at[pl.ds(pl.multiple_of(r, 16), self.q_rows), pl.ds(pl.multiple_of(self.col + c, LANES), self.q_cols)]

    def own(self):
        return self.shard.at[:, pl.ds(self.col, self.cols)]

    def place(self, f, q=None, half=None):
        r, c = (0, 0) if q is None else self.quarter(q)
        r = f * self.rows + r
        if q is None:
            n_r, n_c = self.rows, self.cols
        elif half is None:
            n_r, n_c = self.q_rows, self.q_cols
        else:
            dr, n_r, dc, n_c = self.halves[half]
            r, c = r + dr, c + dc
        if n_c == self.cols:
            return self.full.at[pl.ds(pl.multiple_of(r, 16), n_r)]
        return self.full.at[pl.ds(pl.multiple_of(r, 16), n_r), pl.ds(pl.multiple_of(c, LANES), n_c)]


class Net:
    def __init__(self, send_sem, recv_sem):
        self.send_sem, self.recv_sem = send_sem, recv_sem
        self.d, self.f = lax.axis_index('dp'), lax.axis_index('fsdp')
        self.z, self.core = self.f // 2, lax.rem(self.f, 2)
        self.dx = lax.rem(self.d + 2, 4)
        self.dy = self.d + 1 - 2 * lax.rem(self.d, 2)
        self.dd = lax.rem(self.dy + 2, 4)
        self.sib = self.z * 2 + 1 - self.core

    def to(self, k):
        return lax.rem(self.z + k, 4) * 2 + self.core

    def plane(self, k):
        return lax.rem(self.z + 4 - k, 4)

    def origin(self, k):
        return self.plane(k) * 2 + self.core

    def copy(self, it, src, dst, s, r, dev):
        return pltpu.make_async_remote_copy(
            src_ref=src, dst_ref=dst, send_sem=self.send_sem.at[it.index, s], recv_sem=self.recv_sem.at[it.index, r],
            device_id=dev, device_id_type=MESH,
        )

    def along_z(self, it, k):
        return self.copy(it, it.source(self.d), it.place(self.f, self.d), k - 1, k - 1, (self.d, self.to(k)))

    def to_x(self, it, k):
        ref = it.place(self.origin(k), self.d)
        return self.copy(it, ref, ref, 2 + k, 2 + k, (self.dx, self.f))

    def to_y(self, it, k):
        ref = it.place(self.origin(k), self.d)
        return self.copy(it, ref, ref, 5 + k, 5 + k, (self.dy, self.f))

    def diag_y(self, it, k):
        ref = it.place(self.origin(k), self.dx, 0)
        return self.copy(it, ref, ref, 8 + k, 8 + k, (self.dy, self.f))

    def diag_x(self, it, k):
        ref = it.place(self.origin(k), self.dy, 1)
        return self.copy(it, ref, ref, 11 + k, 11 + k, (self.dx, self.f))

    def to_core(self, it, k):
        ref = it.place(self.origin(k))
        return self.copy(it, ref, ref, 14 + k, 14 + k, (self.d, self.sib))

    def own_copy(self, it):
        return self.copy(it, it.own(), it.place(self.f), 18, 18, (self.d, self.sib))

    def arrived(self, it, ref, r):
        self.copy(it, ref, ref, 0, r, (self.d, self.f)).wait_recv()

    def barrier(self, peers):
        sem = pltpu.get_barrier_semaphore()
        for peer in peers:
            pl.semaphore_signal(sem, inc=1, device_id=peer, device_id_type=MESH)
        pl.semaphore_wait(sem, len(peers))

    def send_z(self, its, ks=PLANES):
        for k in ks:
            for it in its:
                self.along_z(it, k).start()

    def a2(self, its, ks=PLANES):
        for k in ks:
            for it in its:
                self.arrived(it, it.place(self.origin(k), self.d), k - 1)
                self.to_x(it, k).start()
                self.to_y(it, k).start()

    def a3(self, its, ks=PLANES):
        for k in ks:
            for it in its:
                self.arrived(it, it.place(self.origin(k), self.dx), 2 + k)
                self.diag_y(it, k).start()
                self.arrived(it, it.place(self.origin(k), self.dy), 5 + k)
                self.diag_x(it, k).start()

    def a4(self, its, ks=PLANES):
        for k in ks:
            for it in its:
                self.arrived(it, it.place(self.origin(k), self.dd, 0), 8 + k)
                self.arrived(it, it.place(self.origin(k), self.dd, 1), 11 + k)
                self.to_core(it, k).start()

    def a5(self, its, ks=PLANES):
        for k in ks:
            for it in its:
                self.arrived(it, it.place(self.plane(k) * 2 + 1 - self.core), 14 + k)

    def from_core(self, its):
        for it in its:
            self.arrived(it, it.place(self.sib), 18)

    def sent(self, its):
        for it in its:
            for k in PLANES:
                for make in (self.along_z, self.to_x, self.to_y, self.diag_y, self.diag_x, self.to_core):
                    make(it, k).wait_send()
            self.own_copy(it).wait_send()


def scores(tiles, rt, low, j):
    qn, qp, kn, _ = tiles
    t = j // 2
    odd, slot, pe = j % 2, j % PE_TILE * HALF, qp[j // PE_TILE]
    nope = qn[t][odd * NOPE:(odd + 1) * NOPE]
    rotary = [pe[slot:slot + HALF], pe[LANES // 2 + slot:LANES // 2 + slot + HALF]]
    rotary.append(jnp.zeros((LANES - NOPE - ROPE, pe.shape[1]), jnp.bfloat16))
    q_tile = jnp.concatenate(rotary + [nope] if odd else [nope] + rotary, axis=0)
    k_tile = jnp.where(low, rt, kn[t]) if odd else jnp.where(low, kn[t], rt)
    return jnp.dot(k_tile, q_tile, preferred_element_type=jnp.float32)


def softmax(s, diag, zero, scale):
    half = s.shape[0] // 2
    left = jnp.where(diag, s[:half, :half], MASKED)
    up = s[:half, half:]
    right = jnp.where(diag, s[half:, half:], MASKED)
    m_l = jnp.max(left, axis=0, keepdims=True) * scale
    m_r = jnp.max(jnp.maximum(up, right), axis=0, keepdims=True) * scale
    e_l = jnp.exp2(left * scale - m_l)
    e_u = jnp.exp2(up * scale - m_r)
    e_r = jnp.exp2(right * scale - m_r)
    r_l = 1.0 / jnp.sum(e_l, axis=0, keepdims=True)
    r_r = 1.0 / jnp.sum(e_u + e_r, axis=0, keepdims=True)
    p_top = jnp.concatenate([(e_l * r_l).astype(jnp.bfloat16), (e_u * r_r).astype(jnp.bfloat16)], axis=1)
    p_bot = jnp.concatenate([zero, (e_r * r_r).astype(jnp.bfloat16)], axis=1)
    return jnp.concatenate([p_top, p_bot], axis=0)


def pieces(cq, lat, wuq, wukv, g, cos, sin):
    w = 2 * LANES

    def tiles(x, weights, cols, n, pe=False):
        r = jnp.dot(x, weights[:, g * cols + n * w:g * cols + (n + 1) * w], preferred_element_type=jnp.float32)
        both = [r[:, :LANES], r[:, LANES:]]
        return [(rotate(t, cos, sin) if pe else t).astype(jnp.bfloat16) for t in both]

    n_q, n_kv = Q_COLS // w, KV_COLS // w
    return [functools.partial(tiles, cq, wuq, Q_COLS, n, n == n_q - 1) for n in range(n_q)] + [
        functools.partial(tiles, lat, wukv, KV_COLS, n) for n in range(n_kv)
    ]


def arrange_tiles(made):
    flat = [t for pair in made for t in pair]
    n = GROUP // 2
    m = n + GROUP // PE_TILE
    turned = [t.T for t in flat[:m]]
    return turned[:n], turned[n:], flat[m:m + n], [t.T for t in flat[m + n:]]


def attend(cq, lat, rt, cq_next, lat_next, start, wuq, wukv, cos, sin, hold, o_ref):
    n_groups = wuq.shape[1] // Q_COLS
    scale = (NOPE + ROPE) ** -0.5 * LOG2E
    seq_len = cq.shape[0]
    half = seq_len // 2
    low = lax.broadcasted_iota(jnp.int32, (1, LANES), 1) < NOPE
    diag = lax.broadcasted_iota(jnp.int32, (half, half), 0) <= lax.broadcasted_iota(jnp.int32, (half, half), 1)
    zero = jnp.zeros((half, half), jnp.bfloat16)
    n_pieces = hold.shape[0] // 2

    def put(n, made):
        for m, t in enumerate(made):
            hold[2 * n + m] = t

    @pl.when(start)
    def _():
        for n, make in enumerate(pieces(cq, lat, wuq, wukv, 0, cos, sin)):
            put(n, make())

    tiles = {0: arrange_tiles([[hold[2 * n], hold[2 * n + 1]] for n in range(n_pieces)])}
    total = n_groups * GROUP
    s, p, outs = {}, {}, {}
    for u in range(-AHEAD, total + 1):
        g, j = divmod(u, GROUP)
        if u >= 0 and u < total:
            p[u] = softmax(s.pop(u), diag, zero, scale)
            if j == 0:
                made = []
                if g + 1 < n_groups:
                    todo = pieces(cq, lat, wuq, wukv, g + 1, cos, sin)
                else:
                    todo = pieces(cq_next, lat_next, wuq, wukv, 0, cos, sin)
            if j < SPREAD:
                for n in range(j * n_pieces // SPREAD, (j + 1) * n_pieces // SPREAD):
                    made.append(todo[n]())
                if len(made) == n_pieces and g + 1 < n_groups:
                    tiles[g + 1] = arrange_tiles(made)
                elif len(made) == n_pieces:
                    for n, m in enumerate(made):
                        put(n, m)
        if u + AHEAD < total:
            v = u + AHEAD
            s[v] = scores(tiles[v // GROUP], rt, low, v % GROUP)
        if u >= 1:
            h = u - 1
            hj = h % GROUP
            vt = tiles[h // GROUP][3][hj // 2][hj % 2 * VDIM:(hj % 2 + 1) * VDIM]
            outs[h] = jnp.dot(vt, p.pop(h), preferred_element_type=jnp.float32).astype(jnp.bfloat16)
            if h % 2 == 1:
                pair = jnp.concatenate([outs.pop(h - 1), outs.pop(h)], axis=0)
                o_ref[0, :, h // 2 * LANES:(h // 2 + 1) * LANES] = pair.T


def core_kernel(
    n_prompts, x_ref, gs_ref, dq_s, dkv_s, uq_s, ukv_s, out_s, cos_ref, sin_ref, kcos, kahead, kbehind,
    c_all, r_ref, oa_ref, ob_ref, wout_ref,
    wdq, wdkv, wuqa, wuqb, wukva, wukvb, gains, gvec, a_all, acc, cq_all, rt_all, stage, hold,
    send_sem, recv_sem, g_send, g_recv, local_sem,
):
    i = pl.program_id(0)
    key_tables = (kcos, kahead, kbehind)
    net = Net(send_sem, recv_sem)
    d, f = net.d, net.f
    n_a, m_a = wuqa.shape[1], wukva.shape[1]
    todo = [
        (dkv_s, 0, wdkv), (dq_s, 0, wdq), (ukv_s, 0, wukva), (uq_s, 0, wuqa),
        (ukv_s, m_a, wukvb), (uq_s, n_a, wuqb), (out_s, 0, wout_ref),
    ]
    items = [Item(n, shard, col, full.shape[1], full) for n, (shard, col, full) in enumerate(todo)]
    down, first, rest, last = items[:2], items[2:4], items[4:6], items[6:]
    wo = items[6]
    others = range(1, 8)

    def keep(it):
        return pltpu.make_async_copy(it.own(), stage if it is wo else it.place(f), local_sem.at[it.index])

    def keep_out():
        return pltpu.make_async_copy(stage, wo.place(f), local_sem.at[7])

    def keep_gain():
        return pltpu.make_async_copy(gs_ref, gains.at[f], local_sem.at[8])

    def gain_copy(j):
        return pltpu.make_async_remote_copy(
            src_ref=gs_ref, dst_ref=gains.at[f], send_sem=g_send.at[j - 1], recv_sem=g_recv.at[j - 1],
            device_id=(d, lax.rem(f + j, 8)), device_id_type=MESH,
        )

    @pl.when(i == 0)
    def _():
        net.barrier([(net.dx, f), (net.dy, f)] + [(d, lax.rem(f + j, 8)) for j in others])
        for j in others:
            gain_copy(j).start()
        keep_gain().start()
        for it in down:
            net.own_copy(it).start()
            keep(it).start()
        net.send_z(down)
        for it in items[2:]:
            net.own_copy(it).start()
            keep(it).start()
        for j in others:
            gain_copy(j).wait_recv()
        keep_gain().wait()
        total = jnp.sum(gains[...], axis=0)
        for t in range(gvec.shape[1] // LANES):
            gvec[:, t * LANES:(t + 1) * LANES] = total[t:t + 1, :]
        for it in down:
            keep(it).wait()
        net.from_core(down)

    d_model, q_rank, kv_rank = x_ref.shape[-1], cq_all.shape[-1], c_all.shape[-1]
    seq_len = x_ref.shape[1]
    k_rows = d_model // 4
    half = n_prompts // 2
    c1 = n_prompts
    c2 = c1 + half
    fin = c2 + half
    pa = fin + half
    pb = pa + n_prompts
    end = pb + n_prompts - 1
    one, two, three = ((k,) for k in PLANES)

    @pl.when(i == 1)
    def _():
        keep(wo).wait()
        keep_out().start()

    def ready(its):
        for it in its:
            (keep_out() if it is wo else keep(it)).wait()
        net.from_core(its)
        net.a5(its)

    plan = [
        (1, [(net.send_z, first, one)]),
        (2, [(net.send_z, rest, one)]),
        (3, [(net.send_z, first, three)]),
        (5, [(net.a2, down, one), (net.send_z, first, two)]),
        (6, [(net.a3, down, one)]),
        (7, [(net.a2, down, two)]),
        (8, [(net.a4, down, one), (net.a2, down, three), (net.a5, down, one), (net.a3, down, two)]),
        (9, [(net.a2, first, one)]),
        (10, [(net.send_z, rest, three), (net.send_z, last, one)]),
        (11, [(net.a4, down, two), (net.a3, down, three)]),
        (12, [(net.a2, first, three), (net.a3, first, one), (net.a5, down, two), (net.send_z, rest, two)]),
        (13, [(net.a2, first, two), (net.a2, rest, one), (net.a4, down, three)]),
        (15, [(net.a3, first, two), (net.a5, down, three)]),
        (16, [(net.a4, first, one), (net.a3, first, three), (net.a2, rest, three)]),
        (17, [(net.a4, first, two)]),
        (19, [(net.a4, first, three), (net.a3, rest, three)]),
        (20, [(net.send_z, last, two), (net.a2, rest, two)]),
        (21, [(net.a3, rest, one)]),
        (22, [(net.a2, last, one)]),
        (24, [(net.a4, rest, one), (net.send_z, last, three)]),
        (25, [(net.a3, rest, two), (net.a4, rest, three)]),
        (27, [(net.a4, rest, two), (net.a2, last, two)]),
        (28, [(net.a3, last, one)]),
        (29, [(net.a2, last, three)]),
        (31, [(net.a3, last, two)]),
        (32, [(net.a4, last, one)]),
        (33, [(net.a3, last, three)]),
        (34, [(net.a4, last, two)]),
        (35, [(net.a4, last, three)]),
    ]
    for step, acts in plan:
        @pl.when(i == step)
        def _(acts=acts):
            for act, its, ks in acts:
                act(its, ks)

    for step, its in ((pa, first), (pb, rest)):
        @pl.when(i == step)
        def _(its=its):
            ready(its)

    def partial_sums(p, n, k):
        rows = pl.ds(pl.multiple_of(net.plane(k) * k_rows, LANES), k_rows)
        a = a_all[pl.ds(p, n), :, rows].reshape(n * seq_len, k_rows)
        qd = jnp.dot(a, wdq[rows], preferred_element_type=jnp.float32)
        kd = jnp.dot(a, wdkv[rows], preferred_element_type=jnp.float32)
        if k > 0:
            old = acc[pl.ds(p, n)].reshape(n * seq_len, q_rank + kv_rank + LANES)
            qd += old[:, :q_rank]
            kd += old[:, q_rank:]
        return qd, kd

    def add_plane(p, n, k):
        qd, kd = partial_sums(p, n, k)
        acc[pl.ds(p, n), :, :q_rank] = qd.reshape(n, seq_len, q_rank)
        acc[pl.ds(p, n), :, q_rank:] = kd.reshape(n, seq_len, kv_rank + LANES)

    @pl.when(i < c1)
    def _():
        x = x_ref[0].astype(jnp.float32)
        a_all[i] = (x * inv_rms(x) * gvec[:, :d_model]).astype(jnp.bfloat16)
        add_plane(i, 1, 0)

    @pl.when(jnp.logical_and(i >= c1, i < c2))
    def _():
        add_plane((i - c1) * 2, 2, 1)

    @pl.when(jnp.logical_and(i >= c2, i < fin))
    def _():
        add_plane((i - c2) * 2, 2, 2)

    @pl.when(jnp.logical_and(i >= fin, i < pa))
    def _():
        p = (i - fin) * 2
        qd, kd = partial_sums(p, 2, 3)
        cq = (qd * inv_rms(qd) * gvec[:, d_model:d_model + q_rank]).astype(jnp.bfloat16)
        cq_all[pl.ds(p, 2)] = cq.reshape(2, seq_len, q_rank)
        lat = kd[:, :kv_rank]
        lat = (lat * inv_rms(lat) * gvec[:, d_model + q_rank:]).astype(jnp.bfloat16)
        c_all[pl.ds(p, 2)] = lat.reshape(2, seq_len, kv_rank)
        for n in range(2):
            pe = kd[n * seq_len:(n + 1) * seq_len, kv_rank:]
            rt = rotate_key(pe, *[t[...] for t in key_tables]).astype(jnp.bfloat16)
            rt_all[p + n] = rt
            r_ref[p + n] = rt.T[:ROPE]

    def attend_step(p, wuq, wukv, o_ref):
        after = jnp.minimum(p + 1, n_prompts - 1)
        attend(
            cq_all[p], c_all[p], rt_all[p], cq_all[after], c_all[after], p == 0,
            wuq, wukv, cos_ref[...], sin_ref[...], hold, o_ref,
        )

    @pl.when(jnp.logical_and(i >= pa, i < pb))
    def _():
        attend_step(i - pa, wuqa, wukva, oa_ref)

    @pl.when(i >= pb)
    def _():
        attend_step(i - pb, wuqb, wukvb, ob_ref)

    @pl.when(i == end)
    def _():
        ready(last)
        for j in others:
            gain_copy(j).wait_send()
        net.sent(items)


def one_hot(source, n_rows):
    rows = lax.broadcasted_iota(jnp.int32, (n_rows, source.shape[1]), 0)
    return (rows == source).astype(jnp.float32).astype(jnp.bfloat16)


def pick(w, matrix):
    return jnp.dot(w, matrix, preferred_element_type=jnp.float32).astype(jnp.bfloat16)


def prepare_kernel(g1_ref, gq_ref, gkv_ref, wuq_ref, wukv_ref, wdkv_ref, gs_ref, uq_ref, ukv_ref, dkv_ref):
    f = lax.axis_index('fsdp')
    row = 0
    gs_ref[...] = jnp.zeros_like(gs_ref)
    for g in (g1_ref, gq_ref, gkv_ref):
        n = g.shape[1]
        for t in range(n * 8 // LANES):
            index = lax.broadcasted_iota(jnp.int32, (1, LANES), 1) + (t * LANES - f * n)
            gs_ref[row:row + 1, :] = jnp.dot(g[...], one_hot(index, n), preferred_element_type=jnp.float32)
            row += 1

    def column(n):
        return lax.broadcasted_iota(jnp.int32, (1, n), 1)

    c = column(Q_COLS)
    n_nope = GROUP * NOPE
    pe = c - n_nope
    head = pe // LANES * PE_TILE + lax.rem(pe, LANES // 2) // HALF
    pe = head * (NOPE + ROPE) + NOPE + lax.rem(pe, LANES) // (LANES // 2) * HALF + lax.rem(pe, HALF)
    order = one_hot(jnp.where(c < n_nope, c // NOPE * (NOPE + ROPE) + lax.rem(c, NOPE), pe), Q_COLS)
    for g in range(wuq_ref.shape[1] // Q_COLS):
        cols = slice(g * Q_COLS, (g + 1) * Q_COLS)
        uq_ref[:, cols] = pick(wuq_ref[:, cols], order)

    c = column(KV_COLS)
    part = lax.rem(c, n_nope)
    order = one_hot(part // NOPE * (NOPE + VDIM) + c // n_nope * NOPE + lax.rem(part, NOPE), KV_COLS)
    for g in range(wukv_ref.shape[1] // KV_COLS):
        cols = slice(g * KV_COLS, (g + 1) * KV_COLS)
        ukv_ref[:, cols] = pick(wukv_ref[:, cols], order)

    kv_rank = dkv_ref.shape[1] - LANES
    c = column(LANES)
    wdkv = wdkv_ref[...].T
    dkv_ref[:, :kv_rank] = wdkv[:, :kv_rank]
    c = lax.rem(c, LANES // 2)
    order = one_hot(jnp.where(c < ROPE, c, -1), ROPE)
    dkv_ref[:, kv_rank:] = pick(wdkv[:, kv_rank:], order)


def out_kernel(x_ref, oa_ref, ob_ref, w_hbm, c_in, r_in, y_ref, c_out, r_out, w, sem):
    step = 512
    n_steps = y_ref.shape[1] // step
    first = pl.program_id(0) == 0
    cols = [slice(n * step, (n + 1) * step) for n in range(n_steps)]
    load = [pltpu.make_async_copy(w_hbm.at[:, c], w.at[:, c], sem.at[n]) for n, c in enumerate(cols)]

    o = jnp.concatenate([oa_ref[...], ob_ref[...]], axis=1)
    c_out[...] = c_in[...]
    r_out[...] = r_in[...]

    def product(c):
        acc = jnp.dot(o, w[:, c], preferred_element_type=jnp.float32)
        y_ref[:, c] = (x_ref[:, c].astype(jnp.float32) + acc).astype(jnp.bfloat16)

    @pl.when(first)
    def _():
        for part in load:
            part.start()
        for part, c in zip(load, cols):
            part.wait()
            product(c)

    @pl.when(jnp.logical_not(first))
    def _():
        for c in cols:
            product(c)


def whole(shape):
    return pl.BlockSpec(shape, lambda i: (0,) * len(shape))


def solution(mesh):
    n_fsdp = mesh.shape['fsdp']

    def local_block(x, g1, wdq, gq, wuq, wdkv, gkv, wukv, wout):
        n_p, seq_len, d_model = x.shape
        kv_rank, q_rank = gkv.shape[0] * n_fsdp, wdq.shape[1]
        tables = [jnp.asarray(t) for t in rope_tiles(seq_len)]
        n_gain = d_model + q_rank + kv_rank
        like = lambda w, cols: jax.ShapeDtypeStruct((w.shape[0], cols), jnp.bfloat16)
        gs, uq, ukv, dkv = pl.pallas_call(
            prepare_kernel,
            out_shape=[
                jax.ShapeDtypeStruct((GAIN_ROWS, LANES), jnp.float32),
                like(wuq, wuq.shape[1]), like(wukv, wukv.shape[1]), like(wdkv, kv_rank + LANES),
            ],
            name="prepare",
        )(g1[None], gq[None], gkv[None], wuq, wukv, wdkv.T)
        shards = [wdq, dkv, uq, ukv]
        full = lambda w, cols: pltpu.VMEM((w.shape[0] * n_fsdp, cols), jnp.bfloat16)
        o_cols = GROUP * VDIM
        n_groups = wuq.shape[1] // Q_COLS
        first, rest = GROUPS_FIRST, n_groups - GROUPS_FIRST
        last = n_p - 1
        pa = 2 * n_p + n_p // 2
        blk = lambda cols, lag: pl.BlockSpec((1, seq_len, cols), lambda i: (jnp.clip(i - lag, 0, last), 0, 0))
        out = lambda cols: jax.ShapeDtypeStruct((n_p, seq_len, cols), jnp.bfloat16)
        r_shape = jax.ShapeDtypeStruct((n_p, ROPE, seq_len), jnp.bfloat16)
        hbm = pl.BlockSpec(memory_space=pl.ANY)
        c, r, oa, ob, wout_all = pl.pallas_call(
            functools.partial(core_kernel, n_p),
            grid=(4 * n_p + n_p // 2,),
            in_specs=[blk(d_model, 0)] + [hbm] * 6 + [whole(tables[0].shape)] * len(tables),
            out_specs=[
                whole((n_p, seq_len, kv_rank)), whole((n_p, ROPE, seq_len)),
                blk(first * o_cols, pa), blk(rest * o_cols, pa + n_p), hbm,
            ],
            out_shape=[
                out(kv_rank), r_shape, out(first * o_cols), out(rest * o_cols),
                jax.ShapeDtypeStruct((wout.shape[0] * n_fsdp, wout.shape[1]), jnp.bfloat16),
            ],
            scratch_shapes=[
                full(wdq, q_rank), full(wdkv, kv_rank + LANES),
                full(wuq, first * Q_COLS), full(wuq, rest * Q_COLS),
                full(wukv, first * KV_COLS), full(wukv, rest * KV_COLS),
                pltpu.VMEM((n_fsdp, GAIN_ROWS, LANES), jnp.float32),
                pltpu.VMEM((1, n_gain), jnp.float32),
                pltpu.VMEM((n_p, seq_len, d_model), jnp.bfloat16),
                pltpu.VMEM((n_p, seq_len, q_rank + kv_rank + LANES), jnp.float32),
                pltpu.VMEM((n_p, seq_len, q_rank), jnp.bfloat16),
                pltpu.VMEM((n_p, seq_len, LANES), jnp.bfloat16),
                pltpu.VMEM(wout.shape, jnp.bfloat16),
                pltpu.VMEM(((Q_COLS + KV_COLS) // LANES, seq_len, LANES), jnp.bfloat16),
                pltpu.SemaphoreType.DMA((7, N_COPIES)),
                pltpu.SemaphoreType.DMA((7, N_COPIES)),
                pltpu.SemaphoreType.DMA((7,)),
                pltpu.SemaphoreType.DMA((7,)),
                pltpu.SemaphoreType.DMA((9,)),
            ],
            compiler_params=pltpu.CompilerParams(
                vmem_limit_bytes=VMEM_LIMIT, dimension_semantics=("arbitrary",), collective_id=0, has_side_effects=True,
            ),
            name="core",
        )(x, gs, *shards, wout, *tables)
        rows = 512
        tile = lambda cols: pl.BlockSpec((rows, cols), lambda i: (i, 0))
        r_tile = pl.BlockSpec((rows // seq_len, ROPE, seq_len), lambda i: (i, 0, 0))
        flat = lambda v: v.reshape(n_p * seq_len, v.shape[-1])
        flat_out = lambda cols: jax.ShapeDtypeStruct((n_p * seq_len, cols), jnp.bfloat16)
        y, c, r = pl.pallas_call(
            out_kernel,
            grid=(n_p * seq_len // rows,),
            in_specs=[tile(d_model), tile(oa.shape[-1]), tile(ob.shape[-1]), hbm, tile(kv_rank), r_tile],
            out_specs=[tile(d_model), tile(kv_rank), r_tile],
            out_shape=[flat_out(d_model), flat_out(kv_rank), r_shape],
            scratch_shapes=[pltpu.VMEM(wout_all.shape, jnp.bfloat16), pltpu.SemaphoreType.DMA((8,))],
            compiler_params=pltpu.CompilerParams(vmem_limit_bytes=VMEM_LIMIT, dimension_semantics=("arbitrary",)),
            name="project",
        )(flat(x), flat(oa), flat(ob), wout_all, flat(c), r)
        back = lambda v: v.reshape(n_p, seq_len, v.shape[-1])
        return back(y), back(c), jnp.swapaxes(r, 1, 2)

    batch, row, mat = P(('dp', 'fsdp')), P('fsdp'), P('fsdp', None)
    return jax.shard_map(
        local_block,
        mesh=mesh,
        in_specs=(batch, row, mat, row, mat, mat, row, mat, mat),
        out_specs=(batch, batch, batch),
        check_vma=False,
    )
```
